128 devices in a mesh: band: 32 (over z, y, x_hi), grid: 4 (over x_lo, core).
Axes of the slice: x: 4 (x_hi: 2, x_lo: 2; x = x_hi * 2 + x_lo), y: 4, z: 4, core: 2. Of those that a mesh axis runs over, the one named last changes fastest.
Arguments:
- orbitals: float32 [128, 110592], P('band', 'grid'), may hold values from -6 to 6
Outputs:
- exchange_vectors: float32 [128, 110592], P('band', 'grid')
- margin: float32 [128, 128], P('grid', 'band')
The draws below stay inside these ranges and needn't reach their ends.
All inputs are finite; a program needn't handle non-finite values.
Results may differ from the reference program's by a relative error of at most 0.00012.
Values sent between devices are 32-bit elements; how exact they have to be, the bound alone decides.
A program may use at most 128 MiB of HBM per device.

```python
import jax
import jax.numpy as jnp
from jax import lax

NG = 48
BAND_DEV = 4
NBANDS = 128
NCELL = 110592
N_BAND = 32


def steps_of(rng, dims, split, least, top_value):
    gain, own = 1.0, jax.random.fold_in(rng, 6)
    for position, shards_of in split:
        heights = jnp.exp(jax.random.uniform(jax.random.fold_in(own, position), (shards_of,), jnp.float32, least / len(split), top_value / len(split)))
        gain = gain * jnp.repeat(heights, dims[position] // shards_of).reshape([-1 if axis == position else 1 for axis in range(len(dims))])
    return gain


def normal_values(stream_key, shape, deviation, reach, split=(), kind=jnp.bfloat16):
    result = jax.random.normal(stream_key, shape, jnp.float32) * deviation
    if len(split) > 0:
        result = steps_of(stream_key, shape, split, -0.22, 0.18) * result
    return jnp.clip(result, min=-reach, max=reach).astype(kind)


def setup_inputs(seed: int = 0) -> dict:
    streams_of = jax.random.split(jax.random.key(seed), 2)
    orbitals = normal_values(streams_of[0], (NBANDS, NCELL), 1.0, 6.0, ((0, 32), (1, 4)), jnp.float32)
    return dict(orbitals=orbitals)


def folded_freq(count):
    indices = jnp.arange(count)
    return ((indices + count // 2) % count - count // 2).astype(jnp.float32)


def kernel_table():
    freqs = folded_freq(NG)
    squares = freqs[:, None, None] ** 2 + freqs[None, :, None] ** 2 + freqs[None, None, :] ** 2
    safe_sq = jnp.where(squares > 0, squares, jnp.float32(1.0))
    return jnp.where(squares > 0, 40.0 * (1.0 - jnp.exp(-squares / 16.0)) / safe_sq, jnp.float32(0.0))


def reference(orbitals):
    kernel = kernel_table()
    blocks = orbitals.reshape(N_BAND, BAND_DEV, NCELL)
    window = jnp.concatenate([blocks, jnp.roll(blocks, 1, axis=0), jnp.roll(blocks, -1, axis=0)], axis=1)

    def per_band(single, partners):
        density = (single[None, :] * partners).reshape(-1, NG, NG, NG)
        spectrum = jnp.fft.fftn(density, axes=(1, 2, 3))
        potential = jnp.real(jnp.fft.ifftn(spectrum * kernel, axes=(1, 2, 3))).reshape(-1, NCELL)
        return -jnp.sum(partners * potential, axis=0)

    def per_block(args):
        own_block, partners = args
        return lax.map(lambda single: per_band(single, partners), own_block)

    vectors = lax.map(per_block, (blocks, window)).reshape(NBANDS, NCELL).astype(jnp.float32)
    margin = jnp.dot(orbitals, vectors.T, precision=lax.Precision.HIGHEST, preferred_element_type=jnp.float32) / NCELL
    return vectors, margin
```

```python
import functools
import numpy as np
import jax
import jax.numpy as jnp
from jax import lax
from jax.experimental import pallas as pl
from jax.experimental.pallas import tpu as pltpu
from jax.sharding import PartitionSpec as P

NG = 48
NCELL = 110592
BF = jnp.bfloat16
F32 = jnp.float32


def split_np(a):
    hi = a.astype(BF)
    lo = (a - hi.astype(np.float64)).astype(BF)
    return hi, lo


def tables():
    n = np.arange(NG)
    ang = 2.0 * np.pi * ((n[:, None] * n[None, :]) % NG) / NG
    h = np.cos(ang) + np.sin(ang)
    w = np.zeros((8, NG, 6, 8, 8))
    for y in range(8):
        w[y, :, :, y, :] = h.reshape(NG, 6, 8)
    w = w.reshape(384, 384)
    v = np.kron(h, np.eye(8))
    f = ((n + 24) % 48 - 24).astype(np.float64)
    q = f[:, None, None] ** 2 + f[None, :, None] ** 2 + f[None, None, :] ** 2
    k = np.where(q > 0, 40.0 * (1.0 - np.exp(-q / 16.0)) / np.where(q > 0, q, 1.0), 0.0) / NCELL
    k = k.reshape(NG, NG, 6, 8).transpose(2, 0, 1, 3).reshape(288, 384)

    def pack(m):
        hi, lo = split_np(m)
        return np.concatenate([hi, hi, lo], axis=0)

    hh, hl = split_np(h)
    hx = np.concatenate([hh, hh, hl], axis=1)
    return pack(w), pack(v), pack(w.T.copy()), hx, k.astype(np.float32)


def hilo(x):
    hi = x.astype(BF)
    lo = (x - hi.astype(F32)).astype(BF)
    return hi, lo


def put(s_ref, row, rows, lane, x):
    hi, lo = hilo(x)
    n = x.shape[1]
    s_ref[row : row + rows, lane : lane + n] = hi
    s_ref[row : row + rows, 384 + lane : 384 + lane + n] = lo


def mm3(s_ref, w_ref):
    return jnp.dot(s_ref[...], w_ref[0:768, :], preferred_element_type=F32) + jnp.dot(
        s_ref[:, 0:384], w_ref[768:1152, :], preferred_element_type=F32
    )


def swap(t_ref, s_ref, pb, left):
    for p in range(pb):
        for j in range(3):
            for m in range(3):
                r0 = p * 288 + 2 * j * 48
                e = t_ref[r0 : r0 + 48, 128 * m : 128 * m + 128]
                o = t_ref[r0 + 48 : r0 + 96, 128 * m : 128 * m + 128]
                d0 = p * 288 + 2 * m * 48
                put(s_ref, d0, 48, 128 * j, jnp.where(left, e, pltpu.roll(o, 64, 1)))
                put(s_ref, d0 + 48, 48, 128 * j, jnp.where(left, pltpu.roll(e, 64, 1), o))


def potential(pb, s_ref, t_ref, r_ref, w_ref, v_ref, wt_ref, hx_ref, k_ref):
    left = lax.broadcasted_iota(jnp.int32, (48, 128), 1) < 64
    t_ref[...] = mm3(s_ref, w_ref)
    swap(t_ref, s_ref, pb, left)
    t_ref[...] = mm3(s_ref, v_ref)
    h2 = hx_ref[:, 0:96]
    h1 = hx_ref[:, 96:144]

    def xdot(row):
        return jnp.dot(h2, r_ref[row : row + 96, :], preferred_element_type=F32) + jnp.dot(
            h1, r_ref[row : row + 48, :], preferred_element_type=F32
        )

    for i in range(pb * 6):
        hi, lo = hilo(t_ref[i * 48 : i * 48 + 48, :])
        r_ref[i * 192 : i * 192 + 48, :] = hi
        r_ref[i * 192 + 48 : i * 192 + 96, :] = lo
        z = i % 6
        d = xdot(i * 192) * k_ref[z * 48 : z * 48 + 48, :]
        hi, lo = hilo(d)
        r_ref[i * 192 + 96 : i * 192 + 144, :] = hi
        r_ref[i * 192 + 144 : i * 192 + 192, :] = lo
        put(s_ref, i * 48, 48, 0, xdot(i * 192 + 96))
    t_ref[...] = mm3(s_ref, v_ref)
    swap(t_ref, s_ref, pb, left)
    t_ref[...] = mm3(s_ref, wt_ref)


def solve_kernel(pb, idx_ref, own_ref, low_ref, w_ref, v_ref, wt_ref, hx_ref, k_ref, u_out, o_out, a_ref, u_ref, s_ref, t_ref, r_ref):
    for r in range(18):
        for xg in range(6):
            row, lane = (r // 3) * 48 + xg * 8, (r % 3) * 128
            for b in range(4):
                a_ref[b, row : row + 8, lane : lane + 128] = own_ref[pl.ds((xg * 144 + r) * 4 + b, 8, stride=72), :]
            a_ref[4, row : row + 8, lane : lane + 128] = low_ref[pl.ds(xg * 144 + r, 8, stride=18), :]
    u_ref[...] = jnp.zeros_like(u_ref)

    def step(n, carry):
        for p in range(pb):
            i, j = idx_ref[n * pb + p, 0], idx_ref[n * pb + p, 1]
            put(s_ref, p * 288, 288, 0, a_ref[i] * a_ref[j])
        potential(pb, s_ref, t_ref, r_ref, w_ref, v_ref, wt_ref, hx_ref, k_ref)
        for p in range(pb):
            i, j = idx_ref[n * pb + p, 0], idx_ref[n * pb + p, 1]
            use = idx_ref[n * pb + p, 2].astype(F32)
            other = idx_ref[n * pb + p, 3].astype(F32)
            t = t_ref[p * 288 : p * 288 + 288, :]
            u_ref[i] = u_ref[i] - use * a_ref[j] * t
            u_ref[j] = u_ref[j] - other * a_ref[i] * t
        return carry

    lax.fori_loop(0, 8 // pb, step, 0)
    for r in range(18):
        for xg in range(6):
            row, lane = (r // 3) * 48 + xg * 8, (r % 3) * 128
            for b in range(4):
                u_out[pl.ds((xg * 144 + r) * 4 + b, 8, stride=72), :] = u_ref[b, row : row + 8, lane : lane + 128]
            o_out[pl.ds(xg * 144 + r, 8, stride=18), :] = u_ref[4, row : row + 8, lane : lane + 128]


def solve(idx, own, low, pb=2):
    w, v, wt, hx, k = tables()
    vm = pl.BlockSpec(memory_space=pltpu.VMEM)
    return pl.pallas_call(
        functools.partial(solve_kernel, pb),
        out_shape=(jax.ShapeDtypeStruct((3456, 128), F32), jax.ShapeDtypeStruct((864, 128), F32)),
        in_specs=[pl.BlockSpec(memory_space=pltpu.SMEM)] + [vm] * 7,
        out_specs=(vm, vm),
        scratch_shapes=[
            pltpu.VMEM((5, 288, 384), F32),
            pltpu.VMEM((5, 288, 384), F32),
            pltpu.VMEM((pb * 288, 768), BF),
            pltpu.VMEM((pb * 288, 384), F32),
            pltpu.VMEM((pb * 6 * 192, 384), BF),
        ],
        compiler_params=pltpu.CompilerParams(vmem_limit_bytes=60 * 1024 * 1024),
    )(idx, own, low, w, v, wt, hx, k)


N_GRID = 4


def own_pairs(g):
    table = np.array(
        [
            [(0, 0, 1, 0), (1, 1, 1, 0), (0, 1, 1, 1), (0, 0, 0, 0)],
            [(2, 2, 1, 0), (0, 2, 1, 1), (0, 0, 0, 0), (0, 0, 0, 0)],
            [(3, 3, 1, 0), (2, 3, 1, 1), (1, 3, 1, 1), (0, 0, 0, 0)],
            [(0, 3, 1, 1), (1, 2, 1, 1), (0, 0, 0, 0), (0, 0, 0, 0)],
        ],
        np.int32,
    )
    cross = np.array([(i, 4, 1, 1) for i in range(4)], np.int32)
    return jnp.concatenate([cross, lax.dynamic_index_in_dim(jnp.asarray(table), g, 0, False)], axis=0)


def cut_along(shard, dim, length):
    lengths = shard.shape
    pieces = shard.reshape(*lengths[:dim], length, lengths[dim] // length, *lengths[dim + 1 :])
    return jnp.moveaxis(pieces, dim, 0)


def sent_and_summed(shard, axis, dim):
    length = lax.axis_size(axis)
    pieces = lax.all_to_all(cut_along(shard, dim, length), axis, 0, 0, tiled=True)
    return jnp.sum(pieces, axis=0)


def on_device(orbitals):
    g = lax.axis_index("grid")
    nb = lax.axis_size("band")
    mine = orbitals.reshape(4, 216, 128).transpose(1, 0, 2).reshape(864, 128)
    own = lax.all_gather(mine, "grid", axis=0, tiled=True)
    send = lax.dynamic_index_in_dim(own.reshape(864, 4, 128), g, 1, False)
    up = [(b * 4 + k, (b + 1) % nb * 4 + (k + 2) % 4) for b in range(nb) for k in range(4)]
    down = [(t, s) for s, t in up]
    low = lax.ppermute(send, ("band", "grid"), up)
    u, o = solve(own_pairs(g), own, low)
    owed = lax.ppermute(o, ("band", "grid"), down)
    mark = (jnp.arange(4) == g).astype(F32)
    total = u.reshape(864, 4, 128) + owed[:, None, :] * mark[None, :, None]
    parts = lax.all_to_all(total.reshape(4, 864, 128), "grid", 0, 0, tiled=True)
    vec = jnp.sum(parts, axis=0)
    vectors = vec.reshape(216, 4, 128).transpose(1, 0, 2).reshape(4, 27648)
    every = lax.all_gather(orbitals, "band", axis=0, tiled=True)
    margin = sent_and_summed(
        lax.dot_general(
            every, vectors, (((1,), (1,)), ((), ())), precision=lax.Precision.HIGHEST, preferred_element_type=F32
        )
        / NCELL,
        "grid",
        0,
    )
    return vectors, margin


def solution(mesh):
    return jax.shard_map(
        on_device,
        mesh=mesh,
        in_specs=(P("band", "grid"),),
        out_specs=(P("band", "grid"), P("grid", "band")),
        check_vma=False,
    )
```

```python
import functools
import numpy as np
import jax
import jax.numpy as jnp
from jax import lax
from jax.experimental import pallas as pl
from jax.experimental.pallas import tpu as pltpu
from jax.sharding import PartitionSpec as P

NG = 48
NCELL = 110592
BF = jnp.bfloat16
F32 = jnp.float32


def split_np(a):
    hi = a.astype(BF)
    lo = (a - hi.astype(np.float64)).astype(BF)
    return hi, lo


def tables():
    n = np.arange(NG)
    ang = 2.0 * np.pi * ((n[:, None] * n[None, :]) % NG) / NG
    h = np.cos(ang) + np.sin(ang)
    w = np.zeros((8, NG, 6, 8, 8))
    for y in range(8):
        w[y, :, :, y, :] = h.reshape(NG, 6, 8)
    w = w.reshape(384, 384)
    v = np.kron(h, np.eye(8))
    f = ((n + 24) % 48 - 24).astype(np.float64)
    q = f[:, None, None] ** 2 + f[None, :, None] ** 2 + f[None, None, :] ** 2
    k = np.where(q > 0, 40.0 * (1.0 - np.exp(-q / 16.0)) / np.where(q > 0, q, 1.0), 0.0) / NCELL
    k = k.reshape(NG, NG, 6, 8).transpose(2, 0, 1, 3).reshape(288, 384)

    def pack(m):
        hi, lo = split_np(m)
        return np.concatenate([hi, hi, lo], axis=0)

    hh, hl = split_np(h)
    hx = np.concatenate([hh, hh, hl], axis=1)
    return pack(w), pack(v), pack(w.T.copy()), hx, k.astype(np.float32)


def hilo(x):
    hi = x.astype(BF)
    lo = (x - hi.astype(F32)).astype(BF)
    return hi, lo


def put(s_ref, row, rows, lane, x):
    hi, lo = hilo(x)
    n = x.shape[1]
    s_ref[row : row + rows, lane : lane + n] = hi
    s_ref[row : row + rows, 384 + lane : 384 + lane + n] = lo


def mm3(s_ref, w_ref):
    return jnp.dot(s_ref[...], w_ref[0:768, :], preferred_element_type=F32) + jnp.dot(
        s_ref[:, 0:384], w_ref[768:1152, :], preferred_element_type=F32
    )


def swap(t_ref, s_ref, pb, left):
    for p in range(pb):
        for j in range(3):
            for m in range(3):
                r0 = p * 288 + 2 * j * 48
                e = t_ref[r0 : r0 + 48, 128 * m : 128 * m + 128]
                o = t_ref[r0 + 48 : r0 + 96, 128 * m : 128 * m + 128]
                d0 = p * 288 + 2 * m * 48
                put(s_ref, d0, 48, 128 * j, jnp.where(left, e, pltpu.roll(o, 64, 1)))
                put(s_ref, d0 + 48, 48, 128 * j, jnp.where(left, pltpu.roll(e, 64, 1), o))


def potential(pb, s_ref, t_ref, r_ref, w_ref, v_ref, wt_ref, hx_ref, k_ref):
    left = lax.broadcasted_iota(jnp.int32, (48, 128), 1) < 64
    t_ref[...] = mm3(s_ref, w_ref)
    swap(t_ref, s_ref, pb, left)
    t_ref[...] = mm3(s_ref, v_ref)
    h2 = hx_ref[:, 0:96]
    h1 = hx_ref[:, 96:144]

    def xdot(row):
        return jnp.dot(h2, r_ref[row : row + 96, :], preferred_element_type=F32) + jnp.dot(
            h1, r_ref[row : row + 48, :], preferred_element_type=F32
        )

    for i in range(pb * 6):
        hi, lo = hilo(t_ref[i * 48 : i * 48 + 48, :])
        r_ref[i * 192 : i * 192 + 48, :] = hi
        r_ref[i * 192 + 48 : i * 192 + 96, :] = lo
        z = i % 6
        d = xdot(i * 192) * k_ref[z * 48 : z * 48 + 48, :]
        hi, lo = hilo(d)
        r_ref[i * 192 + 96 : i * 192 + 144, :] = hi
        r_ref[i * 192 + 144 : i * 192 + 192, :] = lo
        put(s_ref, i * 48, 48, 0, xdot(i * 192 + 96))
    t_ref[...] = mm3(s_ref, v_ref)
    swap(t_ref, s_ref, pb, left)
    t_ref[...] = mm3(s_ref, wt_ref)


def solve_kernel(pb, idx_ref, own_ref, low_ref, w_ref, v_ref, wt_ref, hx_ref, k_ref, u_out, o_out, a_ref, u_ref, s_ref, t_ref, r_ref):
    for r in range(18):
        for xg in range(6):
            row, lane = (r // 3) * 48 + xg * 8, (r % 3) * 128
            for b in range(4):
                a_ref[b, row : row + 8, lane : lane + 128] = own_ref[pl.ds((xg * 144 + r) * 4 + b, 8, stride=72), :]
            a_ref[4, row : row + 8, lane : lane + 128] = low_ref[pl.ds(xg * 144 + r, 8, stride=18), :]
    u_ref[...] = jnp.zeros_like(u_ref)

    def step(n, carry):
        for p in range(pb):
            i, j = idx_ref[n * pb + p, 0], idx_ref[n * pb + p, 1]
            put(s_ref, p * 288, 288, 0, a_ref[i] * a_ref[j])
        potential(pb, s_ref, t_ref, r_ref, w_ref, v_ref, wt_ref, hx_ref, k_ref)
        for p in range(pb):
            i, j = idx_ref[n * pb + p, 0], idx_ref[n * pb + p, 1]
            use = idx_ref[n * pb + p, 2].astype(F32)
            other = idx_ref[n * pb + p, 3].astype(F32)
            t = t_ref[p * 288 : p * 288 + 288, :]
            u_ref[i] = u_ref[i] - use * a_ref[j] * t
            u_ref[j] = u_ref[j] - other * a_ref[i] * t
        return carry

    lax.fori_loop(0, 8 // pb, step, 0)
    for r in range(18):
        for xg in range(6):
            row, lane = (r // 3) * 48 + xg * 8, (r % 3) * 128
            for b in range(4):
                u_out[pl.ds((xg * 144 + r) * 4 + b, 8, stride=72), :] = u_ref[b, row : row + 8, lane : lane + 128]
            o_out[pl.ds(xg * 144 + r, 8, stride=18), :] = u_ref[4, row : row + 8, lane : lane + 128]


def solve(idx, own, low, pb=2):
    w, v, wt, hx, k = tables()
    vm = pl.BlockSpec(memory_space=pltpu.VMEM)
    return pl.pallas_call(
        functools.partial(solve_kernel, pb),
        out_shape=(jax.ShapeDtypeStruct((3456, 128), F32), jax.ShapeDtypeStruct((864, 128), F32)),
        in_specs=[pl.BlockSpec(memory_space=pltpu.SMEM)] + [vm] * 7,
        out_specs=(vm, vm),
        scratch_shapes=[
            pltpu.VMEM((5, 288, 384), F32),
            pltpu.VMEM((5, 288, 384), F32),
            pltpu.VMEM((pb * 288, 768), BF),
            pltpu.VMEM((pb * 288, 384), F32),
            pltpu.VMEM((pb * 6 * 192, 384), BF),
        ],
        compiler_params=pltpu.CompilerParams(vmem_limit_bytes=60 * 1024 * 1024),
    )(idx, own, low, w, v, wt, hx, k)


MESH = pl.DeviceIdType.MESH
GROUPS = 27
HIGHEST = lax.Precision.HIGHEST


def rcopy(src, dst, send, recv, band, grid):
    return pltpu.make_async_remote_copy(
        src_ref=src, dst_ref=dst, send_sem=send, recv_sem=recv, device_id={"band": band, "grid": grid}, device_id_type=MESH
    )


def landed(ref, sem):
    pltpu.make_async_copy(ref, ref, sem).wait()


def greet(nb, me, g):
    barrier = pltpu.get_barrier_semaphore()

    def one(o, c):
        pl.semaphore_signal(barrier, inc=1, device_id={"band": (me + o) % nb, "grid": g}, device_id_type=MESH)
        return c

    lax.fori_loop(1, nb, one, 0)
    for o in range(1, 4):
        pl.semaphore_signal(barrier, inc=1, device_id={"band": me, "grid": (g + o) % 4}, device_id_type=MESH)
    pl.semaphore_wait(barrier, nb + 2)


def scatter_groups(src, buf, send, recv, nb, me, g):
    def one(o, c):
        dst = (me + o) % nb

        @pl.when(dst < GROUPS)
        def _():
            rcopy(
                src.at[pl.ds(pl.multiple_of(dst * 32, 32), 32)], buf.at[pl.ds(pl.multiple_of(me * 32, 32), 32)], send, recv, dst, g
            ).start()

        return c

    lax.fori_loop(1, nb, one, 0)

    @pl.when(me < GROUPS)
    def _():
        rows = pl.ds(pl.multiple_of(me * 32, 32), 32)
        buf[rows, :] = src[rows, :]


def sent_all(ref, send, me, unit):
    @pl.when(me < GROUPS)
    def _():
        landed(ref.at[0 : (GROUPS - 1) * unit], send)

    @pl.when(me >= GROUPS)
    def _():
        landed(ref.at[0 : GROUPS * unit], send)


def margin_tail(nb, me, g, out_ref, obuf, vbuf, amat, bmat, mt8, red, gsum, rs, rr, gs, gr):
    @pl.when(me < GROUPS)
    def _():
        for c in range(8):
            for b in range(4):
                rows = pl.ds(c * 4 + b, 32, stride=32)
                amat[c * 128 + b * 32 : c * 128 + b * 32 + 32, :] = vbuf[rows, :]
                bmat[pl.ds(c * 128 + b, 32, stride=4), :] = obuf[rows, :]
        m = jnp.zeros((128, 128), F32)
        for c in range(8):
            part = slice(c * 128, c * 128 + 128)
            m = m + lax.dot_general(
                amat[part, :], bmat[part, :], (((1,), (1,)), ((), ())), precision=HIGHEST, preferred_element_type=F32
            )
        m = m * (1.0 / NCELL)
        mt8[...] = jnp.zeros_like(mt8)
        for b in range(4):
            mt8[pl.ds(b, 32, stride=8), :] = m[b * 32 : b * 32 + 32, :]

        def one(o, c):
            dst = (me + o) % nb
            rcopy(
                mt8.at[pl.ds(pl.multiple_of(dst * 8, 8), 8)], red.at[pl.ds(pl.multiple_of(me * 8, 8), 8)], rs, rr, dst, g
            ).start()
            return c

        lax.fori_loop(1, nb, one, 0)
        rows = pl.ds(pl.multiple_of(me * 8, 8), 8)
        red[rows, :] = mt8[rows, :]

    sent_all(red, rr, me, 8)
    total = red[0:8, :]
    for s in range(1, GROUPS):
        total = total + red[s * 8 : s * 8 + 8, :]
    mine = pl.ds(pl.multiple_of(g * 8, 8), 8)
    gsum[mine, :] = total
    sends = [rcopy(gsum.at[mine], gsum.at[mine], gs.at[o - 1], gr.at[o - 1], me, (g + o) % 4) for o in range(1, 4)]
    for s in sends:
        s.start()
    for s in sends:
        s.wait()
    full = gsum[0:8, :] + gsum[8:16, :] + gsum[16:24, :] + gsum[24:32, :]
    picked = jnp.zeros((4, 32), F32)
    for t in range(4):
        picked = picked + jnp.where(g == t, 1.0, 0.0) * full[0:4, t * 32 : t * 32 + 32]
    out_ref[...] = picked

    @pl.when(me < GROUPS)
    def _():
        landed(mt8.at[0 : 31 * 8], rs)


def margin_kernel(nb, orb_ref, vec_ref, out_ref, obuf, vbuf, amat, bmat, mt8, red, gsum, os, orr, vs, vr, rs, rr, gs, gr):
    me, g = lax.axis_index("band"), lax.axis_index("grid")
    greet(nb, me, g)
    scatter_groups(orb_ref, obuf, os, orr, nb, me, g)
    scatter_groups(vec_ref, vbuf, vs, vr, nb, me, g)

    @pl.when(me < GROUPS)
    def _():
        landed(obuf.at[0 : 31 * 32], orr)
        landed(vbuf.at[0 : 31 * 32], vr)

    margin_tail(nb, me, g, out_ref, obuf, vbuf, amat, bmat, mt8, red, gsum, rs, rr, gs, gr)
    sent_all(obuf, os, me, 32)
    sent_all(vbuf, vs, me, 32)


MARGIN_SCRATCH = [
    pltpu.VMEM((1024, 128), F32),
    pltpu.VMEM((1024, 128), F32),
    pltpu.VMEM((1024, 128), F32),
    pltpu.VMEM((1024, 128), F32),
    pltpu.VMEM((256, 128), F32),
    pltpu.VMEM((256, 128), F32),
    pltpu.VMEM((32, 128), F32),
]


def margin_of(mine, vec, nb):
    vm = pl.BlockSpec(memory_space=pltpu.VMEM)
    dma = pltpu.SemaphoreType.DMA
    return pl.pallas_call(
        functools.partial(margin_kernel, nb),
        out_shape=jax.ShapeDtypeStruct((4, 32), F32),
        in_specs=[vm, vm],
        out_specs=vm,
        scratch_shapes=MARGIN_SCRATCH + [dma] * 6 + [dma((3,)), dma((3,))],
        compiler_params=pltpu.CompilerParams(collective_id=3, has_side_effects=True),
    )(mine, vec)


N_GRID = 4


def own_pairs(g):
    table = np.array(
        [
            [(0, 0, 1, 0), (1, 1, 1, 0), (0, 1, 1, 1), (0, 0, 0, 0)],
            [(2, 2, 1, 0), (0, 2, 1, 1), (0, 0, 0, 0), (0, 0, 0, 0)],
            [(3, 3, 1, 0), (2, 3, 1, 1), (1, 3, 1, 1), (0, 0, 0, 0)],
            [(0, 3, 1, 1), (1, 2, 1, 1), (0, 0, 0, 0), (0, 0, 0, 0)],
        ],
        np.int32,
    )
    cross = np.array([(i, 4, 1, 1) for i in range(4)], np.int32)
    return jnp.concatenate([cross, lax.dynamic_index_in_dim(jnp.asarray(table), g, 0, False)], axis=0)


def on_device(orbitals):
    g = lax.axis_index("grid")
    nb = lax.axis_size("band")
    mine = orbitals.reshape(4, 216, 128).transpose(1, 0, 2).reshape(864, 128)
    own = lax.all_gather(mine, "grid", axis=0, tiled=True)
    send = lax.dynamic_index_in_dim(own.reshape(864, 4, 128), g, 1, False)
    up = [(b * 4 + k, (b + 1) % nb * 4 + (k + 2) % 4) for b in range(nb) for k in range(4)]
    down = [(t, s) for s, t in up]
    low = lax.ppermute(send, ("band", "grid"), up)
    u, o = solve(own_pairs(g), own, low)
    owed = lax.ppermute(o, ("band", "grid"), down)
    mark = (jnp.arange(4) == g).astype(F32)
    total = u.reshape(864, 4, 128) + owed[:, None, :] * mark[None, :, None]
    parts = lax.all_to_all(total.reshape(4, 864, 128), "grid", 0, 0, tiled=True)
    vec = jnp.sum(parts, axis=0)
    vectors = vec.reshape(216, 4, 128).transpose(1, 0, 2).reshape(4, 27648)
    margin = margin_of(mine, vec, nb).T
    return vectors, margin


def solution(mesh):
    return jax.shard_map(
        on_device,
        mesh=mesh,
        in_specs=(P("band", "grid"),),
        out_specs=(P("band", "grid"), P("grid", "band")),
        check_vma=False,
    )
```

```python
import functools
import numpy as np
import jax
import jax.numpy as jnp
from jax import lax
from jax.experimental import pallas as pl
from jax.experimental.pallas import tpu as pltpu
from jax.sharding import PartitionSpec as P

NG = 48
NCELL = 110592
BF = jnp.bfloat16
F32 = jnp.float32


def split_np(a):
    hi = a.astype(BF)
    lo = (a - hi.astype(np.float64)).astype(BF)
    return hi, lo


def tables():
    n = np.arange(NG)
    ang = 2.0 * np.pi * ((n[:, None] * n[None, :]) % NG) / NG
    h = np.cos(ang) + np.sin(ang)
    w = np.zeros((8, NG, 6, 8, 8))
    for y in range(8):
        w[y, :, :, y, :] = h.reshape(NG, 6, 8)
    w = w.reshape(384, 384)
    v = np.kron(h, np.eye(8))
    f = ((n + 24) % 48 - 24).astype(np.float64)
    q = f[:, None, None] ** 2 + f[None, :, None] ** 2 + f[None, None, :] ** 2
    k = np.where(q > 0, 40.0 * (1.0 - np.exp(-q / 16.0)) / np.where(q > 0, q, 1.0), 0.0) / NCELL
    k = k.reshape(NG, NG, 6, 8).transpose(2, 0, 1, 3).reshape(288, 384)

    def pack(m):
        hi, lo = split_np(m)
        return np.concatenate([hi, hi, lo], axis=0)

    hh, hl = split_np(h)
    hx = np.concatenate([hh, hh, hl], axis=1)
    return pack(w), pack(v), pack(w.T.copy()), hx, k.astype(np.float32)


def hilo(x):
    hi = x.astype(BF)
    lo = (x - hi.astype(F32)).astype(BF)
    return hi, lo


def put(s_ref, row, rows, lane, x):
    hi, lo = hilo(x)
    n = x.shape[1]
    s_ref[row : row + rows, lane : lane + n] = hi
    s_ref[row : row + rows, 384 + lane : 384 + lane + n] = lo


def mm3(s_ref, w_ref):
    return jnp.dot(s_ref[...], w_ref[0:768, :], preferred_element_type=F32) + jnp.dot(
        s_ref[:, 0:384], w_ref[768:1152, :], preferred_element_type=F32
    )


def swap(t_ref, s_ref, pb, left):
    for p in range(pb):
        for j in range(3):
            for m in range(3):
                r0 = p * 288 + 2 * j * 48
                e = t_ref[r0 : r0 + 48, 128 * m : 128 * m + 128]
                o = t_ref[r0 + 48 : r0 + 96, 128 * m : 128 * m + 128]
                d0 = p * 288 + 2 * m * 48
                put(s_ref, d0, 48, 128 * j, jnp.where(left, e, pltpu.roll(o, 64, 1)))
                put(s_ref, d0 + 48, 48, 128 * j, jnp.where(left, pltpu.roll(e, 64, 1), o))


def potential(pb, s_ref, t_ref, r_ref, w_ref, v_ref, wt_ref, hx_ref, k_ref):
    left = lax.broadcasted_iota(jnp.int32, (48, 128), 1) < 64
    t_ref[...] = mm3(s_ref, w_ref)
    swap(t_ref, s_ref, pb, left)
    t_ref[...] = mm3(s_ref, v_ref)
    h2 = hx_ref[:, 0:96]
    h1 = hx_ref[:, 96:144]

    def xdot(row):
        return jnp.dot(h2, r_ref[row : row + 96, :], preferred_element_type=F32) + jnp.dot(
            h1, r_ref[row : row + 48, :], preferred_element_type=F32
        )

    for i in range(pb * 6):
        hi, lo = hilo(t_ref[i * 48 : i * 48 + 48, :])
        r_ref[i * 192 : i * 192 + 48, :] = hi
        r_ref[i * 192 + 48 : i * 192 + 96, :] = lo
        z = i % 6
        d = xdot(i * 192) * k_ref[z * 48 : z * 48 + 48, :]
        hi, lo = hilo(d)
        r_ref[i * 192 + 96 : i * 192 + 144, :] = hi
        r_ref[i * 192 + 144 : i * 192 + 192, :] = lo
        put(s_ref, i * 48, 48, 0, xdot(i * 192 + 96))
    t_ref[...] = mm3(s_ref, v_ref)
    swap(t_ref, s_ref, pb, left)
    t_ref[...] = mm3(s_ref, wt_ref)


MESH = pl.DeviceIdType.MESH
GROUPS = 27
HIGHEST = lax.Precision.HIGHEST
QR = 864
PARTS = 3
PR = QR // PARTS


def rcopy(src, dst, send, recv, band, grid):
    return pltpu.make_async_remote_copy(
        src_ref=src, dst_ref=dst, send_sem=send, recv_sem=recv, device_id={"band": band, "grid": grid}, device_id_type=MESH
    )


def landed(ref, sem):
    pltpu.make_async_copy(ref, ref, sem).wait()


def greet(nb, me, g):
    barrier = pltpu.get_barrier_semaphore()

    def signal(band, grid):
        pl.semaphore_signal(barrier, inc=1, device_id={"band": band, "grid": grid}, device_id_type=MESH)

    def one(o, c):
        signal((me + o) % nb, g)
        return c

    signal((me + 1) % nb, (g + 2) % 4)
    signal((me + nb - 1) % nb, (g + 2) % 4)
    for o in range(1, 4):
        signal(me, (g + o) % 4)
    lax.fori_loop(1, nb, one, 0)
    pl.semaphore_wait(barrier, nb + 4)


def span(start, size):
    return pl.ds(pl.multiple_of(start, 8), size)


def scatter_groups(src, buf, send, recv, nb, me, g):
    def one(o, c):
        dst = (me + o) % nb

        @pl.when(dst < GROUPS)
        def _():
            rcopy(src.at[span(dst * 32, 32)], buf.at[span(me * 32, 32)], send, recv, dst, g).start()

        return c

    lax.fori_loop(1, nb, one, 0)

    @pl.when(me < GROUPS)
    def _():
        buf[span(me * 32, 32), :] = src[span(me * 32, 32), :]


def sent_all(ref, sem, me, unit):
    @pl.when(me < GROUPS)
    def _():
        landed(ref.at[0 : (GROUPS - 1) * unit], sem)

    @pl.when(me >= GROUPS)
    def _():
        landed(ref.at[0 : GROUPS * unit], sem)


def margin_tail(nb, me, g, out_ref, obuf, vbuf, amat, bmat, mt8, red, gsum, rs, rr, gs, gr):
    @pl.when(me < GROUPS)
    def _():
        for c in range(8):
            for b in range(4):
                rows = pl.ds(c * 4 + b, 32, stride=32)
                amat[c * 128 + b * 32 : c * 128 + b * 32 + 32, :] = vbuf[rows, :]
                bmat[pl.ds(c * 128 + b, 32, stride=4), :] = obuf[rows, :]
        m = jnp.zeros((128, 128), F32)
        for c in range(8):
            part = slice(c * 128, c * 128 + 128)
            m = m + lax.dot_general(
                amat[part, :], bmat[part, :], (((1,), (1,)), ((), ())), precision=HIGHEST, preferred_element_type=F32
            )
        m = m * (1.0 / NCELL)
        mt8[...] = jnp.zeros_like(mt8)
        for b in range(4):
            mt8[pl.ds(b, 32, stride=8), :] = m[b * 32 : b * 32 + 32, :]

        def one(o, c):
            dst = (me + o) % nb
            rcopy(mt8.at[span(dst * 8, 8)], red.at[span(me * 8, 8)], rs, rr, dst, g).start()
            return c

        lax.fori_loop(1, nb, one, 0)
        red[span(me * 8, 8), :] = mt8[span(me * 8, 8), :]

    sent_all(red, rr, me, 8)
    total = red[0:8, :]
    for s in range(1, GROUPS):
        total = total + red[s * 8 : s * 8 + 8, :]
    mine = span(g * 8, 8)
    gsum[mine, :] = total
    sends = [rcopy(gsum.at[mine], gsum.at[mine], gs.at[o - 1], gr.at[o - 1], me, (g + o) % 4) for o in range(1, 4)]
    for s in sends:
        s.start()
    for s in sends:
        s.wait()
    full = gsum[0:8, :] + gsum[8:16, :] + gsum[16:24, :] + gsum[24:32, :]
    picked = jnp.zeros((4, 32), F32)
    for t in range(4):
        picked = picked + jnp.where(g == t, 1.0, 0.0) * full[0:4, t * 32 : t * 32 + 32]
    out_ref[...] = picked

    @pl.when(me < GROUPS)
    def _():
        landed(mt8.at[0 : 31 * 8], rs)


OWN_I = ((0, 1, 0), (2, 0, 0), (3, 2, 1), (0, 1, 0))
OWN_J = ((0, 1, 1), (2, 2, 0), (3, 3, 3), (3, 2, 0))
OWN_N = (3, 2, 3, 2)


def chosen(g, values):
    total = 0
    for t, value in enumerate(values):
        total = total + jnp.where(g == t, value, 0)
    return total


def whole_kernel(
    nb,
    mine,
    w_hbm,
    v_hbm,
    wt_hbm,
    hx_hbm,
    k_hbm,
    vec_out,
    m_out,
    w_ref,
    v_ref,
    wt_ref,
    hx_ref,
    k_ref,
    own,
    low,
    a_ref,
    u_ref,
    s_ref,
    t_ref,
    r_ref,
    un,
    on,
    ow,
    sb,
    xr,
    obuf,
    vbuf,
    amat,
    bmat,
    mt8,
    red,
    gsum,
    tab,
    sib_s,
    sib_r,
    cross_s,
    cross_r,
    fwd_s,
    fwd_r,
    low_s,
    low_r,
    ow_s,
    ow_r,
    sb_s,
    sb_r,
    xr_s,
    xr_r,
    os,
    orr,
    vs,
    vr,
    rs,
    rr,
    gs,
    gr,
):
    me, g = lax.axis_index("band"), lax.axis_index("grid")
    c, s = (g + 2) % 4, g + 1 - 2 * (g % 2)
    cs = (s + 2) % 4
    up, down = (me + 1) % nb, (me + nb - 1) % nb
    loads = [
        pltpu.make_async_copy(a, b, tab.at[n])
        for n, (a, b) in enumerate(
            ((w_hbm, w_ref), (v_hbm, v_ref), (wt_hbm, wt_ref), (hx_hbm, hx_ref), (k_hbm, k_ref))
        )
    ]
    for copy in loads:
        copy.start()
    greet(nb, me, g)

    own3, mine3 = own.reshape(864, 4, 128), mine.reshape(216, 4, 128)

    cross = [
        rcopy(mine.at[span(n * PR, PR)], own.at[span(g * QR + n * PR, PR)], cross_s.at[n], cross_r.at[n], me, c)
        for n in range(PARTS)
    ]
    for copy in cross:
        copy.start()
    sib = rcopy(mine, own.at[span(g * QR, QR)], sib_s, sib_r, me, s)
    sib.start()
    rcopy(mine3.at[:, g, :], low.at[span(g * 216, 216)], low_s, low_r, up, c).start()
    own[span(g * QR, QR), :] = mine[...]

    def low_part(start, size):
        rcopy(own3.at[pl.ds(start, size), g, :], low.at[span(start, size)], low_s, low_r, up, c).start()

    landed(own.at[span(s * QR, QR)], sib_r)
    low_part(s * 216, 216)
    scatter_groups(mine, obuf, os, orr, nb, me, g)
    fwd = []
    for n in range(PARTS):
        part = own.at[span(c * QR + n * PR, PR)]
        landed(part, cross_r.at[n])
        copy = rcopy(part, part, fwd_s.at[n], fwd_r.at[n], me, s)
        copy.start()
        fwd.append(copy)
        low_part(c * 216 + n * 72, 72)
    for n in range(PARTS):
        landed(own.at[span(cs * QR + n * PR, PR)], fwd_r.at[n])
        low_part(cs * 216 + n * 72, 72)

    for r in range(18):
        for xg in range(6):
            row, lane = (r // 3) * 48 + xg * 8, (r % 3) * 128
            for b in range(4):
                a_ref[b, row : row + 8, lane : lane + 128] = own[pl.ds((xg * 144 + r) * 4 + b, 8, stride=72), :]
    u_ref[...] = jnp.zeros_like(u_ref)
    for copy in loads:
        copy.wait()

    def pair(i, j, other):
        put(s_ref, 0, 288, 0, a_ref[i] * a_ref[j])
        potential(1, s_ref, t_ref, r_ref, w_ref, v_ref, wt_ref, hx_ref, k_ref)
        t = t_ref[...]
        u_ref[i] = u_ref[i] - a_ref[j] * t
        u_ref[j] = u_ref[j] - other * a_ref[i] * t

    def own_pair(n, carry):
        i = chosen(g, [row[0] for row in OWN_I])
        j = chosen(g, [row[0] for row in OWN_J])
        for slot in (1, 2):
            i = jnp.where(n == slot, chosen(g, [row[slot] for row in OWN_I]), i)
            j = jnp.where(n == slot, chosen(g, [row[slot] for row in OWN_J]), j)
        pair(i, j, jnp.where(i == j, 0.0, 1.0))
        return carry

    def cross_pair(n, carry):
        pair(n, 4, 1.0)
        return carry

    lax.fori_loop(0, 1, own_pair, 0)
    landed(low, low_r)
    for r in range(18):
        for xg in range(6):
            row, lane = (r // 3) * 48 + xg * 8, (r % 3) * 128
            a_ref[4, row : row + 8, lane : lane + 128] = low[pl.ds(xg * 144 + r, 8, stride=18), :]
    lax.fori_loop(0, 4, cross_pair, 0)

    for r in range(18):
        for xg in range(6):
            row, lane = (r // 3) * 48 + xg * 8, (r % 3) * 128
            on[pl.ds(xg * 144 + r, 8, stride=18), :] = u_ref[4, row : row + 8, lane : lane + 128]
    back = []
    for n, q in enumerate((s, g, cs, c)):
        part = span(q * 216, 216)
        copy = rcopy(on.at[part], ow.at[part], ow_s.at[n], ow_r.at[n], down, c)
        copy.start()
        back.append(copy)
    lax.fori_loop(1, chosen(g, OWN_N), own_pair, 0)

    for r in range(18):
        for xg in range(6):
            row, lane = (r // 3) * 48 + xg * 8, (r % 3) * 128
            for b in range(4):
                un[pl.ds((xg * 144 + r) * 4 + b, 8, stride=72), :] = u_ref[b, row : row + 8, lane : lane + 128]

    def add_owed(n, q):
        landed(ow.at[span(q * 216, 216)], ow_r.at[n])

        def rows(t, carry):
            to = pl.ds(q * QR + t * 32 + g, 8, stride=4)
            un[to, :] = un[to, :] + ow[span(q * 216 + t * 8, 8), :]
            return carry

        lax.fori_loop(0, 27, rows, 0)

    add_owed(0, cs)
    pass_on = [rcopy(un.at[span(q * QR, QR)], sb.at[n], sb_s.at[n], sb_r.at[n], me, s) for n, q in enumerate((cs, s))]
    pass_on[0].start()
    add_owed(1, c)
    landed(sb.at[0], sb_r.at[0])
    away = []
    for n in range(PARTS):
        part = span(c * QR + n * PR, PR)
        un[part, :] = un[part, :] + sb[0, n * PR : n * PR + PR, :]
        copy = rcopy(un.at[part], xr.at[span(n * PR, PR)], xr_s.at[n], xr_r.at[n], me, c)
        copy.start()
        away.append(copy)
    add_owed(2, s)
    pass_on[1].start()
    add_owed(3, g)
    landed(sb.at[1], sb_r.at[1])
    for n in range(PARTS):
        part = slice(n * PR, n * PR + PR)
        landed(xr.at[part], xr_r.at[n])
        vec_out[part, :] = un[span(g * QR + n * PR, PR), :] + sb[1, part, :] + xr[part, :]

    scatter_groups(vec_out, vbuf, vs, vr, nb, me, g)

    @pl.when(me < GROUPS)
    def _():
        landed(obuf.at[0 : 31 * 32], orr)
        landed(vbuf.at[0 : 31 * 32], vr)

    margin_tail(nb, me, g, m_out, obuf, vbuf, amat, bmat, mt8, red, gsum, rs, rr, gs, gr)
    sent_all(obuf, os, me, 32)
    sent_all(vbuf, vs, me, 32)
    for copy in cross + fwd + [sib] + back + pass_on + away:
        copy.wait_send()
    landed(on, low_s)


def on_device(orbitals):
    nb = lax.axis_size("band")
    mine = orbitals.reshape(4, 216, 128).transpose(1, 0, 2).reshape(864, 128)
    vm = pl.BlockSpec(memory_space=pltpu.VMEM)
    hbm = pl.BlockSpec(memory_space=pl.ANY)
    dma = pltpu.SemaphoreType.DMA
    w, v, wt, hx, k = tables()

    def f32(*shape):
        return pltpu.VMEM(shape, F32)

    def b16(*shape):
        return pltpu.VMEM(shape, BF)

    vec, margin = pl.pallas_call(
        functools.partial(whole_kernel, nb),
        out_shape=(jax.ShapeDtypeStruct((864, 128), F32), jax.ShapeDtypeStruct((4, 32), F32)),
        in_specs=[vm] + [hbm] * 5,
        out_specs=(vm, vm),
        scratch_shapes=[b16(1152, 384), b16(1152, 384), b16(1152, 384), b16(48, 144), f32(288, 384)]
        + [f32(3456, 128), f32(864, 128), f32(5, 288, 384), f32(5, 288, 384)]
        + [b16(288, 768), f32(288, 384), b16(1152, 384)]
        + [f32(3456, 128), f32(864, 128), f32(864, 128), f32(2, 864, 128), f32(864, 128)]
        + [f32(1024, 128), f32(1024, 128), f32(1024, 128), f32(1024, 128), f32(256, 128), f32(256, 128), f32(32, 128)]
        + [dma((5,)), dma, dma, dma((3,)), dma((3,)), dma((3,)), dma((3,)), dma, dma]
        + [dma((4,)), dma((4,)), dma((2,)), dma((2,)), dma((3,)), dma((3,))]
        + [dma] * 6
        + [dma((3,)), dma((3,))],
        compiler_params=pltpu.CompilerParams(
            collective_id=3, has_side_effects=True, vmem_limit_bytes=60 * 1024 * 1024
        ),
    )(mine, w, v, wt, hx, k)
    return vec.reshape(216, 4, 128).transpose(1, 0, 2).reshape(4, 27648), margin.T


def solution(mesh):
    return jax.shard_map(
        on_device,
        mesh=mesh,
        in_specs=(P("band", "grid"),),
        out_specs=(P("band", "grid"), P("grid", "band")),
        check_vma=False,
    )
```

```python
import functools
import numpy as np
import jax
import jax.numpy as jnp
from jax import lax
from jax.experimental import pallas as pl
from jax.experimental.pallas import tpu as pltpu
from jax.sharding import PartitionSpec as P

NG = 48
NCELL = 110592
BF = jnp.bfloat16
F32 = jnp.float32


def split_np(a):
    hi = a.astype(BF)
    lo = (a - hi.astype(np.float64)).astype(BF)
    return hi, lo


def tables():
    n = np.arange(NG)
    ang = 2.0 * np.pi * ((n[:, None] * n[None, :]) % NG) / NG
    h = np.cos(ang) + np.sin(ang)
    w = np.zeros((8, NG, 6, 8, 8))
    for y in range(8):
        w[y, :, :, y, :] = h.reshape(NG, 6, 8)
    w = w.reshape(384, 384)
    v = np.kron(h, np.eye(8))
    f = ((n + 24) % 48 - 24).astype(np.float64)
    q = f[:, None, None] ** 2 + f[None, :, None] ** 2 + f[None, None, :] ** 2
    k = np.where(q > 0, 40.0 * (1.0 - np.exp(-q / 16.0)) / np.where(q > 0, q, 1.0), 0.0) / NCELL
    k = k.reshape(NG, NG, 6, 8).transpose(2, 0, 1, 3).reshape(288, 384)

    def pack(m):
        hi, lo = split_np(m)
        return np.concatenate([hi, lo], axis=0)

    hh, hl = split_np(h)
    hx = np.concatenate([hh, hh, hl], axis=1)
    return pack(w), pack(v), pack(w.T.copy()), hx, k.astype(np.float32)


def hilo(x):
    hi = x.astype(BF)
    lo = (x - hi.astype(F32)).astype(BF)
    return hi, lo


def put(s_ref, row, rows, lane, x):
    hi, lo = hilo(x)
    n = x.shape[1]
    s_ref[row : row + rows, lane : lane + n] = hi
    s_ref[row : row + rows, 384 + lane : 384 + lane + n] = lo


def mm3(s_ref, w_ref):
    return jnp.dot(s_ref[...], w_ref[0:768, :], preferred_element_type=F32) + jnp.dot(
        s_ref[:, 0:384], w_ref[768:1152, :], preferred_element_type=F32
    )


def swap(t_ref, s_ref, pb, left):
    for p in range(pb):
        for j in range(3):
            for m in range(3):
                r0 = p * 288 + 2 * j * 48
                e = t_ref[r0 : r0 + 48, 128 * m : 128 * m + 128]
                o = t_ref[r0 + 48 : r0 + 96, 128 * m : 128 * m + 128]
                d0 = p * 288 + 2 * m * 48
                put(s_ref, d0, 48, 128 * j, jnp.where(left, e, pltpu.roll(o, 64, 1)))
                put(s_ref, d0 + 48, 48, 128 * j, jnp.where(left, pltpu.roll(e, 64, 1), o))


def potential(pb, s_ref, t_ref, r_ref, w_ref, v_ref, wt_ref, hx_ref, k_ref):
    left = lax.broadcasted_iota(jnp.int32, (48, 128), 1) < 64
    t_ref[...] = mm3(s_ref, w_ref)
    swap(t_ref, s_ref, pb, left)
    t_ref[...] = mm3(s_ref, v_ref)
    h2 = hx_ref[:, 0:96]
    h1 = hx_ref[:, 96:144]

    def xdot(row):
        return jnp.dot(h2, r_ref[row : row + 96, :], preferred_element_type=F32) + jnp.dot(
            h1, r_ref[row : row + 48, :], preferred_element_type=F32
        )

    for i in range(pb * 6):
        hi, lo = hilo(t_ref[i * 48 : i * 48 + 48, :])
        r_ref[i * 192 : i * 192 + 48, :] = hi
        r_ref[i * 192 + 48 : i * 192 + 96, :] = lo
        z = i % 6
        d = xdot(i * 192) * k_ref[z * 48 : z * 48 + 48, :]
        hi, lo = hilo(d)
        r_ref[i * 192 + 96 : i * 192 + 144, :] = hi
        r_ref[i * 192 + 144 : i * 192 + 192, :] = lo
        put(s_ref, i * 48, 48, 0, xdot(i * 192 + 96))
    t_ref[...] = mm3(s_ref, v_ref)
    swap(t_ref, s_ref, pb, left)
    t_ref[...] = mm3(s_ref, wt_ref)


MESH = pl.DeviceIdType.MESH
GROUPS = 27
HIGHEST = lax.Precision.HIGHEST


def rcopy(src, dst, send, recv, band, grid):
    return pltpu.make_async_remote_copy(
        src_ref=src, dst_ref=dst, send_sem=send, recv_sem=recv, device_id={"band": band, "grid": grid}, device_id_type=MESH
    )


def landed(ref, sem):
    pltpu.make_async_copy(ref, ref, sem).wait()


def greet(nb, me, g):
    barrier = pltpu.get_barrier_semaphore()

    def signal(band, grid):
        pl.semaphore_signal(barrier, inc=1, device_id={"band": band, "grid": grid}, device_id_type=MESH)

    def one(o, c):
        signal((me + o) % nb, g)
        return c

    signal((me + 1) % nb, (g + 2) % 4)
    signal((me + nb - 1) % nb, (g + 2) % 4)
    for o in range(1, 4):
        signal(me, (g + o) % 4)
    lax.fori_loop(1, nb, one, 0)
    pl.semaphore_wait(barrier, nb + 4)


def span(start, size):
    return pl.ds(pl.multiple_of(start, 8), size)


def nth(g, n):
    return (n + 2 * (g // 2)) % 4


def scatter_groups(src, buf, send, recv, nb, me, g, rows=32, at=0):
    def one(o, c):
        dst = (me + o) % nb

        @pl.when(dst < GROUPS)
        def _():
            rcopy(src.at[span(dst * rows, rows)], buf.at[span(me * 32 + at, rows)], send, recv, dst, g).start()

        return c

    lax.fori_loop(1, nb, one, 0)

    @pl.when(me < GROUPS)
    def _():
        buf[span(me * 32 + at, rows), :] = src[span(me * rows, rows), :]


def sent_all(ref, sem, me, unit):
    @pl.when(me < GROUPS)
    def _():
        landed(ref.at[0 : (GROUPS - 1) * unit], sem)

    @pl.when(me >= GROUPS)
    def _():
        landed(ref.at[0 : GROUPS * unit], sem)


def margin_tail(nb, me, g, out_ref, obuf, vbuf, amat, bmat, mt8, red, gsum, rs, rr, gs, gr):
    @pl.when(me < GROUPS)
    def _():
        for c in range(8):
            for b in range(4):
                amat[c * 128 + b * 32 : c * 128 + b * 32 + 32, :] = vbuf[pl.ds(b * 8 + c, 32, stride=32), :]
                bmat[pl.ds(c * 128 + b, 32, stride=4), :] = obuf[pl.ds(c * 4 + b, 32, stride=32), :]
        m = jnp.zeros((128, 128), F32)
        for c in range(8):
            part = slice(c * 128, c * 128 + 128)
            m = m + lax.dot_general(
                amat[part, :], bmat[part, :], (((1,), (1,)), ((), ())), precision=HIGHEST, preferred_element_type=F32
            )
        m = m * (1.0 / NCELL)
        mt8[...] = jnp.zeros_like(mt8)
        for n in range(4):
            mt8[pl.ds(nth(g, n + 2), 32, stride=8), :] = m[n * 32 : n * 32 + 32, :]

        def one(o, c):
            dst = (me + o) % nb
            rcopy(mt8.at[span(dst * 8, 8)], red.at[span(me * 8, 8)], rs, rr, dst, g).start()
            return c

        lax.fori_loop(1, nb, one, 0)
        red[span(me * 8, 8), :] = mt8[span(me * 8, 8), :]

    sent_all(red, rr, me, 8)
    total = red[0:8, :]
    for s in range(1, GROUPS):
        total = total + red[s * 8 : s * 8 + 8, :]
    mine = span(g * 8, 8)
    gsum[mine, :] = total
    sends = [rcopy(gsum.at[mine], gsum.at[mine], gs.at[o - 1], gr.at[o - 1], me, (g + o) % 4) for o in range(1, 4)]
    for s in sends:
        s.start()
    for s in sends:
        s.wait()
    full = gsum[0:8, :] + gsum[8:16, :] + gsum[16:24, :] + gsum[24:32, :]
    picked = jnp.zeros((4, 32), F32)
    for t in range(4):
        picked = picked + jnp.where(g == t, 1.0, 0.0) * full[0:4, t * 32 : t * 32 + 32]
    out_ref[...] = picked

    @pl.when(me < GROUPS)
    def _():
        landed(mt8.at[0 : 31 * 8], rs)


OWN_I = ((0, 0, 1), (0, 1, 0), (2, 2, 3), (2, 3, 0))
OWN_J = ((0, 2, 1), (1, 3, 0), (2, 1, 3), (3, 0, 0))
STEPS = (7, 6, 7, 6)


def chosen(g, values):
    total = 0
    for t, value in enumerate(values):
        total = total + jnp.where(g == t, value, 0)
    return total


def whole_kernel(nb, mine, w_hbm, v_hbm, wt_hbm, hx_hbm, k_hbm, vec_out, m_out, *scratch):
    (w_ref, v_ref, wt_ref, hx_ref, k_ref, own, low, a_ref, u_ref, s_ref, t_ref, r_ref, un, on, ow, sb, xr, stage) = scratch[:18]
    (obuf, vbuf, amat, bmat, mt8, red, gsum, tab, sib_s, sib_r, cross_s, cross_r, fwd_s, fwd_r) = scratch[18:32]
    (low_s, low_r, ow_s, ow_r, sb_s, sb_r, xr_s, xr_r, os, orr, vs, vr, vs2, vr2, rs, rr, gs, gr) = scratch[32:]
    me, g = lax.axis_index("band"), lax.axis_index("grid")
    c, s = (g + 2) % 4, g + 1 - 2 * (g % 2)
    cs = (s + 2) % 4
    up, down = (me + 1) % nb, (me + nb - 1) % nb
    loads = []
    for n, (a, b) in enumerate(((w_hbm, w_ref), (v_hbm, v_ref), (wt_hbm, wt_ref))):
        loads.append(pltpu.make_async_copy(a.at[0:384], b.at[0:384], tab.at[2 * n]))
        loads.append(pltpu.make_async_copy(a, b.at[384:1152], tab.at[2 * n + 1]))
    loads.append(pltpu.make_async_copy(hx_hbm, hx_ref, tab.at[6]))
    loads.append(pltpu.make_async_copy(k_hbm, k_ref, tab.at[7]))
    for copy in loads:
        copy.start()
    greet(nb, me, g)

    mine3 = mine.reshape(216, 4, 128)

    def cells(ref, b, q):
        return ref.at[span(b * 864 + q * 216, 216)]

    cross = []
    for n in range(4):
        b = nth(c, n)
        cross.append(rcopy(mine3.at[:, b, :], cells(own, b, g), cross_s.at[n], cross_r.at[n], me, c))
        cross[n].start()
    sib = []
    for b in range(4):
        sib.append(rcopy(mine3.at[:, b, :], cells(own, b, g), sib_s.at[b], sib_r.at[b], me, s))
        sib[b].start()
    rcopy(mine3.at[:, g, :], low.at[span(g * 216, 216)], low_s, low_r, up, c).start()

    def spread(t, carry):
        for b in range(4):
            own[span(b * 864 + g * 216 + t * 8, 8), :] = mine[pl.ds(t * 32 + b, 8, stride=4), :]
        return carry

    lax.fori_loop(0, 27, spread, 0)

    def low_part(q):
        rcopy(cells(own, g, q), low.at[span(q * 216, 216)], low_s, low_r, up, c).start()

    for b in range(4):
        landed(cells(own, b, s), sib_r.at[b])
    low_part(s)
    fwd = [
        rcopy(cells(own, nth(g, n), c), cells(own, nth(g, n), c), fwd_s.at[n], fwd_r.at[n], me, s) for n in range(4)
    ]

    def crossed(n):
        landed(cells(own, nth(g, n), c), cross_r.at[n])
        fwd[n].start()

    def forwarded(n):
        landed(cells(own, nth(g, n), cs), fwd_r.at[n])

    def spread_low(n):
        @pl.when(g % 2 == n)
        def _():
            low_part(c)

    def spread_low2(n):
        @pl.when(g % 2 == n)
        def _():
            low_part(cs)

    for n in range(2):
        crossed(n)
        spread_low(n)
    for n in range(2):
        forwarded(n)
        spread_low2(n)
    u_ref[...] = jnp.zeros_like(u_ref)
    for copy in loads:
        copy.wait()

    def lay(slot, src, base):
        for r in range(18):
            for xg in range(6):
                row, lane = (r // 3) * 48 + xg * 8, (r % 3) * 128
                a_ref[slot, row : row + 8, lane : lane + 128] = src[pl.ds(base + xg * 144 + r, 8, stride=18), :]

    def unlay(slot, dst, base):
        for r in range(18):
            for xg in range(6):
                row, lane = (r // 3) * 48 + xg * 8, (r % 3) * 128
                dst[pl.ds(base + xg * 144 + r, 8, stride=18), :] = u_ref[slot, row : row + 8, lane : lane + 128]

    def lay_band(n):
        b = nth(g, n)
        lay(b, own, b * 864)

    def unlay_band(n):
        b = nth(g, n)
        unlay(b, un, b * 864)

    lay_band(0)
    lay_band(1)

    back = [
        rcopy(on.at[span(q * 216, 216)], ow.at[span(q * 216, 216)], ow_s.at[n], ow_r.at[n], down, c)
        for n, q in enumerate((s, g, cs, c))
    ]
    pass_on = []
    for n in range(4):
        for h, q in enumerate((cs, s)):
            at = n * 2 + h
            pass_on.append(
                rcopy(cells(un, nth(g, n), q), sb.at[at * 216 : at * 216 + 216], sb_s.at[at], sb_r.at[at], me, s)
            )
    away = [
        rcopy(cells(un, nth(g, n), c), xr.at[(n ^ 2) * 216 : (n ^ 2) * 216 + 216], xr_s.at[n], xr_r.at[n ^ 2], me, c)
        for n in range(4)
    ]

    def send_away(n):
        at = n * 2
        landed(sb.at[at * 216 : at * 216 + 216], sb_r.at[at])
        part = span(nth(g, n) * 864 + c * 216, 216)
        un[part, :] = un[part, :] + sb[at * 216 : at * 216 + 216, :]
        away[n].start()

    def step(n, carry):
        @pl.when(n == 1)
        def _():
            crossed(2)
            landed(low, low_r)
            lay(4, low, 0)
            scatter_groups(mine, obuf, os, orr, nb, me, g)

        @pl.when(n == 2)
        def _():
            crossed(3)

        @pl.when(n == 3)
        def _():
            forwarded(2)
            forwarded(3)
            lay_band(2)
            lay_band(3)

        @pl.when(n == 6)
        def _():
            early()

        i, j, other = 0, 4, 1.0
        for at, slot in ((0, 0), (3, 1), (6, 2)):
            i = jnp.where(n == at, chosen(g, [row[slot] for row in OWN_I]), i)
            j = jnp.where(n == at, chosen(g, [row[slot] for row in OWN_J]), j)
        for at, k in ((1, 0), (2, 1), (4, 2), (5, 3)):
            i = jnp.where(n == at, nth(g, k), i)
        other = jnp.where(i == j, 0.0, 1.0)
        put(s_ref, 0, 288, 0, a_ref[i] * a_ref[j])
        potential(1, s_ref, t_ref, r_ref, w_ref, v_ref, wt_ref, hx_ref, k_ref)
        t = t_ref[...]
        u_ref[i] = u_ref[i] - a_ref[j] * t
        u_ref[j] = u_ref[j] - other * a_ref[i] * t
        return carry

    def early():
        unlay(4, on, 0)
        for copy in back:
            copy.start()
        for n in (2, 3):
            unlay_band(n)
            pass_on[2 * n].start()
            pass_on[2 * n + 1].start()
        send_away(2)
        send_away(3)

    lax.fori_loop(0, 6, step, 0)

    @pl.when(g % 2 == 1)
    def _():
        early()

    lax.fori_loop(6, chosen(g, STEPS), step, 0)

    for n in (0, 1):
        unlay_band(n)

    def add_owed(n, q):
        landed(ow.at[span(q * 216, 216)], ow_r.at[n])
        part = span(g * 864 + q * 216, 216)
        un[part, :] = un[part, :] + ow[span(q * 216, 216), :]

    def finish(n, at, rows):
        b = nth(g, n)
        landed(sb.at[(n * 2 + 1) * 216 : (n * 2 + 2) * 216], sb_r.at[n * 2 + 1])
        landed(xr.at[n * 216 : n * 216 + 216], xr_r.at[n])

        def group(t, carry):
            value = (
                un[span(b * 864 + g * 216 + t * 8, 8), :]
                + sb[span((n * 2 + 1) * 216 + t * 8, 8), :]
                + xr[span(n * 216 + t * 8, 8), :]
            )
            vec_out[pl.ds(t * 32 + b, 8, stride=4), :] = value
            stage[span(rows + t * 16 + at * 8, 8), :] = value
            return carry

        lax.fori_loop(0, 27, group, 0)

    add_owed(0, cs)
    pass_on[0].start()
    pass_on[2].start()
    add_owed(1, c)
    send_away(0)
    send_away(1)
    add_owed(2, s)
    pass_on[1].start()
    pass_on[3].start()
    finish(2, 0, 0)
    finish(3, 1, 0)
    scatter_groups(stage.at[0:432], vbuf, vs, vr, nb, me, g, 16, 0)
    add_owed(3, g)
    finish(0, 0, 432)
    finish(1, 1, 432)
    scatter_groups(stage.at[432:864], vbuf, vs2, vr2, nb, me, g, 16, 16)

    @pl.when(me < GROUPS)
    def _():
        landed(obuf.at[0 : 31 * 32], orr)
        landed(vbuf.at[0 : 31 * 16], vr)
        landed(vbuf.at[0 : 31 * 16], vr2)

    margin_tail(nb, me, g, m_out, obuf, vbuf, amat, bmat, mt8, red, gsum, rs, rr, gs, gr)
    sent_all(obuf, os, me, 32)
    sent_all(obuf, vs, me, 16)
    sent_all(obuf, vs2, me, 16)
    for copy in cross + fwd + sib + back + pass_on + away:
        copy.wait_send()
    landed(on, low_s)


def on_device(orbitals):
    nb = lax.axis_size("band")
    mine = orbitals.reshape(4, 216, 128).transpose(1, 0, 2).reshape(864, 128)
    vm = pl.BlockSpec(memory_space=pltpu.VMEM)
    hbm = pl.BlockSpec(memory_space=pl.ANY)
    dma = pltpu.SemaphoreType.DMA
    w, v, wt, hx, k = tables()

    def f32(*shape):
        return pltpu.VMEM(shape, F32)

    def b16(*shape):
        return pltpu.VMEM(shape, BF)

    vec, margin = pl.pallas_call(
        functools.partial(whole_kernel, nb),
        out_shape=(jax.ShapeDtypeStruct((864, 128), F32), jax.ShapeDtypeStruct((4, 32), F32)),
        in_specs=[vm] + [hbm] * 5,
        out_specs=(vm, vm),
        scratch_shapes=[b16(1152, 384), b16(1152, 384), b16(1152, 384), b16(48, 144), f32(288, 384)]
        + [f32(3456, 128), f32(864, 128), f32(5, 288, 384), f32(5, 288, 384)]
        + [b16(288, 768), f32(288, 384), b16(1152, 384)]
        + [f32(3456, 128), f32(864, 128), f32(864, 128), f32(1728, 128), f32(864, 128), f32(864, 128)]
        + [f32(1024, 128), f32(1024, 128), f32(1024, 128), f32(1024, 128), f32(256, 128), f32(256, 128), f32(32, 128)]
        + [dma((8,)), dma((4,)), dma((4,)), dma((4,)), dma((4,)), dma((4,)), dma((4,)), dma, dma]
        + [dma((4,)), dma((4,)), dma((8,)), dma((8,)), dma((4,)), dma((4,))]
        + [dma] * 8
        + [dma((3,)), dma((3,))],
        compiler_params=pltpu.CompilerParams(
            collective_id=3, has_side_effects=True, vmem_limit_bytes=60 * 1024 * 1024
        ),
    )(mine, w, v, wt, hx, k)
    return vec.reshape(216, 4, 128).transpose(1, 0, 2).reshape(4, 27648), margin.T


def solution(mesh):
    return jax.shard_map(
        on_device,
        mesh=mesh,
        in_specs=(P("band", "grid"),),
        out_specs=(P("band", "grid"), P("grid", "band")),
        check_vma=False,
    )
```

```python
import functools
import numpy as np
import jax
import jax.numpy as jnp
from jax import lax
from jax.experimental import pallas as pl
from jax.experimental.pallas import tpu as pltpu
from jax.sharding import PartitionSpec as P

NG = 48
NCELL = 110592
BF = jnp.bfloat16
F32 = jnp.float32


def split_np(a):
    hi = a.astype(BF)
    lo = (a - hi.astype(np.float64)).astype(BF)
    return hi, lo


def tables():
    n = np.arange(NG)
    ang = 2.0 * np.pi * ((n[:, None] * n[None, :]) % NG) / NG
    h = np.cos(ang) + np.sin(ang)
    w = np.zeros((8, NG, 6, 8, 8))
    for y in range(8):
        w[y, :, :, y, :] = h.reshape(NG, 6, 8)
    w = w.reshape(384, 384)
    v = np.kron(h, np.eye(8))
    f = ((n + 24) % 48 - 24).astype(np.float64)
    q = f[:, None, None] ** 2 + f[None, :, None] ** 2 + f[None, None, :] ** 2
    k = np.where(q > 0, 40.0 * (1.0 - np.exp(-q / 16.0)) / np.where(q > 0, q, 1.0), 0.0) / NCELL
    k = k.reshape(NG, NG, 6, 8).transpose(2, 0, 1, 3).reshape(288, 384)

    def pack(m):
        hi, lo = split_np(m)
        return np.concatenate([hi, lo], axis=0)

    hh, hl = split_np(h)
    hx = np.concatenate([hh, hh, hl], axis=1)
    return pack(w), pack(v), pack(w.T.copy()), hx, k.astype(np.float32)


def hilo(x):
    hi = x.astype(BF)
    lo = (x - hi.astype(F32)).astype(BF)
    return hi, lo


def put(s_ref, row, rows, lane, x):
    hi, lo = hilo(x)
    n = x.shape[1]
    s_ref[row : row + rows, lane : lane + n] = hi
    s_ref[row : row + rows, 384 + lane : 384 + lane + n] = lo


def mm3(s_ref, w_ref):
    return jnp.dot(s_ref[...], w_ref[0:768, :], preferred_element_type=F32) + jnp.dot(
        s_ref[:, 0:384], w_ref[768:1152, :], preferred_element_type=F32
    )


def swap(t_ref, s_ref, pb, left):
    for p in range(pb):
        for j in range(3):
            for m in range(3):
                r0 = p * 288 + 2 * j * 48
                e = t_ref[r0 : r0 + 48, 128 * m : 128 * m + 128]
                o = t_ref[r0 + 48 : r0 + 96, 128 * m : 128 * m + 128]
                d0 = p * 288 + 2 * m * 48
                put(s_ref, d0, 48, 128 * j, jnp.where(left, e, pltpu.roll(o, 64, 1)))
                put(s_ref, d0 + 48, 48, 128 * j, jnp.where(left, pltpu.roll(e, 64, 1), o))


def potential(pb, s_ref, t_ref, r_ref, w_ref, v_ref, wt_ref, hx_ref, k_ref):
    left = lax.broadcasted_iota(jnp.int32, (48, 128), 1) < 64
    t_ref[...] = mm3(s_ref, w_ref)
    swap(t_ref, s_ref, pb, left)
    t_ref[...] = mm3(s_ref, v_ref)
    h2 = hx_ref[:, 0:96]
    h1 = hx_ref[:, 96:144]

    def xdot(row):
        return jnp.dot(h2, r_ref[row : row + 96, :], preferred_element_type=F32) + jnp.dot(
            h1, r_ref[row : row + 48, :], preferred_element_type=F32
        )

    for i in range(pb * 6):
        hi, lo = hilo(t_ref[i * 48 : i * 48 + 48, :])
        r_ref[i * 192 : i * 192 + 48, :] = hi
        r_ref[i * 192 + 48 : i * 192 + 96, :] = lo
        z = i % 6
        d = xdot(i * 192) * k_ref[z * 48 : z * 48 + 48, :]
        hi, lo = hilo(d)
        r_ref[i * 192 + 96 : i * 192 + 144, :] = hi
        r_ref[i * 192 + 144 : i * 192 + 192, :] = lo
        put(s_ref, i * 48, 48, 0, xdot(i * 192 + 96))
    t_ref[...] = mm3(s_ref, v_ref)
    swap(t_ref, s_ref, pb, left)
    t_ref[...] = mm3(s_ref, wt_ref)


MESH = pl.DeviceIdType.MESH


def rcopy(src, dst, send, recv, band, grid):
    return pltpu.make_async_remote_copy(
        src_ref=src, dst_ref=dst, send_sem=send, recv_sem=recv, device_id={"band": band, "grid": grid}, device_id_type=MESH
    )


def landed(ref, sem):
    pltpu.make_async_copy(ref, ref, sem).wait()


def greet(nb, me, g):
    barrier = pltpu.get_barrier_semaphore()
    plane, w = me // 8, me % 8

    def signal(band, grid):
        pl.semaphore_signal(barrier, inc=1, device_id={"band": band, "grid": grid}, device_id_type=MESH)

    def one(o, c):
        n = (w * 4 + g + o) % 32
        signal(plane * 8 + n // 4, n % 4)
        return c

    signal((me + 1) % nb, (g + 2) % 4)
    signal((me + nb - 1) % nb, (g + 2) % 4)
    lax.fori_loop(1, 32, one, 0)
    for o in range(1, 4):
        signal((me + 8 * o) % nb, g)
    pl.semaphore_wait(barrier, 36)


def span(start, size):
    return pl.ds(pl.multiple_of(start, 8), size)


def nth(g, n):
    return (n + 2 * (g // 2)) % 4


def scatter_slices(src3, buf3, base, send, recv, me, g):
    plane, w = me // 8, me % 8

    def one(o, c):
        dst = (w + o) % 8
        rcopy(
            src3.at[pl.ds(dst * 27, 27)], buf3.at[pl.ds(base + w * 27, 27)], send, recv, plane * 8 + dst, g
        ).start()
        return c

    lax.fori_loop(1, 8, one, 0)
    buf3[pl.ds(base + w * 27, 27)] = src3[pl.ds(w * 27, 27)]


def lay_orbitals(obuf, bmat):
    flat = obuf.reshape(3456, 128)

    def chunk(c, carry):
        for z in range(4):
            for b in range(4):
                bmat[pl.ds(c * 128 + z * 32 + b, 8, stride=4), :] = flat[pl.ds(z * 864 + c * 4 + b, 8, stride=108), :]
        return carry

    lax.fori_loop(0, 27, chunk, 0)


def margin_tail(me, g, out_ref, vbuf, bmat, mt8, red, rs, rr):
    plane, w = me // 8, me % 8
    flat = vbuf.reshape(864, 128)
    m = jnp.zeros((32, 128), F32)
    dims = (((1,), (1,)), ((), ()))
    for c in range(27):
        a = jnp.concatenate([flat[pl.ds(c * 4 + b, 8, stride=108), :] for b in range(4)], axis=0)
        ah, al = hilo(a)
        bh, bl = hilo(bmat[c * 128 : c * 128 + 128, :])
        m = m + (
            lax.dot_general(ah, bh, dims, preferred_element_type=F32)
            + lax.dot_general(al, bh, dims, preferred_element_type=F32)
            + lax.dot_general(ah, bl, dims, preferred_element_type=F32)
        )
    m = m * (1.0 / NCELL)
    lane = lax.broadcasted_iota(jnp.int32, (8, 128), 1) // 32
    for t in range(4):
        piece = jnp.zeros((8, 128), F32)
        for b in range(4):
            row = m[b * 8 : b * 8 + 8, :]
            turn = 32 * ((b - t) % 4)
            piece = jnp.where(lane == b, pltpu.roll(row, turn, 1) if turn else row, piece)
        mt8[pl.ds(t * 64, 8, stride=8), :] = piece
    here = (g * 8 + w) * 8

    def one(o, c):
        n = (w * 4 + g + o) % 32
        dst, to = n // 4, n % 4
        rcopy(mt8.at[span((to * 8 + dst) * 8, 8)], red.at[span(here, 8)], rs, rr, plane * 8 + dst, to).start()
        return c

    lax.fori_loop(1, 32, one, 0)
    red[span(here, 8), :] = mt8[span(here, 8), :]
    landed(red.at[0 : 31 * 8], rr)
    total = jnp.sum(red[pl.ds(0, 32, stride=8), :], axis=0, keepdims=True)
    for b in range(4):
        out_ref[b : b + 1, :] = total[:, b * 32 : b * 32 + 32]
    landed(mt8.at[0 : 31 * 8], rs)


OWN_I = ((0, 0, 1), (0, 1, 0), (2, 2, 3), (2, 3, 0))
OWN_J = ((0, 2, 1), (1, 3, 0), (2, 1, 3), (3, 0, 0))
STEPS = (7, 6, 7, 6)


def chosen(g, values):
    total = 0
    for t, value in enumerate(values):
        total = total + jnp.where(g == t, value, 0)
    return total


def whole_kernel(nb, mine, w_hbm, v_hbm, wt_hbm, hx_hbm, k_hbm, vec_out, m_out, *scratch):
    (w_ref, v_ref, wt_ref, hx_ref, k_ref, own, low, a_ref, u_ref, s_ref, t_ref, r_ref, un, on, ow, sb, xr) = scratch[:17]
    (obuf, vbuf, bmat, mt8, red, tab, sib_s, sib_r, cross_s, cross_r, fwd_s, fwd_r) = scratch[17:29]
    (low_s, low_r, ow_s, ow_r, sb_s, sb_r, xr_s, xr_r, os, orr, vs, vr, zs, zr, rs, rr) = scratch[29:]
    me, g = lax.axis_index("band"), lax.axis_index("grid")
    c, s = (g + 2) % 4, g + 1 - 2 * (g % 2)
    cs = (s + 2) % 4
    up, down = (me + 1) % nb, (me + nb - 1) % nb
    loads = []
    for n, (a, b) in enumerate(((w_hbm, w_ref), (v_hbm, v_ref), (wt_hbm, wt_ref))):
        loads.append(pltpu.make_async_copy(a.at[0:384], b.at[0:384], tab.at[2 * n]))
        loads.append(pltpu.make_async_copy(a, b.at[384:1152], tab.at[2 * n + 1]))
    loads.append(pltpu.make_async_copy(hx_hbm, hx_ref, tab.at[6]))
    loads.append(pltpu.make_async_copy(k_hbm, k_ref, tab.at[7]))
    for copy in loads:
        copy.start()
    greet(nb, me, g)

    mine3 = mine.reshape(216, 4, 128)

    def cells(ref, b, q):
        return ref.at[span(b * 864 + q * 216, 216)]

    cross = []
    for n in range(4):
        b = nth(c, n)
        cross.append(rcopy(mine3.at[:, b, :], cells(own, b, g), cross_s.at[n], cross_r.at[n], me, c))
        cross[n].start()
    sib = []
    for b in range(4):
        sib.append(rcopy(mine3.at[:, b, :], cells(own, b, g), sib_s.at[b], sib_r.at[b], me, s))
        sib[b].start()
    rcopy(mine3.at[:, g, :], low.at[span(g * 216, 216)], low_s, low_r, up, c).start()

    def spread(t, carry):
        for b in range(4):
            own[span(b * 864 + g * 216 + t * 8, 8), :] = mine[pl.ds(t * 32 + b, 8, stride=4), :]
        return carry

    lax.fori_loop(0, 27, spread, 0)

    def low_part(q):
        rcopy(cells(own, g, q), low.at[span(q * 216, 216)], low_s, low_r, up, c).start()

    for b in range(4):
        landed(cells(own, b, s), sib_r.at[b])
    low_part(s)
    fwd = [
        rcopy(cells(own, nth(g, n), c), cells(own, nth(g, n), c), fwd_s.at[n], fwd_r.at[n], me, s) for n in range(4)
    ]

    def crossed(n):
        landed(cells(own, nth(g, n), c), cross_r.at[n])
        fwd[n].start()

    def forwarded(n):
        landed(cells(own, nth(g, n), cs), fwd_r.at[n])

    def spread_low(n):
        @pl.when(g % 2 == n)
        def _():
            low_part(c)

    def spread_low2(n):
        @pl.when(g % 2 == n)
        def _():
            low_part(cs)

    for n in range(2):
        crossed(n)
        spread_low(n)
    for n in range(2):
        forwarded(n)
        spread_low2(n)
    u_ref[...] = jnp.zeros_like(u_ref)
    for copy in loads:
        copy.wait()

    def lay(slot, src, base):
        for r in range(18):
            for xg in range(6):
                row, lane = (r // 3) * 48 + xg * 8, (r % 3) * 128
                a_ref[slot, row : row + 8, lane : lane + 128] = src[pl.ds(base + xg * 144 + r, 8, stride=18), :]

    def unlay(slot, dst, base):
        for r in range(18):
            for xg in range(6):
                row, lane = (r // 3) * 48 + xg * 8, (r % 3) * 128
                dst[pl.ds(base + xg * 144 + r, 8, stride=18), :] = u_ref[slot, row : row + 8, lane : lane + 128]

    def lay_band(n):
        b = nth(g, n)
        lay(b, own, b * 864)

    def unlay_band(n):
        b = nth(g, n)
        unlay(b, un, b * 864)

    lay_band(0)
    lay_band(1)

    back = [
        rcopy(on.at[span(q * 216, 216)], ow.at[span(q * 216, 216)], ow_s.at[n], ow_r.at[n], down, c)
        for n, q in enumerate((s, g, cs, c))
    ]
    pass_on = []
    for n in range(4):
        for h, q in enumerate((cs, s)):
            at = n * 2 + h
            pass_on.append(
                rcopy(cells(un, nth(g, n), q), sb.at[at * 216 : at * 216 + 216], sb_s.at[at], sb_r.at[at], me, s)
            )
    away = [
        rcopy(cells(un, nth(g, n), c), xr.at[(n ^ 2) * 216 : (n ^ 2) * 216 + 216], xr_s.at[n], xr_r.at[n ^ 2], me, c)
        for n in range(4)
    ]

    def send_away(n):
        at = n * 2
        landed(sb.at[at * 216 : at * 216 + 216], sb_r.at[at])
        part = span(nth(g, n) * 864 + c * 216, 216)
        un[part, :] = un[part, :] + sb[at * 216 : at * 216 + 216, :]
        away[n].start()

    plane = me // 8
    above, below = (me + 8) % nb, (me + nb - 8) % nb
    pu, pd = (plane + 1) % 4, (plane + 3) % 4
    along = []
    for n, (rows, to) in enumerate(
        (
            (pl.ds(plane * 216, 216), above),
            (pl.ds(plane * 216, 216), below),
            (pl.ds(pd * 216, 108), above),
            (pl.ds(pu * 216 + 108, 108), below),
        )
    ):
        along.append(rcopy(obuf.at[rows], obuf.at[rows], zs.at[n], zr.at[n], to, g))

    def step(n, carry):
        @pl.when(n == 1)
        def _():
            crossed(2)
            landed(low, low_r)
            lay(4, low, 0)
            scatter_slices(mine3, obuf, plane * 216, os, orr, me, g)

        @pl.when(n == 2)
        def _():
            crossed(3)
            landed(obuf.at[0:189], orr)
            along[0].start()
            along[1].start()

        @pl.when(n == 3)
        def _():
            forwarded(2)
            forwarded(3)
            lay_band(2)
            lay_band(3)

        @pl.when(n == 5)
        def _():
            landed(obuf.at[0:216], zr.at[0])
            landed(obuf.at[0:216], zr.at[1])
            along[2].start()
            along[3].start()

        @pl.when(n == 6)
        def _():
            early()

        i, j, other = 0, 4, 1.0
        for at, slot in ((0, 0), (3, 1), (6, 2)):
            i = jnp.where(n == at, chosen(g, [row[slot] for row in OWN_I]), i)
            j = jnp.where(n == at, chosen(g, [row[slot] for row in OWN_J]), j)
        for at, k in ((1, 0), (2, 1), (4, 2), (5, 3)):
            i = jnp.where(n == at, nth(g, k), i)
        other = jnp.where(i == j, 0.0, 1.0)
        put(s_ref, 0, 288, 0, a_ref[i] * a_ref[j])
        potential(1, s_ref, t_ref, r_ref, w_ref, v_ref, wt_ref, hx_ref, k_ref)
        t = t_ref[...]
        u_ref[i] = u_ref[i] - a_ref[j] * t
        u_ref[j] = u_ref[j] - other * a_ref[i] * t
        return carry

    def early():
        unlay(4, on, 0)
        for copy in back:
            copy.start()
        for n in (2, 3):
            unlay_band(n)
            pass_on[2 * n].start()
            pass_on[2 * n + 1].start()
        send_away(2)
        send_away(3)

    lax.fori_loop(0, 6, step, 0)

    @pl.when(g % 2 == 1)
    def _():
        early()

    lax.fori_loop(6, chosen(g, STEPS), step, 0)

    for n in (0, 1):
        unlay_band(n)

    def add_owed(n, q):
        landed(ow.at[span(q * 216, 216)], ow_r.at[n])
        part = span(g * 864 + q * 216, 216)
        un[part, :] = un[part, :] + ow[span(q * 216, 216), :]

    def finish(n):
        b = nth(g, n)
        landed(sb.at[(n * 2 + 1) * 216 : (n * 2 + 2) * 216], sb_r.at[n * 2 + 1])
        landed(xr.at[n * 216 : n * 216 + 216], xr_r.at[n])

        def group(t, carry):
            value = (
                un[span(b * 864 + g * 216 + t * 8, 8), :]
                + sb[span((n * 2 + 1) * 216 + t * 8, 8), :]
                + xr[span(n * 216 + t * 8, 8), :]
            )
            vec_out[pl.ds(t * 32 + b, 8, stride=4), :] = value
            return carry

        lax.fori_loop(0, 27, group, 0)

    add_owed(0, cs)
    pass_on[0].start()
    pass_on[2].start()
    add_owed(1, c)
    send_away(0)
    send_away(1)
    landed(obuf.at[0:108], zr.at[2])
    landed(obuf.at[0:108], zr.at[3])
    lay_orbitals(obuf, bmat)
    add_owed(2, s)
    pass_on[1].start()
    pass_on[3].start()
    finish(2)
    finish(3)
    add_owed(3, g)
    finish(0)
    finish(1)
    scatter_slices(vec_out.reshape(216, 4, 128), vbuf, 0, vs, vr, me, g)
    landed(vbuf.at[0:189], vr)
    margin_tail(me, g, m_out, vbuf, bmat, mt8, red, rs, rr)
    landed(vbuf.at[0:189], os)
    landed(vbuf.at[0:189], vs)
    for copy in cross + fwd + sib + back + pass_on + away + along:
        copy.wait_send()
    landed(on, low_s)


def on_device(orbitals):
    nb = lax.axis_size("band")
    mine = orbitals.reshape(4, 216, 128).transpose(1, 0, 2).reshape(864, 128)
    vm = pl.BlockSpec(memory_space=pltpu.VMEM)
    hbm = pl.BlockSpec(memory_space=pl.ANY)
    dma = pltpu.SemaphoreType.DMA
    w, v, wt, hx, k = tables()

    def f32(*shape):
        return pltpu.VMEM(shape, F32)

    def b16(*shape):
        return pltpu.VMEM(shape, BF)

    vec, margin = pl.pallas_call(
        functools.partial(whole_kernel, nb),
        out_shape=(jax.ShapeDtypeStruct((864, 128), F32), jax.ShapeDtypeStruct((4, 32), F32)),
        in_specs=[vm] + [hbm] * 5,
        out_specs=(vm, vm),
        scratch_shapes=[b16(1152, 384), b16(1152, 384), b16(1152, 384), b16(48, 144), f32(288, 384)]
        + [f32(3456, 128), f32(864, 128), f32(5, 288, 384), f32(5, 288, 384)]
        + [b16(288, 768), f32(288, 384), b16(1152, 384)]
        + [f32(3456, 128), f32(864, 128), f32(864, 128), f32(1728, 128), f32(864, 128)]
        + [f32(864, 4, 128), f32(216, 4, 128), f32(3456, 128), f32(256, 128), f32(256, 128)]
        + [dma((8,)), dma((4,)), dma((4,)), dma((4,)), dma((4,)), dma((4,)), dma((4,)), dma, dma]
        + [dma((4,)), dma((4,)), dma((8,)), dma((8,)), dma((4,)), dma((4,))]
        + [dma] * 4
        + [dma((4,)), dma((4,)), dma, dma],
        compiler_params=pltpu.CompilerParams(
            collective_id=3, has_side_effects=True, vmem_limit_bytes=60 * 1024 * 1024
        ),
    )(mine, w, v, wt, hx, k)
    return vec.reshape(216, 4, 128).transpose(1, 0, 2).reshape(4, 27648), margin.T


def solution(mesh):
    return jax.shard_map(
        on_device,
        mesh=mesh,
        in_specs=(P("band", "grid"),),
        out_specs=(P("band", "grid"), P("grid", "band")),
        check_vma=False,
    )
```

```python
import functools
import numpy as np
import jax
import jax.numpy as jnp
from jax import lax
from jax.experimental import pallas as pl
from jax.experimental.pallas import tpu as pltpu
from jax.sharding import PartitionSpec as P

NG = 48
NCELL = 110592
BF = jnp.bfloat16
F32 = jnp.float32


def split_np(a):
    hi = a.astype(BF)
    lo = (a - hi.astype(np.float64)).astype(BF)
    return hi, lo


def tables():
    n = np.arange(NG)
    ang = 2.0 * np.pi * ((n[:, None] * n[None, :]) % NG) / NG
    h = np.cos(ang) + np.sin(ang)
    w = np.zeros((8, NG, 6, 8, 8))
    for y in range(8):
        w[y, :, :, y, :] = h.reshape(NG, 6, 8)
    w = w.reshape(384, 384)
    v = np.kron(h, np.eye(8))
    f = ((n + 24) % 48 - 24).astype(np.float64)
    q = f[:, None, None] ** 2 + f[None, :, None] ** 2 + f[None, None, :] ** 2
    k = np.where(q > 0, 40.0 * (1.0 - np.exp(-q / 16.0)) / np.where(q > 0, q, 1.0), 0.0) / NCELL
    k = k.reshape(NG, NG, 6, 8).transpose(2, 0, 1, 3).reshape(288, 384)

    def pack(m):
        hi, lo = split_np(m)
        return np.concatenate([hi, lo], axis=0)

    hh, hl = split_np(h)
    hx = np.concatenate([hh, hh, hl], axis=1)
    return pack(w), pack(v), pack(w.T.copy()), hx, k.astype(np.float32)


def hilo(x):
    hi = x.astype(BF)
    lo = (x - hi.astype(F32)).astype(BF)
    return hi, lo


def put(s_ref, row, rows, lane, x):
    hi, lo = hilo(x)
    n = x.shape[1]
    s_ref[row : row + rows, lane : lane + n] = hi
    s_ref[row : row + rows, 384 + lane : 384 + lane + n] = lo


def mm3(s_ref, w_ref):
    return jnp.dot(s_ref[...], w_ref[0:768, :], preferred_element_type=F32) + jnp.dot(
        s_ref[:, 0:384], w_ref[768:1152, :], preferred_element_type=F32
    )


def swap(t_ref, s_ref, pb, left):
    for p in range(pb):
        for j in range(3):
            for m in range(3):
                r0 = p * 288 + 2 * j * 48
                e = t_ref[r0 : r0 + 48, 128 * m : 128 * m + 128]
                o = t_ref[r0 + 48 : r0 + 96, 128 * m : 128 * m + 128]
                d0 = p * 288 + 2 * m * 48
                put(s_ref, d0, 48, 128 * j, jnp.where(left, e, pltpu.roll(o, 64, 1)))
                put(s_ref, d0 + 48, 48, 128 * j, jnp.where(left, pltpu.roll(e, 64, 1), o))


def potential(pb, s_ref, t_ref, r_ref, w_ref, v_ref, wt_ref, hx_ref, k_ref):
    left = lax.broadcasted_iota(jnp.int32, (48, 128), 1) < 64
    t_ref[...] = mm3(s_ref, w_ref)
    swap(t_ref, s_ref, pb, left)
    t_ref[...] = mm3(s_ref, v_ref)
    h2 = hx_ref[:, 0:96]
    h1 = hx_ref[:, 96:144]

    def xdot(row):
        return jnp.dot(h2, r_ref[row : row + 96, :], preferred_element_type=F32) + jnp.dot(
            h1, r_ref[row : row + 48, :], preferred_element_type=F32
        )

    for i in range(pb * 6):
        hi, lo = hilo(t_ref[i * 48 : i * 48 + 48, :])
        r_ref[i * 192 : i * 192 + 48, :] = hi
        r_ref[i * 192 + 48 : i * 192 + 96, :] = lo
        z = i % 6
        d = xdot(i * 192) * k_ref[z * 48 : z * 48 + 48, :]
        hi, lo = hilo(d)
        r_ref[i * 192 + 96 : i * 192 + 144, :] = hi
        r_ref[i * 192 + 144 : i * 192 + 192, :] = lo
        put(s_ref, i * 48, 48, 0, xdot(i * 192 + 96))
    t_ref[...] = mm3(s_ref, v_ref)
    swap(t_ref, s_ref, pb, left)
    t_ref[...] = mm3(s_ref, wt_ref)


MESH = pl.DeviceIdType.MESH


def rcopy(src, dst, send, recv, band, grid):
    return pltpu.make_async_remote_copy(
        src_ref=src, dst_ref=dst, send_sem=send, recv_sem=recv, device_id={"band": band, "grid": grid}, device_id_type=MESH
    )


def landed(ref, sem):
    pltpu.make_async_copy(ref, ref, sem).wait()


def greet(nb, me, g):
    barrier = pltpu.get_barrier_semaphore()
    plane, w = me // 8, me % 8

    def signal(band, grid):
        pl.semaphore_signal(barrier, inc=1, device_id={"band": band, "grid": grid}, device_id_type=MESH)

    def one(o, c):
        n = (w * 4 + g + o) % 32
        signal(plane * 8 + n // 4, n % 4)
        return c

    signal((me + 1) % nb, (g + 2) % 4)
    signal((me + nb - 1) % nb, (g + 2) % 4)
    lax.fori_loop(1, 32, one, 0)
    for o in range(1, 4):
        signal((me + 8 * o) % nb, g)
    pl.semaphore_wait(barrier, 36)


def span(start, size):
    return pl.ds(pl.multiple_of(start, 8), size)


def nth(g, n):
    return (n + 2 * (g // 2)) % 4


def scatter_slices(src3, buf3, base, send, recv, me, g):
    plane, w = me // 8, me % 8

    def one(o, c):
        dst = (w + o) % 8
        rcopy(
            src3.at[pl.ds(dst * 27, 27)],
            buf3.at[pl.ds(base + w * 27, 27)],
            send,
            recv,
            plane * 8 + dst,
            (g + 2) % 4,
        ).start()
        return c

    lax.fori_loop(0, 8, one, 0)


def lay_orbitals(obuf, line, bh, bl):
    flat = obuf.reshape(3456, 128)

    def chunks(p, carry):
        for h in range(2):
            c = jnp.minimum(2 * p + h, 26)
            for z in range(4):
                for b in range(4):
                    line[pl.ds(h * 128 + z * 32 + b, 8, stride=4), :] = flat[
                        pl.ds(z * 864 + c * 4 + b, 8, stride=108), :
                    ]
            hi, lo = hilo(line[h * 128 : h * 128 + 128, :])
            bh[span(p * 128, 128), h * 128 : h * 128 + 128] = hi
            bl[span(p * 128, 128), h * 128 : h * 128 + 128] = lo
        return carry

    lax.fori_loop(0, 14, chunks, 0)


def margin_tail(me, g, out_ref, vbuf, bh_ref, bl_ref, mt8, red, rs, rr):
    plane, w = me // 8, me % 8
    flat = vbuf.reshape(864, 128)
    m = jnp.zeros((32, 128), F32)
    dims = (((1,), (1,)), ((), ()))
    for p in range(14):
        parts = [
            jnp.concatenate([flat[pl.ds(c * 4 + b, 8, stride=108), :] for b in range(4)], axis=0)
            for c in range(2 * p, min(2 * p + 2, 27))
        ]
        ah, al = hilo(jnp.concatenate(parts, axis=1))
        width = 128 * len(parts)
        bh, bl = bh_ref[p * 128 : p * 128 + 128, 0:width], bl_ref[p * 128 : p * 128 + 128, 0:width]
        m = m + (
            lax.dot_general(ah, bh, dims, preferred_element_type=F32)
            + lax.dot_general(al, bh, dims, preferred_element_type=F32)
            + lax.dot_general(ah, bl, dims, preferred_element_type=F32)
        )
    m = m * (1.0 / NCELL)
    lane = lax.broadcasted_iota(jnp.int32, (8, 128), 1) // 32
    for t in range(4):
        piece = jnp.zeros((8, 128), F32)
        for b in range(4):
            row = m[b * 8 : b * 8 + 8, :]
            turn = 32 * ((b - t) % 4)
            piece = jnp.where(lane == b, pltpu.roll(row, turn, 1) if turn else row, piece)
        mt8[pl.ds(t * 64, 8, stride=8), :] = piece
    here = (g * 8 + w) * 8

    def one(o, c):
        n = (w * 4 + g + o) % 32
        dst, to = n // 4, n % 4
        rcopy(mt8.at[span((to * 8 + dst) * 8, 8)], red.at[span(here, 8)], rs, rr, plane * 8 + dst, to).start()
        return c

    lax.fori_loop(1, 32, one, 0)
    red[span(here, 8), :] = mt8[span(here, 8), :]
    landed(red.at[0 : 31 * 8], rr)
    total = jnp.sum(red[pl.ds(0, 32, stride=8), :], axis=0, keepdims=True)
    for b in range(4):
        out_ref[b : b + 1, :] = total[:, b * 32 : b * 32 + 32]
    landed(mt8.at[0 : 31 * 8], rs)


OWN_I = ((0, 0, 1), (0, 1, 0), (2, 2, 3), (2, 3, 0))
OWN_J = ((0, 2, 1), (1, 3, 0), (2, 1, 3), (3, 0, 0))
STEPS = (7, 6, 7, 6)


def chosen(g, values):
    total = 0
    for t, value in enumerate(values):
        total = total + jnp.where(g == t, value, 0)
    return total


def whole_kernel(nb, mine, w_hbm, v_hbm, wt_hbm, hx_hbm, k_hbm, vec_out, m_out, *scratch):
    (w_ref, v_ref, wt_ref, hx_ref, k_ref, own, low, a_ref, u_ref, s_ref, t_ref, r_ref, un, on, ow, sb, xr) = scratch[:17]
    (obuf, vbuf, line, bh, bl, mt8, red, tab, sib_s, sib_r, cross_s, cross_r, fwd_s, fwd_r) = scratch[17:31]
    (low_s, low_r, ow_s, ow_r, sb_s, sb_r, xr_s, xr_r, os, orr, vs, vr, zs, zr, rs, rr) = scratch[31:]
    me, g = lax.axis_index("band"), lax.axis_index("grid")
    c, s = (g + 2) % 4, g + 1 - 2 * (g % 2)
    cs = (s + 2) % 4
    up, down = (me + 1) % nb, (me + nb - 1) % nb
    loads = []
    for n, (a, b) in enumerate(((w_hbm, w_ref), (v_hbm, v_ref), (wt_hbm, wt_ref))):
        loads.append(pltpu.make_async_copy(a.at[0:384], b.at[0:384], tab.at[2 * n]))
        loads.append(pltpu.make_async_copy(a, b.at[384:1152], tab.at[2 * n + 1]))
    loads.append(pltpu.make_async_copy(hx_hbm, hx_ref, tab.at[6]))
    loads.append(pltpu.make_async_copy(k_hbm, k_ref, tab.at[7]))
    for copy in loads:
        copy.start()
    greet(nb, me, g)

    mine3 = mine.reshape(216, 4, 128)

    def cells(ref, b, q):
        return ref.at[span(b * 864 + q * 216, 216)]

    cross = []
    for n in range(4):
        b = nth(c, n)
        cross.append(rcopy(mine3.at[:, b, :], cells(own, b, g), cross_s.at[n], cross_r.at[n], me, c))
        cross[n].start()
    sib = []
    for b in range(4):
        sib.append(rcopy(mine3.at[:, b, :], cells(own, b, g), sib_s.at[b], sib_r.at[b], me, s))
        sib[b].start()
    rcopy(mine3.at[:, g, :], low.at[span(g * 216, 216)], low_s, low_r, up, c).start()

    def spread(t, carry):
        for b in range(4):
            own[span(b * 864 + g * 216 + t * 8, 8), :] = mine[pl.ds(t * 32 + b, 8, stride=4), :]
        return carry

    lax.fori_loop(0, 27, spread, 0)

    def low_part(q):
        rcopy(cells(own, g, q), low.at[span(q * 216, 216)], low_s, low_r, up, c).start()

    for b in range(4):
        landed(cells(own, b, s), sib_r.at[b])
    low_part(s)
    fwd = [
        rcopy(cells(own, nth(g, n), c), cells(own, nth(g, n), c), fwd_s.at[n], fwd_r.at[n], me, s) for n in range(4)
    ]

    def crossed(n):
        landed(cells(own, nth(g, n), c), cross_r.at[n])
        fwd[n].start()

    def forwarded(n):
        landed(cells(own, nth(g, n), cs), fwd_r.at[n])

    def spread_low(n):
        @pl.when(g % 2 == n)
        def _():
            low_part(c)

    def spread_low2(n):
        @pl.when(g % 2 == n)
        def _():
            low_part(cs)

    for n in range(2):
        crossed(n)
        spread_low(n)
    for n in range(2):
        forwarded(n)
        spread_low2(n)
    u_ref[...] = jnp.zeros_like(u_ref)
    for copy in loads:
        copy.wait()

    def lay(slot, src, base):
        for r in range(18):
            for xg in range(6):
                row, lane = (r // 3) * 48 + xg * 8, (r % 3) * 128
                a_ref[slot, row : row + 8, lane : lane + 128] = src[pl.ds(base + xg * 144 + r, 8, stride=18), :]

    def unlay(slot, dst, base):
        for r in range(18):
            for xg in range(6):
                row, lane = (r // 3) * 48 + xg * 8, (r % 3) * 128
                dst[pl.ds(base + xg * 144 + r, 8, stride=18), :] = u_ref[slot, row : row + 8, lane : lane + 128]

    def lay_band(n):
        b = nth(g, n)
        lay(b, own, b * 864)

    def unlay_band(n):
        b = nth(g, n)
        unlay(b, un, b * 864)

    lay_band(0)
    lay_band(1)

    back = [
        rcopy(on.at[span(q * 216, 216)], ow.at[span(q * 216, 216)], ow_s.at[n], ow_r.at[n], down, c)
        for n, q in enumerate((s, g, cs, c))
    ]
    pass_on = []
    for n in range(4):
        for h, q in enumerate((cs, s)):
            at = n * 2 + h
            pass_on.append(
                rcopy(cells(un, nth(g, n), q), sb.at[at * 216 : at * 216 + 216], sb_s.at[at], sb_r.at[at], me, s)
            )
    away = [
        rcopy(cells(un, nth(g, n), c), xr.at[(n ^ 2) * 216 : (n ^ 2) * 216 + 216], xr_s.at[n], xr_r.at[n ^ 2], me, c)
        for n in range(4)
    ]

    def send_away(n):
        at = n * 2
        landed(sb.at[at * 216 : at * 216 + 216], sb_r.at[at])
        part = span(nth(g, n) * 864 + c * 216, 216)
        un[part, :] = un[part, :] + sb[at * 216 : at * 216 + 216, :]
        away[n].start()

    plane = me // 8
    above, below = (me + 8) % nb, (me + nb - 8) % nb
    pu, pd = (plane + 1) % 4, (plane + 3) % 4
    along = []
    for n, (rows, to) in enumerate(
        (
            (pl.ds(plane * 216, 216), above),
            (pl.ds(plane * 216, 216), below),
            (pl.ds(pd * 216, 108), above),
            (pl.ds(pu * 216 + 108, 108), below),
        )
    ):
        along.append(rcopy(obuf.at[rows], obuf.at[rows], zs.at[n], zr.at[n], to, g))

    def step(n, carry):
        @pl.when(n == 1)
        def _():
            crossed(2)
            landed(low, low_r)
            lay(4, low, 0)
            scatter_slices(mine3, obuf, plane * 216, os, orr, me, g)

        @pl.when(n == 2)
        def _():
            crossed(3)

        @pl.when(n == 3)
        def _():
            forwarded(2)
            forwarded(3)
            lay_band(2)
            lay_band(3)
            landed(obuf.at[0:216], orr)
            along[0].start()
            along[1].start()

        @pl.when(n == 6)
        def _():
            early()

        i, j, other = 0, 4, 1.0
        for at, slot in ((0, 0), (3, 1), (6, 2)):
            i = jnp.where(n == at, chosen(g, [row[slot] for row in OWN_I]), i)
            j = jnp.where(n == at, chosen(g, [row[slot] for row in OWN_J]), j)
        for at, k in ((1, 0), (2, 1), (4, 2), (5, 3)):
            i = jnp.where(n == at, nth(g, k), i)
        other = jnp.where(i == j, 0.0, 1.0)
        put(s_ref, 0, 288, 0, a_ref[i] * a_ref[j])
        potential(1, s_ref, t_ref, r_ref, w_ref, v_ref, wt_ref, hx_ref, k_ref)
        t = t_ref[...]
        u_ref[i] = u_ref[i] - a_ref[j] * t
        u_ref[j] = u_ref[j] - other * a_ref[i] * t
        return carry

    def early():
        unlay(4, on, 0)
        for copy in back:
            copy.start()
        for n in (2, 3):
            unlay_band(n)
            pass_on[2 * n].start()
            pass_on[2 * n + 1].start()
        send_away(2)
        send_away(3)
        landed(obuf.at[0:216], zr.at[0])
        landed(obuf.at[0:216], zr.at[1])
        along[2].start()
        along[3].start()

    lax.fori_loop(0, 6, step, 0)

    @pl.when(g % 2 == 1)
    def _():
        early()

    lax.fori_loop(6, chosen(g, STEPS), step, 0)

    for n in (0, 1):
        unlay_band(n)

    def add_owed(n, q):
        landed(ow.at[span(q * 216, 216)], ow_r.at[n])
        part = span(g * 864 + q * 216, 216)
        un[part, :] = un[part, :] + ow[span(q * 216, 216), :]

    def finish(n):
        b = nth(g, n)
        landed(sb.at[(n * 2 + 1) * 216 : (n * 2 + 2) * 216], sb_r.at[n * 2 + 1])
        landed(xr.at[n * 216 : n * 216 + 216], xr_r.at[n])

        def group(t, carry):
            value = (
                un[span(b * 864 + g * 216 + t * 8, 8), :]
                + sb[span((n * 2 + 1) * 216 + t * 8, 8), :]
                + xr[span(n * 216 + t * 8, 8), :]
            )
            vec_out[pl.ds(t * 32 + b, 8, stride=4), :] = value
            return carry

        lax.fori_loop(0, 27, group, 0)

    add_owed(0, cs)
    pass_on[0].start()
    pass_on[2].start()
    add_owed(1, c)
    send_away(0)
    send_away(1)
    add_owed(2, s)
    pass_on[1].start()
    pass_on[3].start()
    finish(2)
    finish(3)
    add_owed(3, g)
    finish(0)
    finish(1)
    scatter_slices(vec_out.reshape(216, 4, 128), vbuf, 0, vs, vr, me, g)
    landed(obuf.at[0:108], zr.at[2])
    landed(obuf.at[0:108], zr.at[3])
    lay_orbitals(obuf, line, bh, bl)
    landed(vbuf, vr)
    margin_tail(me, g, m_out, vbuf, bh, bl, mt8, red, rs, rr)
    landed(vbuf, os)
    landed(vbuf, vs)
    for copy in cross + fwd + sib + back + pass_on + away + along:
        copy.wait_send()
    landed(on, low_s)


def on_device(orbitals):
    nb = lax.axis_size("band")
    mine = orbitals.reshape(4, 216, 128).transpose(1, 0, 2).reshape(864, 128)
    vm = pl.BlockSpec(memory_space=pltpu.VMEM)
    hbm = pl.BlockSpec(memory_space=pl.ANY)
    dma = pltpu.SemaphoreType.DMA
    w, v, wt, hx, k = tables()

    def f32(*shape):
        return pltpu.VMEM(shape, F32)

    def b16(*shape):
        return pltpu.VMEM(shape, BF)

    vec, margin = pl.pallas_call(
        functools.partial(whole_kernel, nb),
        out_shape=(jax.ShapeDtypeStruct((864, 128), F32), jax.ShapeDtypeStruct((4, 32), F32)),
        in_specs=[vm] + [hbm] * 5,
        out_specs=(vm, vm),
        scratch_shapes=[b16(1152, 384), b16(1152, 384), b16(1152, 384), b16(48, 144), f32(288, 384)]
        + [f32(3456, 128), f32(864, 128), f32(5, 288, 384), f32(5, 288, 384)]
        + [b16(288, 768), f32(288, 384), b16(1152, 384)]
        + [f32(3456, 128), f32(864, 128), f32(864, 128), f32(1728, 128), f32(864, 128)]
        + [f32(864, 4, 128), f32(216, 4, 128), f32(256, 128), b16(1792, 256), b16(1792, 256), f32(256, 128), f32(256, 128)]
        + [dma((8,)), dma((4,)), dma((4,)), dma((4,)), dma((4,)), dma((4,)), dma((4,)), dma, dma]
        + [dma((4,)), dma((4,)), dma((8,)), dma((8,)), dma((4,)), dma((4,))]
        + [dma] * 4
        + [dma((4,)), dma((4,)), dma, dma],
        compiler_params=pltpu.CompilerParams(
            collective_id=3, has_side_effects=True, vmem_limit_bytes=60 * 1024 * 1024
        ),
    )(mine, w, v, wt, hx, k)
    return vec.reshape(216, 4, 128).transpose(1, 0, 2).reshape(4, 27648), margin.T


def solution(mesh):
    return jax.shard_map(
        on_device,
        mesh=mesh,
        in_specs=(P("band", "grid"),),
        out_specs=(P("band", "grid"), P("grid", "band")),
        check_vma=False,
    )
```

```python
import functools
import numpy as np
import jax
import jax.numpy as jnp
from jax import lax
from jax.experimental import pallas as pl
from jax.experimental.pallas import tpu as pltpu
from jax.sharding import PartitionSpec as P

NG = 48
NCELL = 110592
BF = jnp.bfloat16
F32 = jnp.float32


def split_np(a):
    hi = a.astype(BF)
    lo = (a - hi.astype(np.float64)).astype(BF)
    return hi, lo


def tables():
    n = np.arange(NG)
    ang = 2.0 * np.pi * ((n[:, None] * n[None, :]) % NG) / NG
    h = np.cos(ang) + np.sin(ang)
    w = np.zeros((8, NG, 6, 8, 8))
    for y in range(8):
        w[y, :, :, y, :] = h.reshape(NG, 6, 8)
    w = w.reshape(384, 384)
    v = np.kron(h, np.eye(8))
    f = ((n + 24) % 48 - 24).astype(np.float64)
    q = f[:, None, None] ** 2 + f[None, :, None] ** 2 + f[None, None, :] ** 2
    k = np.where(q > 0, 40.0 * (1.0 - np.exp(-q / 16.0)) / np.where(q > 0, q, 1.0), 0.0) / NCELL
    k = k.reshape(NG, NG, 6, 8).transpose(2, 0, 1, 3).reshape(288, 384)

    def pack(m):
        hi, lo = split_np(m)
        return np.concatenate([hi, lo], axis=0)

    hh, hl = split_np(h)
    hx = np.concatenate([np.concatenate([hh, hh], axis=1), np.concatenate([hl, np.zeros_like(hl)], axis=1)], axis=0)
    return pack(w), pack(v), pack(w.T.copy()), hx, k.astype(np.float32)


def hilo(x):
    hi = x.astype(BF)
    lo = (x - hi.astype(F32)).astype(BF)
    return hi, lo


def put(s_ref, row, rows, lane, x):
    hi, lo = hilo(x)
    n = x.shape[1]
    s_ref[row : row + rows, lane : lane + n] = hi
    s_ref[row : row + rows, 384 + lane : 384 + lane + n] = lo


def mm3(s_ref, w_ref):
    return jnp.dot(s_ref[...], w_ref[0:768, :], preferred_element_type=F32) + jnp.dot(
        s_ref[:, 0:384], w_ref[768:1152, :], preferred_element_type=F32
    )


def swap(t_ref, s_ref, left):
    for j in range(3):
        for m in range(3):
            r0, d0 = 2 * j * 48, 2 * m * 48
            e = t_ref[r0 : r0 + 48, 128 * m : 128 * m + 128]
            o = t_ref[r0 + 48 : r0 + 96, 128 * m : 128 * m + 128]
            put(s_ref, d0, 48, 128 * j, jnp.where(left, e, pltpu.roll(o, 64, 1)))
            put(s_ref, d0 + 48, 48, 128 * j, jnp.where(left, pltpu.roll(e, 64, 1), o))


def middle(s_ref, t_ref, r_ref, hx_ref, k_ref):
    def xdot(g, base):
        y = jnp.dot(hx_ref[...], r_ref[g * 192 + base : g * 192 + base + 96, :], preferred_element_type=F32)
        return y[0:48] + y[48:96]

    for g in range(3):
        for h in range(2):
            z = 2 * g + h
            hi, lo = hilo(t_ref[z * 48 : z * 48 + 48, :])
            r_ref[g * 192 : g * 192 + 48, h * 384 : h * 384 + 384] = hi
            r_ref[g * 192 + 48 : g * 192 + 96, h * 384 : h * 384 + 384] = lo
    for g in range(3):
        d = xdot(g, 0)
        for h in range(2):
            z = 2 * g + h
            hi, lo = hilo(d[:, h * 384 : h * 384 + 384] * k_ref[z * 48 : z * 48 + 48, :])
            r_ref[g * 192 + 96 : g * 192 + 144, h * 384 : h * 384 + 384] = hi
            r_ref[g * 192 + 144 : g * 192 + 192, h * 384 : h * 384 + 384] = lo
    for g in range(3):
        d = xdot(g, 96)
        for h in range(2):
            put(s_ref, (2 * g + h) * 48, 48, 0, d[:, h * 384 : h * 384 + 384])


def stages(s_ref, t_ref, r_ref, w_ref, v_ref, wt_ref, hx_ref, k_ref):
    left = lax.broadcasted_iota(jnp.int32, (48, 128), 1) < 64

    def mm(weights):
        def run():
            t_ref[...] = mm3(s_ref, weights)

        return run

    def turn():
        swap(t_ref, s_ref, left)

    def mid():
        middle(s_ref, t_ref, r_ref, hx_ref, k_ref)

    return [mm(w_ref), turn, mm(v_ref), mid, mm(v_ref), turn, mm(wt_ref)]


def potentials(sets, tables_, between=None):
    lists = [stages(*refs, *tables_) for refs in sets]
    count = len(lists[0])
    for n in range(count + len(lists) - 1):
        if n == 3 and between is not None:
            between()
        for p, steps in enumerate(lists):
            if 0 <= n - p < count:
                steps[n - p]()
MESH = pl.DeviceIdType.MESH
RELAY = 6


def rcopy(src, dst, send, recv, band, grid):
    return pltpu.make_async_remote_copy(
        src_ref=src, dst_ref=dst, send_sem=send, recv_sem=recv, device_id={"band": band, "grid": grid}, device_id_type=MESH
    )


def landed(ref, sem):
    pltpu.make_async_copy(ref, ref, sem).wait()


def greet(nb, me, g):
    barrier = pltpu.get_barrier_semaphore()
    plane, w = me // 8, me % 8

    def signal(band, grid):
        pl.semaphore_signal(barrier, inc=1, device_id={"band": band, "grid": grid}, device_id_type=MESH)

    def one(o, c):
        n = (w * 4 + g + o) % 32
        signal(plane * 8 + n // 4, n % 4)
        return c

    signal((me + 1) % nb, (g + 2) % 4)
    signal((me + nb - 1) % nb, (g + 2) % 4)
    lax.fori_loop(1, 32, one, 0)
    for o in range(1, 4):
        signal((me + 8 * o) % nb, g)
    pl.semaphore_wait(barrier, 36)


def span(start, size):
    return pl.ds(pl.multiple_of(start, 8), size)


def nth(g, n):
    return (n + 2 * (g // 2)) % 4


def slice_copy(src3, at, buf, rows, send, recv, me, g, w):
    part = src3.at[pl.ds(at * 27, 27)]
    return rcopy(part, buf.at[pl.ds(rows, 27)], send, recv, me // 8 * 8 + w, g)


def scatter_slices(src3, buf3, base, send, recv, me, g, steps):
    w = me % 8

    def one(o, c):
        dst = (w + o) % 8
        slice_copy(src3, dst, buf3, base + w * 27, send, recv, me, (g + 2) % 4, dst).start()
        return c

    for first, last in steps:
        lax.fori_loop(first, last, one, 0)


def lay_orbitals(obuf, line, bh, bl):
    flat = obuf.reshape(3456, 128)

    def chunks(p, carry):
        for h in range(2):
            c = jnp.minimum(2 * p + h, 26)
            for z in range(4):
                for b in range(4):
                    line[pl.ds(h * 128 + z * 32 + b, 8, stride=4), :] = flat[
                        pl.ds(z * 864 + c * 4 + b, 8, stride=108), :
                    ]
            hi, lo = hilo(line[h * 128 : h * 128 + 128, :])
            bh[span(p * 128, 128), h * 128 : h * 128 + 128] = hi
            bl[span(p * 128, 128), h * 128 : h * 128 + 128] = lo
        return carry

    lax.fori_loop(0, 14, chunks, 0)


def margin_tail(me, g, out_ref, vbuf, bh_ref, bl_ref, mt8, red, rs, rr):
    plane, w = me // 8, me % 8
    flat = vbuf.reshape(864, 128)
    m = jnp.zeros((32, 128), F32)
    dims = (((1,), (1,)), ((), ()))
    for p in range(14):
        parts = [
            jnp.concatenate([flat[pl.ds(c * 4 + b, 8, stride=108), :] for b in range(4)], axis=0)
            for c in range(2 * p, min(2 * p + 2, 27))
        ]
        ah, al = hilo(jnp.concatenate(parts, axis=1))
        width = 128 * len(parts)
        bh, bl = bh_ref[p * 128 : p * 128 + 128, 0:width], bl_ref[p * 128 : p * 128 + 128, 0:width]
        m = m + (
            lax.dot_general(ah, bh, dims, preferred_element_type=F32)
            + lax.dot_general(al, bh, dims, preferred_element_type=F32)
            + lax.dot_general(ah, bl, dims, preferred_element_type=F32)
        )
    m = m * (1.0 / NCELL)
    lane = lax.broadcasted_iota(jnp.int32, (8, 128), 1) // 32
    for t in range(4):
        piece = jnp.zeros((8, 128), F32)
        for b in range(4):
            row = m[b * 8 : b * 8 + 8, :]
            turn = 32 * ((b - t) % 4)
            piece = jnp.where(lane == b, pltpu.roll(row, turn, 1) if turn else row, piece)
        mt8[pl.ds(t * 64, 8, stride=8), :] = piece
    here = (g * 8 + w) * 8

    def one(o, c):
        n = (w * 4 + g + o) % 32
        dst, to = n // 4, n % 4
        rcopy(mt8.at[span((to * 8 + dst) * 8, 8)], red.at[span(here, 8)], rs, rr, plane * 8 + dst, to).start()
        return c

    lax.fori_loop(1, 32, one, 0)
    red[span(here, 8), :] = mt8[span(here, 8), :]
    landed(red.at[0 : 31 * 8], rr)
    total = jnp.sum(red[pl.ds(0, 32, stride=8), :], axis=0, keepdims=True)
    for b in range(4):
        out_ref[b : b + 1, :] = total[:, b * 32 : b * 32 + 32]
    landed(mt8.at[0 : 31 * 8], rs)


OWN_I = ((0, 0, 1), (0, 1, 0), (2, 2, 3), (2, 3, 2))
OWN_J = ((0, 2, 1), (1, 3, 0), (2, 1, 3), (3, 0, 2))


def chosen(g, values):
    total = 0
    for t, value in enumerate(values):
        total = total + jnp.where(g == t, value, 0)
    return total


def whole_kernel(nb, mine, w_hbm, v_hbm, wt_hbm, hx_hbm, k_hbm, vec_out, m_out, *scratch):
    (w_ref, v_ref, wt_ref, hx_ref, k_ref, own, low, a_ref, u_ref, un, on, ow, sb, xr) = scratch[:14]
    (obuf, vbuf, line, bh, bl, mt8, red, tab, sib_s, sib_r, cross_s, cross_r, fwd_s, fwd_r) = scratch[14:28]
    relay, relay_r, onward_s, onward_r = scratch[53:]
    (low_s, low_r, ow_s, ow_r, sb_s, sb_r, xr_s, xr_r, os, orr, vs, vr, zs, zr, rs, rr) = scratch[28:44]
    sets = [scratch[44 + 3 * p : 47 + 3 * p] for p in range(3)]
    shared = (w_ref, v_ref, wt_ref, hx_ref, k_ref)
    me, g = lax.axis_index("band"), lax.axis_index("grid")
    c, s = (g + 2) % 4, g + 1 - 2 * (g % 2)
    cs = (s + 2) % 4
    up, down = (me + 1) % nb, (me + nb - 1) % nb
    loads = []
    for n, (a, b) in enumerate(((w_hbm, w_ref), (v_hbm, v_ref), (wt_hbm, wt_ref))):
        loads.append(pltpu.make_async_copy(a.at[0:384], b.at[0:384], tab.at[2 * n]))
        loads.append(pltpu.make_async_copy(a, b.at[384:1152], tab.at[2 * n + 1]))
    loads.append(pltpu.make_async_copy(hx_hbm, hx_ref, tab.at[6]))
    loads.append(pltpu.make_async_copy(k_hbm, k_ref, tab.at[7]))
    for copy in loads:
        copy.start()
    greet(nb, me, g)

    mine3 = mine.reshape(216, 4, 128)

    def cells(ref, b, q):
        return ref.at[span(b * 864 + q * 216, 216)]

    cross = []
    for n in range(4):
        b = nth(c, n)
        cross.append(rcopy(mine3.at[:, b, :], cells(own, b, g), cross_s.at[n], cross_r.at[n], me, c))
        cross[n].start()
    sib = []
    for b in range(4):
        sib.append(rcopy(mine3.at[:, b, :], cells(own, b, g), sib_s.at[b], sib_r.at[b], me, s))
        sib[b].start()
    rcopy(mine3.at[:, g, :], low.at[span(g * 216, 216)], low_s, low_r, up, c).start()

    def spread(t, carry):
        for b in range(4):
            own[span(b * 864 + g * 216 + t * 8, 8), :] = mine[pl.ds(t * 32 + b, 8, stride=4), :]
        return carry

    lax.fori_loop(0, 27, spread, 0)

    def low_part(q):
        rcopy(cells(own, g, q), low.at[span(q * 216, 216)], low_s, low_r, up, c).start()

    for b in range(4):
        landed(cells(own, b, s), sib_r.at[b])
    low_part(s)
    fwd = [
        rcopy(cells(own, nth(g, n), c), cells(own, nth(g, n), c), fwd_s.at[n], fwd_r.at[n], me, s) for n in range(4)
    ]

    def crossed(n):
        landed(cells(own, nth(g, n), c), cross_r.at[n])
        fwd[n].start()

    def forwarded(n):
        landed(cells(own, nth(g, n), cs), fwd_r.at[n])

    def spread_low(n):
        @pl.when(g % 2 == n)
        def _():
            low_part(c)

    def spread_low2(n):
        @pl.when(g % 2 == n)
        def _():
            low_part(cs)

    for n in range(2):
        crossed(n)
        spread_low(n)
    for n in range(2):
        forwarded(n)
        spread_low2(n)
    u_ref[...] = jnp.zeros_like(u_ref)
    for copy in loads:
        copy.wait()

    def lay(slot, src, base):
        for r in range(18):
            for xg in range(6):
                row, lane = (r // 3) * 48 + xg * 8, (r % 3) * 128
                a_ref[slot, row : row + 8, lane : lane + 128] = src[pl.ds(base + xg * 144 + r, 8, stride=18), :]

    def unlay(slot, dst, base):
        for r in range(18):
            for xg in range(6):
                row, lane = (r // 3) * 48 + xg * 8, (r % 3) * 128
                dst[pl.ds(base + xg * 144 + r, 8, stride=18), :] = u_ref[slot, row : row + 8, lane : lane + 128]

    def lay_band(n):
        b = nth(g, n)
        lay(b, own, b * 864)

    def unlay_band(n):
        b = nth(g, n)
        unlay(b, un, b * 864)

    lay_band(0)
    lay_band(1)

    back = [
        rcopy(on.at[span(q * 216, 216)], ow.at[span(q * 216, 216)], ow_s.at[n], ow_r.at[n], down, c)
        for n, q in enumerate((s, g, cs, c))
    ]
    pass_on = []
    for n in range(4):
        for h, q in enumerate((cs, s)):
            at = n * 2 + h
            pass_on.append(
                rcopy(cells(un, nth(g, n), q), sb.at[at * 216 : at * 216 + 216], sb_s.at[at], sb_r.at[at], me, s)
            )
    away = [
        rcopy(cells(un, nth(g, n), c), xr.at[(n ^ 2) * 216 : (n ^ 2) * 216 + 216], xr_s.at[n], xr_r.at[n ^ 2], me, c)
        for n in range(4)
    ]

    def send_away(n):
        at = n * 2
        landed(sb.at[at * 216 : at * 216 + 216], sb_r.at[at])
        part = span(nth(g, n) * 864 + c * 216, 216)
        un[part, :] = un[part, :] + sb[at * 216 : at * 216 + 216, :]
        away[n].start()

    plane = me // 8
    above, below = (me + 8) % nb, (me + nb - 8) % nb
    pu, pd = (plane + 1) % 4, (plane + 3) % 4
    along = []
    for n, (rows, to) in enumerate(
        (
            (pl.ds(plane * 216, 216), above),
            (pl.ds(plane * 216, 216), below),
            (pl.ds(pd * 216, 108), above),
            (pl.ds(pu * 216 + 108, 108), below),
        )
    ):
        along.append(rcopy(obuf.at[rows], obuf.at[rows], zs.at[n], zr.at[n], to, g))

    def own_slot(slot):
        return chosen(g, [row[slot] for row in OWN_I]), chosen(g, [row[slot] for row in OWN_J])

    def step(n, carry):
        @pl.when(n == 1)
        def _():
            scatter_slices(mine3, obuf, plane * 216, os, orr, me, g, ((0, 8),))
            crossed(2)
            crossed(3)
            landed(low, low_r)
            lay(4, low, 0)

        pairs = []
        for p, slot in ((0, 0), (1, 2)):
            i, j = own_slot(slot)
            weight = jnp.where((n == 0) & (p == 1) & (g % 2 == 1), 0.0, 1.0)
            i, j = jnp.where(n == 0, i, nth(g, p)), jnp.where(n == 0, j, 4)
            pairs.append((i, j, weight, jnp.where(i == j, 0.0, weight)))
        for p, (i, j, _, _) in enumerate(pairs):
            put(sets[p][0], 0, 288, 0, a_ref[i] * a_ref[j])
        potentials(sets[:2], shared)
        for p, (i, j, one, two) in enumerate(pairs):
            t = sets[p][1][...]
            u_ref[i] = u_ref[i] - one * a_ref[j] * t
            u_ref[j] = u_ref[j] - two * a_ref[i] * t
        return carry

    lax.fori_loop(0, 2, step, 0)

    forwarded(2)
    forwarded(3)
    lay_band(2)
    lay_band(3)
    pairs = [(nth(g, 2), 4), (nth(g, 3), 4), own_slot(1)]
    for p, (i, j) in enumerate(pairs):
        put(sets[p][0], 0, 288, 0, a_ref[i] * a_ref[j])
    def pass_orbitals():
        landed(obuf.at[0:216], orr)
        along[0].start()
        along[1].start()

    potentials(sets, shared, pass_orbitals)
    for p, (i, j) in enumerate(pairs):
        t = sets[p][1][...]
        u_ref[i] = u_ref[i] - a_ref[j] * t
        u_ref[j] = u_ref[j] - a_ref[i] * t

    unlay(4, on, 0)
    for copy in back:
        copy.start()
    for n in (2, 3):
        unlay_band(n)
        pass_on[2 * n].start()
        pass_on[2 * n + 1].start()
    for n in (0, 1):
        unlay_band(n)
    send_away(2)
    send_away(3)
    def add_owed(n, q):
        landed(ow.at[span(q * 216, 216)], ow_r.at[n])
        part = span(g * 864 + q * 216, 216)
        un[part, :] = un[part, :] + ow[span(q * 216, 216), :]

    def finish(n):
        b = nth(g, n)
        landed(sb.at[(n * 2 + 1) * 216 : (n * 2 + 2) * 216], sb_r.at[n * 2 + 1])
        landed(xr.at[n * 216 : n * 216 + 216], xr_r.at[n])

        def group(t, carry):
            value = (
                un[span(b * 864 + g * 216 + t * 8, 8), :]
                + sb[span((n * 2 + 1) * 216 + t * 8, 8), :]
                + xr[span(n * 216 + t * 8, 8), :]
            )
            vec_out[pl.ds(t * 32 + b, 8, stride=4), :] = value
            return carry

        lax.fori_loop(0, 27, group, 0)

    add_owed(0, cs)
    pass_on[0].start()
    pass_on[2].start()
    add_owed(1, c)
    send_away(0)
    send_away(1)
    add_owed(2, s)
    pass_on[1].start()
    pass_on[3].start()
    landed(obuf.at[0:216], zr.at[0])
    landed(obuf.at[0:216], zr.at[1])
    along[2].start()
    along[3].start()
    finish(2)
    finish(3)
    add_owed(3, g)
    finish(0)
    finish(1)
    vec3, w = vec_out.reshape(216, 4, 128), me % 8
    slice_copy(vec3, (w + 4) % 8, relay, 0, vs, relay_r, me, c, (w + RELAY) % 8).start()
    scatter_slices(vec3, vbuf, 0, vs, vr, me, g, ((1, 4), (5, 8), (0, 1)))
    landed(relay, relay_r)
    onward = slice_copy(relay, 0, vbuf, (w + 8 - RELAY) % 8 * 27, onward_s, onward_r, me, g, (w + RELAY) % 8)
    onward.start()
    landed(obuf.at[0:108], zr.at[2])
    landed(obuf.at[0:108], zr.at[3])
    lay_orbitals(obuf, line, bh, bl)
    landed(vbuf.at[0:189], vr)
    landed(relay, onward_r)
    margin_tail(me, g, m_out, vbuf, bh, bl, mt8, red, rs, rr)
    landed(vbuf, os)
    landed(vbuf, vs)
    for copy in cross + fwd + sib + back + pass_on + away + along + [onward]:
        copy.wait_send()
    landed(on, low_s)


def on_device(orbitals):
    nb = lax.axis_size("band")
    mine = orbitals.reshape(4, 216, 128).transpose(1, 0, 2).reshape(864, 128)
    vm = pl.BlockSpec(memory_space=pltpu.VMEM)
    hbm = pl.BlockSpec(memory_space=pl.ANY)
    dma = pltpu.SemaphoreType.DMA
    w, v, wt, hx, k = tables()

    def f32(*shape):
        return pltpu.VMEM(shape, F32)

    def b16(*shape):
        return pltpu.VMEM(shape, BF)

    vec, margin = pl.pallas_call(
        functools.partial(whole_kernel, nb),
        out_shape=(jax.ShapeDtypeStruct((864, 128), F32), jax.ShapeDtypeStruct((4, 32), F32)),
        in_specs=[vm] + [hbm] * 5,
        out_specs=(vm, vm),
        scratch_shapes=[b16(1152, 384), b16(1152, 384), b16(1152, 384), b16(96, 96), f32(288, 384)]
        + [f32(3456, 128), f32(864, 128), f32(5, 288, 384), f32(5, 288, 384)]
        + [f32(3456, 128), f32(864, 128), f32(864, 128), f32(1728, 128), f32(864, 128)]
        + [f32(864, 4, 128), f32(216, 4, 128), f32(256, 128), b16(1792, 256), b16(1792, 256), f32(256, 128), f32(256, 128)]
        + [dma((8,)), dma((4,)), dma((4,)), dma((4,)), dma((4,)), dma((4,)), dma((4,)), dma, dma]
        + [dma((4,)), dma((4,)), dma((8,)), dma((8,)), dma((4,)), dma((4,))]
        + [dma] * 4
        + [dma((4,)), dma((4,)), dma, dma]
        + [b16(288, 768), f32(288, 384), b16(576, 768)] * 3
        + [f32(27, 4, 128), dma, dma, dma],
        compiler_params=pltpu.CompilerParams(
            collective_id=3, has_side_effects=True, vmem_limit_bytes=60 * 1024 * 1024
        ),
    )(mine, w, v, wt, hx, k)
    return vec.reshape(216, 4, 128).transpose(1, 0, 2).reshape(4, 27648), margin.T


def solution(mesh):
    return jax.shard_map(
        on_device,
        mesh=mesh,
        in_specs=(P("band", "grid"),),
        out_specs=(P("band", "grid"), P("grid", "band")),
        check_vma=False,
    )
```

```python
import functools
import numpy as np
import jax
import jax.numpy as jnp
from jax import lax
from jax.experimental import pallas as pl
from jax.experimental.pallas import tpu as pltpu
from jax.sharding import PartitionSpec as P

NG = 48
NCELL = 110592
BF = jnp.bfloat16
F32 = jnp.float32


def split_np(a):
    hi = a.astype(BF)
    lo = (a - hi.astype(np.float64)).astype(BF)
    return hi, lo


def tables():
    n = np.arange(NG)
    ang = 2.0 * np.pi * ((n[:, None] * n[None, :]) % NG) / NG
    h = np.cos(ang) + np.sin(ang)
    w = np.zeros((8, NG, 6, 8, 8))
    for y in range(8):
        w[y, :, :, y, :] = h.reshape(NG, 6, 8)
    w = w.reshape(384, 384)
    v = np.kron(h, np.eye(8))
    f = ((n + 24) % 48 - 24).astype(np.float64)
    q = f[:, None, None] ** 2 + f[None, :, None] ** 2 + f[None, None, :] ** 2
    k = np.where(q > 0, 40.0 * (1.0 - np.exp(-q / 16.0)) / np.where(q > 0, q, 1.0), 0.0) / NCELL
    k = k.reshape(NG, NG, 6, 8).transpose(2, 0, 1, 3).reshape(288, 384)

    def pack(m):
        hi, lo = split_np(m)
        return np.concatenate([hi, lo], axis=0)

    hh, hl = split_np(h)
    hx = np.concatenate([np.concatenate([hh, hh], axis=1), np.concatenate([hl, np.zeros_like(hl)], axis=1)], axis=0)
    return pack(w), pack(v), pack(w.T.copy()), hx, k.astype(np.float32)


def hilo(x):
    hi = x.astype(BF)
    lo = (x - hi.astype(F32)).astype(BF)
    return hi, lo


def put(s_ref, row, rows, lane, x):
    hi, lo = hilo(x)
    n = x.shape[1]
    s_ref[row : row + rows, lane : lane + n] = hi
    s_ref[row : row + rows, 384 + lane : 384 + lane + n] = lo


def mm3(s_ref, w_ref):
    return jnp.dot(s_ref[...], w_ref[0:768, :], preferred_element_type=F32) + jnp.dot(
        s_ref[:, 0:384], w_ref[768:1152, :], preferred_element_type=F32
    )


def swap(t_ref, s_ref, left):
    for j in range(3):
        for m in range(3):
            r0, d0 = 2 * j * 48, 2 * m * 48
            e = t_ref[r0 : r0 + 48, 128 * m : 128 * m + 128]
            o = t_ref[r0 + 48 : r0 + 96, 128 * m : 128 * m + 128]
            put(s_ref, d0, 48, 128 * j, jnp.where(left, e, pltpu.roll(o, 64, 1)))
            put(s_ref, d0 + 48, 48, 128 * j, jnp.where(left, pltpu.roll(e, 64, 1), o))


def middle(s_ref, t_ref, r_ref, hx_ref, k_ref):
    def xdot(g, base):
        y = jnp.dot(hx_ref[...], r_ref[g * 192 + base : g * 192 + base + 96, :], preferred_element_type=F32)
        return y[0:48] + y[48:96]

    for g in range(3):
        for h in range(2):
            z = 2 * g + h
            hi, lo = hilo(t_ref[z * 48 : z * 48 + 48, :])
            r_ref[g * 192 : g * 192 + 48, h * 384 : h * 384 + 384] = hi
            r_ref[g * 192 + 48 : g * 192 + 96, h * 384 : h * 384 + 384] = lo
    for g in range(3):
        d = xdot(g, 0)
        for h in range(2):
            z = 2 * g + h
            hi, lo = hilo(d[:, h * 384 : h * 384 + 384] * k_ref[z * 48 : z * 48 + 48, :])
            r_ref[g * 192 + 96 : g * 192 + 144, h * 384 : h * 384 + 384] = hi
            r_ref[g * 192 + 144 : g * 192 + 192, h * 384 : h * 384 + 384] = lo
    for g in range(3):
        d = xdot(g, 96)
        for h in range(2):
            put(s_ref, (2 * g + h) * 48, 48, 0, d[:, h * 384 : h * 384 + 384])


def stages(s_ref, t_ref, r_ref, w_ref, v_ref, wt_ref, hx_ref, k_ref):
    left = lax.broadcasted_iota(jnp.int32, (48, 128), 1) < 64

    def mm(weights):
        def run():
            t_ref[...] = mm3(s_ref, weights)

        return run

    def turn():
        swap(t_ref, s_ref, left)

    def mid():
        middle(s_ref, t_ref, r_ref, hx_ref, k_ref)

    return [mm(w_ref), turn, mm(v_ref), mid, mm(v_ref), turn, mm(wt_ref)]


def potentials(sets, tables_, between=None):
    lists = [stages(*refs, *tables_) for refs in sets]
    count = len(lists[0])
    for n in range(count + len(lists) - 1):
        if n == 3 and between is not None:
            between()
        for p, steps in enumerate(lists):
            if 0 <= n - p < count:
                steps[n - p]()
MESH = pl.DeviceIdType.MESH
RELAY = 6


def rcopy(src, dst, send, recv, band, grid):
    return pltpu.make_async_remote_copy(
        src_ref=src, dst_ref=dst, send_sem=send, recv_sem=recv, device_id={"band": band, "grid": grid}, device_id_type=MESH
    )


def landed(ref, sem):
    pltpu.make_async_copy(ref, ref, sem).wait()


def greet(nb, me, g):
    barrier = pltpu.get_barrier_semaphore()
    plane, w = me // 8, me % 8

    def signal(band, grid):
        pl.semaphore_signal(barrier, inc=1, device_id={"band": band, "grid": grid}, device_id_type=MESH)

    def one(o, c):
        n = (w * 4 + g + o) % 32
        signal(plane * 8 + n // 4, n % 4)
        return c

    signal((me + 1) % nb, (g + 2) % 4)
    signal((me + nb - 1) % nb, (g + 2) % 4)
    lax.fori_loop(1, 32, one, 0)
    for o in range(1, 4):
        signal((me + 8 * o) % nb, g)
    pl.semaphore_wait(barrier, 36)


def span(start, size):
    return pl.ds(pl.multiple_of(start, 8), size)


def nth(g, n):
    return (n + 2 * (g // 2)) % 4


def slice_copy(src3, at, buf, rows, send, recv, me, g, w):
    part = src3.at[pl.ds(at * 27, 27)]
    return rcopy(part, buf.at[pl.ds(rows, 27)], send, recv, me // 8 * 8 + w, g)


def scatter_slices(src3, buf3, base, send, recv, me, g, steps):
    w = me % 8

    def one(o, c):
        dst = (w + o) % 8
        slice_copy(src3, dst, buf3, base + w * 27, send, recv, me, (g + 2) % 4, dst).start()
        return c

    for first, last in steps:
        lax.fori_loop(first, last, one, 0)


def lay_orbitals(obuf, line, bh, bl):
    flat = obuf.reshape(3456, 128)

    def chunks(p, carry):
        for h in range(2):
            c = jnp.minimum(2 * p + h, 26)
            for z in range(4):
                for b in range(4):
                    line[pl.ds(h * 128 + z * 32 + b, 8, stride=4), :] = flat[
                        pl.ds(z * 864 + c * 4 + b, 8, stride=108), :
                    ]
            hi, lo = hilo(line[h * 128 : h * 128 + 128, :])
            bh[span(p * 128, 128), h * 128 : h * 128 + 128] = hi
            bl[span(p * 128, 128), h * 128 : h * 128 + 128] = lo
        return carry

    lax.fori_loop(0, 14, chunks, 0)


def margin_tail(me, g, out_ref, vbuf, bh_ref, bl_ref, mt8, red, rs, rr):
    plane, w = me // 8, me % 8
    flat = vbuf.reshape(864, 128)
    m = jnp.zeros((32, 128), F32)
    dims = (((1,), (1,)), ((), ()))
    for p in range(14):
        parts = [
            jnp.concatenate([flat[pl.ds(c * 4 + b, 8, stride=108), :] for b in range(4)], axis=0)
            for c in range(2 * p, min(2 * p + 2, 27))
        ]
        ah, al = hilo(jnp.concatenate(parts, axis=1))
        width = 128 * len(parts)
        bh, bl = bh_ref[p * 128 : p * 128 + 128, 0:width], bl_ref[p * 128 : p * 128 + 128, 0:width]
        both = lax.dot_general(jnp.concatenate([ah, al], axis=0), bh, dims, preferred_element_type=F32)
        m = m + (
            both[0:32]
            + both[32:64]
            + lax.dot_general(ah, bl, dims, preferred_element_type=F32)
        )
    m = m * (1.0 / NCELL)
    lane = lax.broadcasted_iota(jnp.int32, (8, 128), 1) // 32
    for t in range(4):
        piece = jnp.zeros((8, 128), F32)
        for b in range(4):
            row = m[b * 8 : b * 8 + 8, :]
            turn = 32 * ((b - t) % 4)
            piece = jnp.where(lane == b, pltpu.roll(row, turn, 1) if turn else row, piece)
        mt8[pl.ds(t * 64, 8, stride=8), :] = piece
    here = (g * 8 + w) * 8

    def one(o, c):
        n = (w * 4 + g + o) % 32
        dst, to = n // 4, n % 4
        rcopy(mt8.at[span((to * 8 + dst) * 8, 8)], red.at[span(here, 8)], rs, rr, plane * 8 + dst, to).start()
        return c

    lax.fori_loop(1, 32, one, 0)
    red[span(here, 8), :] = mt8[span(here, 8), :]
    landed(red.at[0 : 31 * 8], rr)
    total = jnp.sum(red[pl.ds(0, 32, stride=8), :], axis=0, keepdims=True)
    for b in range(4):
        out_ref[b : b + 1, :] = total[:, b * 32 : b * 32 + 32]
    landed(mt8.at[0 : 31 * 8], rs)


OWN_I = ((0, 0, 1), (0, 1, 0), (2, 2, 3), (2, 3, 2))
OWN_J = ((0, 2, 1), (1, 3, 0), (2, 1, 3), (3, 0, 2))


def chosen(g, values):
    total = 0
    for t, value in enumerate(values):
        total = total + jnp.where(g == t, value, 0)
    return total


def whole_kernel(nb, mine_hbm, w_hbm, v_hbm, wt_hbm, hx_hbm, k_hbm, vec_hbm, m_out, *scratch):
    (w_ref, v_ref, wt_ref, hx_ref, k_ref, own, low, a_ref, u_ref, un, on, ow, sb, xr) = scratch[:14]
    (obuf, vbuf, line, bh, bl, mt8, red, tab, sib_s, sib_r, cross_s, cross_r, fwd_s, fwd_r) = scratch[14:28]
    relay, relay_r, onward_s, onward_r, mine, vec_out, edge = scratch[53:]
    (low_s, low_r, ow_s, ow_r, sb_s, sb_r, xr_s, xr_r, os, orr, vs, vr, zs, zr, rs, rr) = scratch[28:44]
    sets = [scratch[44 + 3 * p : 47 + 3 * p] for p in range(3)]
    shared = (w_ref, v_ref, wt_ref, hx_ref, k_ref)
    me, g = lax.axis_index("band"), lax.axis_index("grid")
    c, s = (g + 2) % 4, g + 1 - 2 * (g % 2)
    cs = (s + 2) % 4
    up, down = (me + 1) % nb, (me + nb - 1) % nb
    begin = pltpu.make_async_copy(mine_hbm, mine, edge.at[0])
    begin.start()
    loads = []
    for n, (a, b) in enumerate(((w_hbm, w_ref), (v_hbm, v_ref), (wt_hbm, wt_ref))):
        loads.append(pltpu.make_async_copy(a.at[0:384], b.at[0:384], tab.at[2 * n]))
        loads.append(pltpu.make_async_copy(a, b.at[384:1152], tab.at[2 * n + 1]))
    loads.append(pltpu.make_async_copy(hx_hbm, hx_ref, tab.at[6]))
    loads.append(pltpu.make_async_copy(k_hbm, k_ref, tab.at[7]))
    for copy in loads:
        copy.start()
    greet(nb, me, g)
    begin.wait()

    mine3 = mine.reshape(216, 4, 128)

    def cells(ref, b, q):
        return ref.at[span(b * 864 + q * 216, 216)]

    cross = []
    for n in range(4):
        b = nth(c, n)
        cross.append(rcopy(mine3.at[:, b, :], cells(own, b, g), cross_s.at[n], cross_r.at[n], me, c))
        cross[n].start()
    sib = []
    for b in range(4):
        sib.append(rcopy(mine3.at[:, b, :], cells(own, b, g), sib_s.at[b], sib_r.at[b], me, s))
        sib[b].start()
    rcopy(mine3.at[:, g, :], low.at[span(g * 216, 216)], low_s, low_r, up, c).start()

    def spread(t, carry):
        for b in range(4):
            own[span(b * 864 + g * 216 + t * 8, 8), :] = mine[pl.ds(t * 32 + b, 8, stride=4), :]
        return carry

    lax.fori_loop(0, 27, spread, 0)

    def low_part(q):
        rcopy(cells(own, g, q), low.at[span(q * 216, 216)], low_s, low_r, up, c).start()

    for b in range(4):
        landed(cells(own, b, s), sib_r.at[b])
    low_part(s)
    fwd = [
        rcopy(cells(own, nth(g, n), c), cells(own, nth(g, n), c), fwd_s.at[n], fwd_r.at[n], me, s) for n in range(4)
    ]

    def crossed(n):
        landed(cells(own, nth(g, n), c), cross_r.at[n])
        fwd[n].start()

    def forwarded(n):
        landed(cells(own, nth(g, n), cs), fwd_r.at[n])

    def spread_low(n):
        @pl.when(g % 2 == n)
        def _():
            low_part(c)

    def spread_low2(n):
        @pl.when(g % 2 == n)
        def _():
            low_part(cs)

    for n in range(2):
        crossed(n)
        spread_low(n)
    for n in range(2):
        forwarded(n)
        spread_low2(n)
    u_ref[...] = jnp.zeros_like(u_ref)
    for copy in loads:
        copy.wait()

    def lay(slot, src, base):
        for r in range(18):
            for xg in range(6):
                row, lane = (r // 3) * 48 + xg * 8, (r % 3) * 128
                a_ref[slot, row : row + 8, lane : lane + 128] = src[pl.ds(base + xg * 144 + r, 8, stride=18), :]

    def unlay(slot, dst, base):
        for r in range(18):
            for xg in range(6):
                row, lane = (r // 3) * 48 + xg * 8, (r % 3) * 128
                dst[pl.ds(base + xg * 144 + r, 8, stride=18), :] = u_ref[slot, row : row + 8, lane : lane + 128]

    def lay_band(n):
        b = nth(g, n)
        lay(b, own, b * 864)

    def unlay_band(n):
        b = nth(g, n)
        unlay(b, un, b * 864)

    lay_band(0)
    lay_band(1)

    back = [
        rcopy(on.at[span(q * 216, 216)], ow.at[span(q * 216, 216)], ow_s.at[n], ow_r.at[n], down, c)
        for n, q in enumerate((s, g, cs, c))
    ]
    pass_on = []
    for n in range(4):
        for h, q in enumerate((cs, s)):
            at = n * 2 + h
            pass_on.append(
                rcopy(cells(un, nth(g, n), q), sb.at[at * 216 : at * 216 + 216], sb_s.at[at], sb_r.at[at], me, s)
            )
    away = [
        rcopy(cells(un, nth(g, n), c), xr.at[(n ^ 2) * 216 : (n ^ 2) * 216 + 216], xr_s.at[n], xr_r.at[n ^ 2], me, c)
        for n in range(4)
    ]

    def send_away(n):
        at = n * 2
        landed(sb.at[at * 216 : at * 216 + 216], sb_r.at[at])
        part = span(nth(g, n) * 864 + c * 216, 216)
        un[part, :] = un[part, :] + sb[at * 216 : at * 216 + 216, :]
        away[n].start()

    plane = me // 8
    above, below = (me + 8) % nb, (me + nb - 8) % nb
    pd = (plane + 3) % 4
    along = []
    for n, (rows, to) in enumerate(
        (
            (pl.ds(plane * 216, 216), above),
            (pl.ds(plane * 216, 216), below),
            (pl.ds(pd * 216, 216), above),
        )
    ):
        along.append(rcopy(obuf.at[rows], obuf.at[rows], zs.at[n], zr.at[n], to, g))

    def own_slot(slot):
        return chosen(g, [row[slot] for row in OWN_I]), chosen(g, [row[slot] for row in OWN_J])

    def own_slot(slot):
        return chosen(g, [row[slot] for row in OWN_I]), chosen(g, [row[slot] for row in OWN_J])

    def pass_orbitals():
        landed(obuf.at[0:216], orr)
        along[0].start()

        @pl.when(me % 8 < 6)
        def _():
            along[1].start()

    def step(n, carry):
        @pl.when(n == 1)
        def _():
            scatter_slices(mine3, obuf, plane * 216, os, orr, me, g, ((0, 8),))
            crossed(2)
            crossed(3)
            landed(low, low_r)
            lay(4, low, 0)

        @pl.when(n == 2)
        def _():
            forwarded(2)
            forwarded(3)
            lay_band(2)
            lay_band(3)

        pairs = []
        for p, slot in ((0, 0), (1, 2)):
            i, j = own_slot(slot)
            weight = jnp.where((n == 0) & (p == 1) & (g % 2 == 1), 0.0, 1.0)
            i, j = jnp.where(n == 0, i, nth(g, 2 * n - 2 + p)), jnp.where(n == 0, j, 4)
            pairs.append((i, j, weight, jnp.where(i == j, 0.0, weight)))
        for p, (i, j, _, _) in enumerate(pairs):
            put(sets[p][0], 0, 288, 0, a_ref[i] * a_ref[j])

        potentials(sets[:2], shared)
        for p, (i, j, one, two) in enumerate(pairs):
            t = sets[p][1][...]
            u_ref[i] = u_ref[i] - one * a_ref[j] * t
            u_ref[j] = u_ref[j] - two * a_ref[i] * t
        return carry

    lax.fori_loop(0, 3, step, 0)

    unlay(4, on, 0)
    for copy in back:
        copy.start()
    pass_orbitals()
    i, j = own_slot(1)
    put(sets[0][0], 0, 288, 0, a_ref[i] * a_ref[j])
    potentials(sets[:1], shared)
    t = sets[0][1][...]
    u_ref[i] = u_ref[i] - a_ref[j] * t
    u_ref[j] = u_ref[j] - a_ref[i] * t
    for n in (2, 3):
        unlay_band(n)
        pass_on[2 * n].start()
        pass_on[2 * n + 1].start()
    for n in (0, 1):
        unlay_band(n)
    send_away(2)
    send_away(3)

    def add_owed(n, q):
        landed(ow.at[span(q * 216, 216)], ow_r.at[n])
        part = span(g * 864 + q * 216, 216)
        un[part, :] = un[part, :] + ow[span(q * 216, 216), :]

    def finish(n):
        b = nth(g, n)
        landed(sb.at[(n * 2 + 1) * 216 : (n * 2 + 2) * 216], sb_r.at[n * 2 + 1])
        landed(xr.at[n * 216 : n * 216 + 216], xr_r.at[n])

        def group(t, carry):
            value = (
                un[span(b * 864 + g * 216 + t * 8, 8), :]
                + sb[span((n * 2 + 1) * 216 + t * 8, 8), :]
                + xr[span(n * 216 + t * 8, 8), :]
            )
            vec_out[pl.ds(t * 32 + b, 8, stride=4), :] = value
            return carry

        lax.fori_loop(0, 27, group, 0)

    add_owed(0, cs)
    pass_on[0].start()
    pass_on[2].start()
    add_owed(1, c)
    send_away(0)
    send_away(1)
    add_owed(2, s)

    @pl.when(me % 8 >= 6)
    def _():
        along[1].start()

    pass_on[1].start()
    pass_on[3].start()
    landed(obuf.at[0:216], zr.at[0])
    along[2].start()
    finish(2)
    finish(3)
    add_owed(3, g)
    finish(0)
    finish(1)
    keep = pltpu.make_async_copy(vec_out, vec_hbm, edge.at[1])
    vec3, w = vec_out.reshape(216, 4, 128), me % 8
    slice_copy(vec3, (w + 4) % 8, relay, 0, vs, relay_r, me, c, (w + RELAY) % 8).start()
    scatter_slices(vec3, vbuf, 0, vs, vr, me, g, ((1, 4), (5, 8), (0, 1)))
    landed(relay, relay_r)
    onward = slice_copy(relay, 0, vbuf, (w + 8 - RELAY) % 8 * 27, onward_s, onward_r, me, g, (w + RELAY) % 8)
    onward.start()
    keep.start()
    landed(obuf.at[0:216], zr.at[1])
    landed(obuf.at[0:216], zr.at[2])
    lay_orbitals(obuf, line, bh, bl)
    landed(vbuf.at[0:189], vr)
    landed(relay, onward_r)
    margin_tail(me, g, m_out, vbuf, bh, bl, mt8, red, rs, rr)
    landed(vbuf, os)
    landed(vbuf, vs)
    for copy in cross + fwd + sib + back + pass_on + away + along + [onward]:
        copy.wait_send()
    landed(on, low_s)
    keep.wait()


def on_device(orbitals):
    nb = lax.axis_size("band")
    mine = orbitals.reshape(4, 216, 128).transpose(1, 0, 2).reshape(864, 128)
    vm = pl.BlockSpec(memory_space=pltpu.VMEM)
    hbm = pl.BlockSpec(memory_space=pl.ANY)
    dma = pltpu.SemaphoreType.DMA
    w, v, wt, hx, k = tables()

    def f32(*shape):
        return pltpu.VMEM(shape, F32)

    def b16(*shape):
        return pltpu.VMEM(shape, BF)

    vec, margin = pl.pallas_call(
        functools.partial(whole_kernel, nb),
        out_shape=(jax.ShapeDtypeStruct((864, 128), F32), jax.ShapeDtypeStruct((4, 32), F32)),
        in_specs=[hbm] * 6,
        out_specs=(hbm, vm),
        scratch_shapes=[b16(1152, 384), b16(1152, 384), b16(1152, 384), b16(96, 96), f32(288, 384)]
        + [f32(3456, 128), f32(864, 128), f32(5, 288, 384), f32(5, 288, 384)]
        + [f32(3456, 128), f32(864, 128), f32(864, 128), f32(1728, 128), f32(864, 128)]
        + [f32(864, 4, 128), f32(216, 4, 128), f32(256, 128), b16(1792, 256), b16(1792, 256), f32(256, 128), f32(256, 128)]
        + [dma((8,)), dma((4,)), dma((4,)), dma((4,)), dma((4,)), dma((4,)), dma((4,)), dma, dma]
        + [dma((4,)), dma((4,)), dma((8,)), dma((8,)), dma((4,)), dma((4,))]
        + [dma] * 4
        + [dma((4,)), dma((4,)), dma, dma]
        + [b16(288, 768), f32(288, 384), b16(576, 768)] * 3
        + [f32(27, 4, 128), dma, dma, dma, f32(864, 128), f32(864, 128), dma((2,))],
        compiler_params=pltpu.CompilerParams(
            collective_id=3, has_side_effects=True, vmem_limit_bytes=60 * 1024 * 1024
        ),
    )(mine, w, v, wt, hx, k)
    return vec.reshape(216, 4, 128).transpose(1, 0, 2).reshape(4, 27648), margin.T


def solution(mesh):
    return jax.shard_map(
        on_device,
        mesh=mesh,
        in_specs=(P("band", "grid"),),
        out_specs=(P("band", "grid"), P("grid", "band")),
        check_vma=False,
    )
```

```python
import functools
import numpy as np
import jax
import jax.numpy as jnp
from jax import lax
from jax.experimental import pallas as pl
from jax.experimental.pallas import tpu as pltpu
from jax.sharding import PartitionSpec as P

NG = 48
NCELL = 110592
BF = jnp.bfloat16
F32 = jnp.float32


def split_np(a):
    hi = a.astype(BF)
    lo = (a - hi.astype(np.float64)).astype(BF)
    return hi, lo


def tables():
    n = np.arange(NG)
    ang = 2.0 * np.pi * ((n[:, None] * n[None, :]) % NG) / NG
    h = np.cos(ang) + np.sin(ang)
    w = np.zeros((8, NG, 6, 8, 8))
    for y in range(8):
        w[y, :, :, y, :] = h.reshape(NG, 6, 8)
    w = w.reshape(384, 384)
    v = np.kron(h, np.eye(8))
    f = ((n + 24) % 48 - 24).astype(np.float64)
    q = f[:, None, None] ** 2 + f[None, :, None] ** 2 + f[None, None, :] ** 2
    k = np.where(q > 0, 40.0 * (1.0 - np.exp(-q / 16.0)) / np.where(q > 0, q, 1.0), 0.0) / NCELL
    k = k.reshape(NG, NG, 6, 8).transpose(2, 0, 1, 3).reshape(288, 384)

    def pack(m):
        hi, lo = split_np(m)
        return np.concatenate([hi, lo], axis=0)

    hh, hl = split_np(h)
    hx = np.concatenate([np.concatenate([hh, hh], axis=1), np.concatenate([hl, np.zeros_like(hl)], axis=1)], axis=0)
    return pack(w), pack(v), pack(w.T.copy()), hx, k.astype(np.float32)


def hilo(x):
    hi = x.astype(BF)
    lo = (x - hi.astype(F32)).astype(BF)
    return hi, lo


def put(s_ref, row, rows, lane, x):
    hi, lo = hilo(x)
    n = x.shape[1]
    s_ref[row : row + rows, lane : lane + n] = hi
    s_ref[row : row + rows, 384 + lane : 384 + lane + n] = lo


def mm3(s_ref, w_ref):
    return jnp.dot(s_ref[...], w_ref[0:768, :], preferred_element_type=F32) + jnp.dot(
        s_ref[:, 0:384], w_ref[768:1152, :], preferred_element_type=F32
    )


def swap(t_ref, s_ref, left):
    for j in range(3):
        for m in range(3):
            r0, d0 = 2 * j * 48, 2 * m * 48
            e = t_ref[r0 : r0 + 48, 128 * m : 128 * m + 128]
            o = t_ref[r0 + 48 : r0 + 96, 128 * m : 128 * m + 128]
            put(s_ref, d0, 48, 128 * j, jnp.where(left, e, pltpu.roll(o, 64, 1)))
            put(s_ref, d0 + 48, 48, 128 * j, jnp.where(left, pltpu.roll(e, 64, 1), o))


def middle(s_ref, t_ref, r_ref, hx_ref, k_ref):
    def xdot(g, base):
        y = jnp.dot(hx_ref[...], r_ref[g * 192 + base : g * 192 + base + 96, :], preferred_element_type=F32)
        return y[0:48] + y[48:96]

    for g in range(3):
        for h in range(2):
            z = 2 * g + h
            hi, lo = hilo(t_ref[z * 48 : z * 48 + 48, :])
            r_ref[g * 192 : g * 192 + 48, h * 384 : h * 384 + 384] = hi
            r_ref[g * 192 + 48 : g * 192 + 96, h * 384 : h * 384 + 384] = lo
    for g in range(3):
        d = xdot(g, 0)
        for h in range(2):
            z = 2 * g + h
            hi, lo = hilo(d[:, h * 384 : h * 384 + 384] * k_ref[z * 48 : z * 48 + 48, :])
            r_ref[g * 192 + 96 : g * 192 + 144, h * 384 : h * 384 + 384] = hi
            r_ref[g * 192 + 144 : g * 192 + 192, h * 384 : h * 384 + 384] = lo
    for g in range(3):
        d = xdot(g, 96)
        for h in range(2):
            put(s_ref, (2 * g + h) * 48, 48, 0, d[:, h * 384 : h * 384 + 384])


def stages(s_ref, t_ref, r_ref, w_ref, v_ref, wt_ref, hx_ref, k_ref):
    left = lax.broadcasted_iota(jnp.int32, (48, 128), 1) < 64

    def mm(weights):
        def run():
            t_ref[...] = mm3(s_ref, weights)

        return run

    def turn():
        swap(t_ref, s_ref, left)

    def mid():
        middle(s_ref, t_ref, r_ref, hx_ref, k_ref)

    return [mm(w_ref), turn, mm(v_ref), mid, mm(v_ref), turn, mm(wt_ref)]


def potentials(sets, tables_, between=None):
    lists = [stages(*refs, *tables_) for refs in sets]
    count = len(lists[0])
    for n in range(count + len(lists) - 1):
        if n == 3 and between is not None:
            between()
        for p, steps in enumerate(lists):
            if 0 <= n - p < count:
                steps[n - p]()
MESH = pl.DeviceIdType.MESH
RELAY = 6


def rcopy(src, dst, send, recv, band, grid):
    return pltpu.make_async_remote_copy(
        src_ref=src, dst_ref=dst, send_sem=send, recv_sem=recv, device_id={"band": band, "grid": grid}, device_id_type=MESH
    )


def landed(ref, sem):
    pltpu.make_async_copy(ref, ref, sem).wait()


def greet(nb, me, g):
    barrier = pltpu.get_barrier_semaphore()
    plane, w = me // 8, me % 8

    def signal(band, grid):
        pl.semaphore_signal(barrier, inc=1, device_id={"band": band, "grid": grid}, device_id_type=MESH)

    def one(o, c):
        n = (w * 4 + g + o) % 32
        signal(plane * 8 + n // 4, n % 4)
        return c

    signal((me + 1) % nb, (g + 2) % 4)
    signal((me + nb - 1) % nb, (g + 2) % 4)
    lax.fori_loop(1, 32, one, 0)
    for o in range(1, 4):
        signal((me + 8 * o) % nb, g)
    pl.semaphore_wait(barrier, 36)


def span(start, size):
    return pl.ds(pl.multiple_of(start, 8), size)


def nth(g, n):
    return (n + 2 * (g // 2)) % 4


def half_of(w):
    return (w // 2 + w) % 2


def slice_copy(src3, to, buf, rows, send, recv, me, g, w):
    part = src3.at[pl.ds((to // 2 + 4 * half_of(to)) * 27, 27)]
    return rcopy(part, buf.at[pl.ds(rows, 27)], send, recv, me // 8 * 8 + w, g)


def scatter_slices(src3, buf3, base, send, recv, me, g, steps, half=None):
    w = me % 8

    def one(o, c):
        dst = (w + o) % 8

        @pl.when(True if half is None else half_of(dst) == half)
        def _():
            slice_copy(src3, dst, buf3, base + w * 27, send, recv, me, (g + 2) % 4, dst).start()

        return c

    for first, last in steps:
        lax.fori_loop(first, last, one, 0)


def lay_orbitals(obuf, line, bh, bl):
    flat = obuf.reshape(3456, 128)

    def chunks(p, carry):
        for h in range(2):
            c = jnp.minimum(2 * p + h, 26)
            for z in range(4):
                for b in range(4):
                    line[pl.ds(h * 128 + z * 32 + b, 8, stride=4), :] = flat[
                        pl.ds(z * 864 + c * 4 + b, 8, stride=108), :
                    ]
            hi, lo = hilo(line[h * 128 : h * 128 + 128, :])
            bh[span(p * 128, 128), h * 128 : h * 128 + 128] = hi
            bl[span(p * 128, 128), h * 128 : h * 128 + 128] = lo
        return carry

    lax.fori_loop(0, 14, chunks, 0)


def margin_tail(me, g, out_ref, vbuf, bh_ref, bl_ref, mt8, red, rs, rr):
    plane, w = me // 8, me % 8
    flat = vbuf.reshape(864, 128)
    m = jnp.zeros((32, 128), F32)
    dims = (((1,), (1,)), ((), ()))
    for p in range(14):
        parts = [
            jnp.concatenate([flat[pl.ds(c * 4 + b, 8, stride=108), :] for b in range(4)], axis=0)
            for c in range(2 * p, min(2 * p + 2, 27))
        ]
        ah, al = hilo(jnp.concatenate(parts, axis=1))
        width = 128 * len(parts)
        bh, bl = bh_ref[p * 128 : p * 128 + 128, 0:width], bl_ref[p * 128 : p * 128 + 128, 0:width]
        both = lax.dot_general(jnp.concatenate([ah, al], axis=0), bh, dims, preferred_element_type=F32)
        m = m + (
            both[0:32]
            + both[32:64]
            + lax.dot_general(ah, bl, dims, preferred_element_type=F32)
        )
    m = m * (1.0 / NCELL)
    lane = lax.broadcasted_iota(jnp.int32, (8, 128), 1) // 32
    for t in range(4):
        piece = jnp.zeros((8, 128), F32)
        for b in range(4):
            row = m[b * 8 : b * 8 + 8, :]
            turn = 32 * ((b - t) % 4)
            piece = jnp.where(lane == b, pltpu.roll(row, turn, 1) if turn else row, piece)
        mt8[pl.ds(t * 64, 8, stride=8), :] = piece
    here = (g * 8 + w) * 8

    def one(o, c):
        n = (w * 4 + g + o) % 32
        dst, to = n // 4, n % 4
        rcopy(mt8.at[span((to * 8 + dst) * 8, 8)], red.at[span(here, 8)], rs, rr, plane * 8 + dst, to).start()
        return c

    for first, last in ((12, 21), (1, 12), (21, 32)):
        lax.fori_loop(first, last, one, 0)
    red[span(here, 8), :] = mt8[span(here, 8), :]
    landed(red.at[0 : 31 * 8], rr)
    total = jnp.sum(red[pl.ds(0, 32, stride=8), :], axis=0, keepdims=True)
    for b in range(4):
        out_ref[b : b + 1, :] = total[:, b * 32 : b * 32 + 32]
    landed(mt8.at[0 : 31 * 8], rs)


OWN_I = ((0, 0, 1), (0, 1, 0), (2, 2, 3), (2, 3, 2))
OWN_J = ((0, 2, 1), (1, 3, 0), (2, 1, 3), (3, 0, 2))


def chosen(g, values):
    total = 0
    for t, value in enumerate(values):
        total = total + jnp.where(g == t, value, 0)
    return total


def whole_kernel(nb, mine_hbm, w_hbm, v_hbm, wt_hbm, hx_hbm, k_hbm, vec_hbm, m_out, *scratch):
    (w_ref, v_ref, wt_ref, hx_ref, k_ref, own, low, a_ref, u_ref, un, on, ow, sb, xr) = scratch[:14]
    (obuf, vbuf, line, bh, bl, mt8, red, tab, sib_s, sib_r, cross_s, cross_r, fwd_s, fwd_r) = scratch[14:28]
    relay, relay_r, onward_s, onward_r, mine, vec_out, edge = scratch[53:]
    (low_s, low_r, ow_s, ow_r, sb_s, sb_r, xr_s, xr_r, os, orr, vs, vr, zs, zr, rs, rr) = scratch[28:44]
    sets = [scratch[44 + 3 * p : 47 + 3 * p] for p in range(3)]
    shared = (w_ref, v_ref, wt_ref, hx_ref, k_ref)
    me, g = lax.axis_index("band"), lax.axis_index("grid")
    c, s = (g + 2) % 4, g + 1 - 2 * (g % 2)
    cs = (s + 2) % 4
    up, down = (me + 1) % nb, (me + nb - 1) % nb
    begin = pltpu.make_async_copy(mine_hbm, mine, edge.at[0])
    begin.start()
    loads = []
    for n, (a, b) in enumerate(((w_hbm, w_ref), (v_hbm, v_ref), (wt_hbm, wt_ref))):
        loads.append(pltpu.make_async_copy(a.at[0:384], b.at[0:384], tab.at[2 * n]))
        loads.append(pltpu.make_async_copy(a, b.at[384:1152], tab.at[2 * n + 1]))
    loads.append(pltpu.make_async_copy(hx_hbm, hx_ref, tab.at[6]))
    loads.append(pltpu.make_async_copy(k_hbm, k_ref, tab.at[7]))
    for copy in loads:
        copy.start()
    greet(nb, me, g)
    begin.wait()

    mine3 = mine.reshape(216, 4, 128)

    def cells(ref, b, q):
        return ref.at[span(b * 864 + q * 216, 216)]

    cross = []
    for n in range(4):
        b = nth(c, n)
        cross.append(rcopy(mine3.at[:, b, :], cells(own, b, g), cross_s.at[n], cross_r.at[n], me, c))
        cross[n].start()
    sib = []
    for b in range(4):
        sib.append(rcopy(mine3.at[:, b, :], cells(own, b, g), sib_s.at[b], sib_r.at[b], me, s))
        sib[b].start()
    rcopy(mine3.at[:, g, :], low.at[span(g * 216, 216)], low_s, low_r, up, c).start()

    def spread(t, carry):
        for b in range(4):
            own[span(b * 864 + g * 216 + t * 8, 8), :] = mine[pl.ds(t * 32 + b, 8, stride=4), :]
        return carry

    lax.fori_loop(0, 27, spread, 0)

    def low_part(q):
        rcopy(cells(own, g, q), low.at[span(q * 216, 216)], low_s, low_r, up, c).start()

    for b in range(4):
        landed(cells(own, b, s), sib_r.at[b])
    low_part(s)
    fwd = [
        rcopy(cells(own, nth(g, n), c), cells(own, nth(g, n), c), fwd_s.at[n], fwd_r.at[n], me, s) for n in range(4)
    ]

    def crossed(n):
        landed(cells(own, nth(g, n), c), cross_r.at[n])
        fwd[n].start()

    def forwarded(n):
        landed(cells(own, nth(g, n), cs), fwd_r.at[n])

    def spread_low(n):
        @pl.when(g % 2 == n)
        def _():
            low_part(c)

    def spread_low2(n):
        @pl.when(g % 2 == n)
        def _():
            low_part(cs)

    for n in range(2):
        crossed(n)
        spread_low(n)
    for n in range(2):
        forwarded(n)
        spread_low2(n)
    u_ref[...] = jnp.zeros_like(u_ref)
    for copy in loads:
        copy.wait()

    def lay(slot, src, base):
        for r in range(18):
            for xg in range(6):
                row, lane = (r // 3) * 48 + xg * 8, (r % 3) * 128
                a_ref[slot, row : row + 8, lane : lane + 128] = src[pl.ds(base + xg * 144 + r, 8, stride=18), :]

    def unlay(slot, dst, base):
        for r in range(18):
            for xg in range(6):
                row, lane = (r // 3) * 48 + xg * 8, (r % 3) * 128
                dst[pl.ds(base + xg * 144 + r, 8, stride=18), :] = u_ref[slot, row : row + 8, lane : lane + 128]

    def lay_band(n):
        b = nth(g, n)
        lay(b, own, b * 864)

    def unlay_band(n):
        b = nth(g, n)
        unlay(b, un, b * 864)

    lay_band(0)
    lay_band(1)

    back = [
        rcopy(on.at[span(q * 216, 216)], ow.at[span(q * 216, 216)], ow_s.at[n], ow_r.at[n], down, c)
        for n, q in enumerate((s, g, cs, c))
    ]
    pass_on = []
    for n in range(4):
        for h, q in enumerate((cs, s)):
            at = n * 2 + h
            pass_on.append(
                rcopy(cells(un, nth(g, n), q), sb.at[at * 216 : at * 216 + 216], sb_s.at[at], sb_r.at[at], me, s)
            )
    def away_copy(n, first, size, sem):
        b, at = nth(g, n), (n ^ 2) * 216 + first
        src = un.at[span(b * 864 + c * 216 + first, size)]
        return rcopy(src, xr.at[at : at + size], xr_s.at[sem], xr_r.at[sem ^ 2], me, c)

    late = {(n, h): away_copy(n, 112 * h, 112 - 8 * h, n + 4 * h) for n in (0, 1) for h in range(2)}
    away = {n: away_copy(n, 0, 216, n) for n in (2, 3)}

    def gathered(n, first, size):
        at = n * 432 + first
        part = span(nth(g, n) * 864 + c * 216 + first, size)
        un[part, :] = un[part, :] + sb[at : at + size, :]

    def send_away(n):
        landed(sb.at[n * 432 : n * 432 + 216], sb_r.at[2 * n])
        gathered(n, 0, 216)
        away[n].start()

    def send_away_part(n, h):
        if h == 0:
            landed(sb.at[n * 432 : n * 432 + 216], sb_r.at[2 * n])
        gathered(n, 112 * h, 112 - 8 * h)
        late[n, h].start()

    plane = me // 8
    above, below = (me + 8) % nb, (me + nb - 8) % nb
    pu, pd = (plane + 1) % 4, (plane + 3) % 4
    along = []
    for n, (first, size, to) in enumerate(
        (
            (plane * 216, 108, above),
            (plane * 216 + 108, 108, above),
            (plane * 216, 216, below),
            (pd * 216, 108, above),
            (pd * 216 + 108, 108, above),
            (pu * 216 + 108, 108, below),
        )
    ):
        rows = obuf.at[pl.ds(first, size)]
        along.append(rcopy(rows, rows, zs.at[min(n, 4)], zr.at[min(n, 4)], to, g))
    last_row = me % 8 >= 6
    not_last = me % 8 < 6

    def own_slot(slot):
        return chosen(g, [row[slot] for row in OWN_I]), chosen(g, [row[slot] for row in OWN_J])

    def own_slot(slot):
        return chosen(g, [row[slot] for row in OWN_I]), chosen(g, [row[slot] for row in OWN_J])

    def pass_orbitals():
        landed(obuf.at[0:216], orr)
        along[0].start()
        along[1].start()

        @pl.when(not_last)
        def _():
            along[2].start()

    def step(n, carry):
        @pl.when(n == 1)
        def _():
            scatter_slices(mine3, obuf, plane * 216, os, orr, me, g, ((0, 8),))
            crossed(2)
            crossed(3)
            landed(low, low_r)
            lay(4, low, 0)

        @pl.when(n == 2)
        def _():
            forwarded(2)
            forwarded(3)
            lay_band(2)
            lay_band(3)

        pairs = []
        for p, slot in ((0, 0), (1, 2)):
            i, j = own_slot(slot)
            weight = jnp.where((n == 0) & (p == 1) & (g % 2 == 1), 0.0, 1.0)
            i, j = jnp.where(n == 0, i, nth(g, 2 * n - 2 + p)), jnp.where(n == 0, j, 4)
            pairs.append((i, j, weight, jnp.where(i == j, 0.0, weight)))
        for p, (i, j, _, _) in enumerate(pairs):
            put(sets[p][0], 0, 288, 0, a_ref[i] * a_ref[j])

        potentials(sets[:2], shared)
        for p, (i, j, one, two) in enumerate(pairs):
            t = sets[p][1][...]
            u_ref[i] = u_ref[i] - one * a_ref[j] * t
            u_ref[j] = u_ref[j] - two * a_ref[i] * t
        return carry

    lax.fori_loop(0, 3, step, 0)

    unlay(4, on, 0)
    for copy in back:
        copy.start()
    pass_orbitals()
    i, j = own_slot(1)
    put(sets[0][0], 0, 288, 0, a_ref[i] * a_ref[j])
    potentials(sets[:1], shared)
    t = sets[0][1][...]
    u_ref[i] = u_ref[i] - a_ref[j] * t
    u_ref[j] = u_ref[j] - a_ref[i] * t
    for n in (2, 3):
        unlay_band(n)
        pass_on[2 * n].start()
        pass_on[2 * n + 1].start()
    for n in (0, 1):
        unlay_band(n)
    send_away(2)
    send_away(3)

    def add_owed(n, q):
        landed(ow.at[span(q * 216, 216)], ow_r.at[n])
        part = span(g * 864 + q * 216, 216)
        un[part, :] = un[part, :] + ow[span(q * 216, 216), :]

    def finish(n, first, last):
        b = nth(g, n)

        def group(t, carry):
            value = (
                un[span(b * 864 + g * 216 + t * 8, 8), :]
                + sb[span((n * 2 + 1) * 216 + t * 8, 8), :]
                + xr[span(n * 216 + t * 8, 8), :]
            )
            vec_out[pl.ds(t * 32 + b, 8, stride=4), :] = value
            return carry

        lax.fori_loop(first, last, group, 0)

    add_owed(0, cs)
    pass_on[0].start()
    pass_on[2].start()
    add_owed(1, c)
    for h in range(2):
        for n in (0, 1):
            send_away_part(n, h)
    landed(obuf.at[0:108], zr.at[0])
    along[3].start()
    add_owed(2, s)
    pass_on[1].start()
    pass_on[3].start()

    @pl.when(last_row)
    def _():
        along[2].start()
        landed(obuf.at[0:108], zr.at[1])
        along[4].start()

    @pl.when(not_last)
    def _():
        landed(obuf.at[0:108], zr.at[1])
        landed(obuf.at[0:216], zr.at[2])
        along[5].start()

    add_owed(3, g)
    for n in (0, 1):
        landed(sb.at[(n * 2 + 1) * 216 : (n * 2 + 2) * 216], sb_r.at[n * 2 + 1])
        landed(xr.at[n * 216 : n * 216 + 216], xr_r.at[n])
        finish(n, 0, 27)
    for n in (2, 3):
        landed(sb.at[(n * 2 + 1) * 216 : (n * 2 + 2) * 216], sb_r.at[n * 2 + 1])
    keep = pltpu.make_async_copy(vec_out, vec_hbm, edge.at[1])
    vec3, w = vec_out.reshape(216, 4, 128), me % 8
    around = slice_copy(vec3, (w + 4) % 8, relay, 0, vs, relay_r, me, c, (w + RELAY) % 8)
    for h in range(2):
        for n in (2, 3):
            at = n * 216 + h * 112
            landed(xr.at[at : at + 112 - 8 * h], xr_r.at[n + 4 * h])
            finish(n, 14 * h, 14 + 13 * h)

        @pl.when(half_of(w) == h)
        def _():
            around.start()

        scatter_slices(vec3, vbuf, 0, vs, vr, me, g, ((3, 4), (5, 6), (1, 3), (6, 8), (0, 1)), h)
    landed(relay, relay_r)
    onward = slice_copy(relay, 0, vbuf, (w + 8 - RELAY) % 8 * 27, onward_s, onward_r, me, g, (w + RELAY) % 8)
    onward.start()
    keep.start()

    @pl.when(last_row)
    def _():
        landed(obuf.at[0:216], zr.at[2])

    landed(obuf.at[0:108], zr.at[3])
    landed(obuf.at[0:108], zr.at[4])
    lay_orbitals(obuf, line, bh, bl)
    landed(vbuf.at[0:189], vr)
    landed(relay, onward_r)
    margin_tail(me, g, m_out, vbuf, bh, bl, mt8, red, rs, rr)
    landed(vbuf, os)
    landed(vbuf, vs)
    for copy in cross + fwd + sib + back + pass_on + [*late.values(), *away.values()] + along[:5] + [onward]:
        copy.wait_send()
    landed(on, low_s)
    keep.wait()


def on_device(orbitals):
    nb = lax.axis_size("band")
    mine = orbitals.reshape(4, 216, 128).transpose(1, 0, 2).reshape(864, 128)
    vm = pl.BlockSpec(memory_space=pltpu.VMEM)
    hbm = pl.BlockSpec(memory_space=pl.ANY)
    dma = pltpu.SemaphoreType.DMA
    w, v, wt, hx, k = tables()

    def f32(*shape):
        return pltpu.VMEM(shape, F32)

    def b16(*shape):
        return pltpu.VMEM(shape, BF)

    vec, margin = pl.pallas_call(
        functools.partial(whole_kernel, nb),
        out_shape=(jax.ShapeDtypeStruct((864, 128), F32), jax.ShapeDtypeStruct((4, 32), F32)),
        in_specs=[hbm] * 6,
        out_specs=(hbm, vm),
        scratch_shapes=[b16(1152, 384), b16(1152, 384), b16(1152, 384), b16(96, 96), f32(288, 384)]
        + [f32(3456, 128), f32(864, 128), f32(5, 288, 384), f32(5, 288, 384)]
        + [f32(3456, 128), f32(864, 128), f32(864, 128), f32(1728, 128), f32(864, 128)]
        + [f32(864, 4, 128), f32(216, 4, 128), f32(256, 128), b16(1792, 256), b16(1792, 256), f32(256, 128), f32(256, 128)]
        + [dma((8,)), dma((4,)), dma((4,)), dma((4,)), dma((4,)), dma((4,)), dma((4,)), dma, dma]
        + [dma((4,)), dma((4,)), dma((8,)), dma((8,)), dma((8,)), dma((8,))]
        + [dma] * 4
        + [dma((5,)), dma((5,)), dma, dma]
        + [b16(288, 768), f32(288, 384), b16(576, 768)] * 3
        + [f32(27, 4, 128), dma, dma, dma, f32(864, 128), f32(864, 128), dma((2,))],
        compiler_params=pltpu.CompilerParams(
            collective_id=3, has_side_effects=True, vmem_limit_bytes=60 * 1024 * 1024
        ),
    )(mine, w, v, wt, hx, k)
    return vec.reshape(216, 4, 128).transpose(1, 0, 2).reshape(4, 27648), margin.T


def solution(mesh):
    return jax.shard_map(
        on_device,
        mesh=mesh,
        in_specs=(P("band", "grid"),),
        out_specs=(P("band", "grid"), P("grid", "band")),
        check_vma=False,
    )
```

```python
import functools
import numpy as np
import jax
import jax.numpy as jnp
from jax import lax
from jax.experimental import pallas as pl
from jax.experimental.pallas import tpu as pltpu
from jax.sharding import PartitionSpec as P

NG = 48
NCELL = 110592
BF = jnp.bfloat16
F32 = jnp.float32


def split_np(a):
    hi = a.astype(BF)
    lo = (a - hi.astype(np.float64)).astype(BF)
    return hi, lo


def tables():
    n = np.arange(NG)
    ang = 2.0 * np.pi * ((n[:, None] * n[None, :]) % NG) / NG
    h = np.cos(ang) + np.sin(ang)
    w = np.zeros((8, NG, 6, 8, 8))
    for y in range(8):
        w[y, :, :, y, :] = h.reshape(NG, 6, 8)
    w = w.reshape(384, 384)
    v = np.kron(h, np.eye(8))
    f = ((n + 24) % 48 - 24).astype(np.float64)
    q = f[:, None, None] ** 2 + f[None, :, None] ** 2 + f[None, None, :] ** 2
    k = np.where(q > 0, 40.0 * (1.0 - np.exp(-q / 16.0)) / np.where(q > 0, q, 1.0), 0.0) / NCELL
    k = k.reshape(NG, NG, 6, 8).transpose(2, 0, 1, 3).reshape(288, 384)

    def pack(m):
        hi, lo = split_np(m)
        return np.concatenate([hi, lo], axis=0)

    hh, hl = split_np(h)
    hx = np.concatenate([np.concatenate([hh, hh], axis=1), np.concatenate([hl, np.zeros_like(hl)], axis=1)], axis=0)
    return pack(w), pack(v), pack(w.T.copy()), hx, k.astype(np.float32)


def hilo(x):
    hi = x.astype(BF)
    lo = (x - hi.astype(F32)).astype(BF)
    return hi, lo


def put(s_ref, row, rows, lane, x):
    hi, lo = hilo(x)
    n = x.shape[1]
    s_ref[row : row + rows, lane : lane + n] = hi
    s_ref[row : row + rows, 384 + lane : 384 + lane + n] = lo


def mm3(s_ref, w_ref):
    return jnp.dot(s_ref[...], w_ref[0:768, :], preferred_element_type=F32) + jnp.dot(
        s_ref[:, 0:384], w_ref[768:1152, :], preferred_element_type=F32
    )


def swap(t_ref, s_ref, left):
    for j in range(3):
        for m in range(3):
            r0, d0 = 2 * j * 48, 2 * m * 48
            e = t_ref[r0 : r0 + 48, 128 * m : 128 * m + 128]
            o = t_ref[r0 + 48 : r0 + 96, 128 * m : 128 * m + 128]
            put(s_ref, d0, 48, 128 * j, jnp.where(left, e, pltpu.roll(o, 64, 1)))
            put(s_ref, d0 + 48, 48, 128 * j, jnp.where(left, pltpu.roll(e, 64, 1), o))


def middle(s_ref, t_ref, r_ref, hx_ref, k_ref):
    def xdot(g, base):
        y = jnp.dot(hx_ref[...], r_ref[g * 192 + base : g * 192 + base + 96, :], preferred_element_type=F32)
        return y[0:48] + y[48:96]

    for g in range(3):
        for h in range(2):
            z = 2 * g + h
            hi, lo = hilo(t_ref[z * 48 : z * 48 + 48, :])
            r_ref[g * 192 : g * 192 + 48, h * 384 : h * 384 + 384] = hi
            r_ref[g * 192 + 48 : g * 192 + 96, h * 384 : h * 384 + 384] = lo
    for g in range(3):
        d = xdot(g, 0)
        for h in range(2):
            z = 2 * g + h
            hi, lo = hilo(d[:, h * 384 : h * 384 + 384] * k_ref[z * 48 : z * 48 + 48, :])
            r_ref[g * 192 + 96 : g * 192 + 144, h * 384 : h * 384 + 384] = hi
            r_ref[g * 192 + 144 : g * 192 + 192, h * 384 : h * 384 + 384] = lo
    for g in range(3):
        d = xdot(g, 96)
        for h in range(2):
            put(s_ref, (2 * g + h) * 48, 48, 0, d[:, h * 384 : h * 384 + 384])


def stages(s_ref, t_ref, r_ref, w_ref, v_ref, wt_ref, hx_ref, k_ref):
    left = lax.broadcasted_iota(jnp.int32, (48, 128), 1) < 64

    def mm(weights):
        def run():
            t_ref[...] = mm3(s_ref, weights)

        return run

    def turn():
        swap(t_ref, s_ref, left)

    def mid():
        middle(s_ref, t_ref, r_ref, hx_ref, k_ref)

    return [mm(w_ref), turn, mm(v_ref), mid, mm(v_ref), turn, mm(wt_ref)]


def potentials(sets, tables_, between=None):
    lists = [stages(*refs, *tables_) for refs in sets]
    count = len(lists[0])
    for n in range(count + len(lists) - 1):
        if n == 3 and between is not None:
            between()
        for p, steps in enumerate(lists):
            if 0 <= n - p < count:
                steps[n - p]()
MESH = pl.DeviceIdType.MESH
RELAY = 6


def rcopy(src, dst, send, recv, band, grid):
    return pltpu.make_async_remote_copy(
        src_ref=src, dst_ref=dst, send_sem=send, recv_sem=recv, device_id={"band": band, "grid": grid}, device_id_type=MESH
    )


def landed(ref, sem):
    pltpu.make_async_copy(ref, ref, sem).wait()


def greet(nb, me, g):
    barrier = pltpu.get_barrier_semaphore()
    plane, w = me // 8, me % 8

    def signal(band, grid):
        pl.semaphore_signal(barrier, inc=1, device_id={"band": band, "grid": grid}, device_id_type=MESH)

    def one(o, c):
        n = (w * 4 + g + o) % 32
        signal(plane * 8 + n // 4, n % 4)
        return c

    signal((me + 1) % nb, (g + 2) % 4)
    signal((me + nb - 1) % nb, (g + 2) % 4)
    lax.fori_loop(1, 32, one, 0)
    for o in range(1, 4):
        signal((me + 8 * o) % nb, g)
    pl.semaphore_wait(barrier, 36)


def span(start, size):
    return pl.ds(pl.multiple_of(start, 8), size)


def nth(g, n):
    return (n + 2 * (g // 2)) % 4


def slice_copy(src3, at, buf, rows, send, recv, me, g, w):
    part = src3.at[pl.ds(at * 27, 27)]
    return rcopy(part, buf.at[pl.ds(rows, 27)], send, recv, me // 8 * 8 + w, g)


def scatter_slices(src3, buf3, base, send, recv, me, g, steps):
    w = me % 8

    def one(o, c):
        dst = (w + o) % 8
        slice_copy(src3, dst, buf3, base + w * 27, send, recv, me, (g + 2) % 4, dst).start()
        return c

    for first, last in steps:
        lax.fori_loop(first, last, one, 0)


def lay_orbitals(obuf, line, bh, bl):
    flat = obuf.reshape(3456, 128)

    def chunks(p, carry):
        for h in range(2):
            c = jnp.minimum(2 * p + h, 26)
            for z in range(4):
                for b in range(4):
                    line[pl.ds(h * 128 + z * 32 + b, 8, stride=4), :] = flat[
                        pl.ds(z * 864 + c * 4 + b, 8, stride=108), :
                    ]
            hi, lo = hilo(line[h * 128 : h * 128 + 128, :])
            bh[span(p * 128, 128), h * 128 : h * 128 + 128] = hi
            bl[span(p * 128, 128), h * 128 : h * 128 + 128] = lo
        return carry

    lax.fori_loop(0, 14, chunks, 0)


def margin_tail(me, g, out_ref, vbuf, bh_ref, bl_ref, mt8, red, rs, rr):
    plane, w = me // 8, me % 8
    flat = vbuf.reshape(864, 128)
    m = jnp.zeros((32, 128), F32)
    dims = (((1,), (1,)), ((), ()))
    for p in range(14):
        parts = [
            jnp.concatenate([flat[pl.ds(c * 4 + b, 8, stride=108), :] for b in range(4)], axis=0)
            for c in range(2 * p, min(2 * p + 2, 27))
        ]
        ah, al = hilo(jnp.concatenate(parts, axis=1))
        width = 128 * len(parts)
        bh, bl = bh_ref[p * 128 : p * 128 + 128, 0:width], bl_ref[p * 128 : p * 128 + 128, 0:width]
        both = lax.dot_general(jnp.concatenate([ah, al], axis=0), bh, dims, preferred_element_type=F32)
        m = m + (
            both[0:32]
            + both[32:64]
            + lax.dot_general(ah, bl, dims, preferred_element_type=F32)
        )
    m = m * (1.0 / NCELL)
    lane = lax.broadcasted_iota(jnp.int32, (8, 128), 1) // 32
    for t in range(4):
        piece = jnp.zeros((8, 128), F32)
        for b in range(4):
            row = m[b * 8 : b * 8 + 8, :]
            turn = 32 * ((b - t) % 4)
            piece = jnp.where(lane == b, pltpu.roll(row, turn, 1) if turn else row, piece)
        mt8[pl.ds(t * 64, 8, stride=8), :] = piece
    here = (g * 8 + w) * 8

    def one(o, c):
        n = (w * 4 + g + o) % 32
        dst, to = n // 4, n % 4
        rcopy(mt8.at[span((to * 8 + dst) * 8, 8)], red.at[span(here, 8)], rs, rr, plane * 8 + dst, to).start()
        return c

    lax.fori_loop(1, 32, one, 0)
    red[span(here, 8), :] = mt8[span(here, 8), :]
    landed(red.at[0 : 31 * 8], rr)
    total = jnp.sum(red[pl.ds(0, 32, stride=8), :], axis=0, keepdims=True)
    for b in range(4):
        out_ref[b : b + 1, :] = total[:, b * 32 : b * 32 + 32]
    landed(mt8.at[0 : 31 * 8], rs)


OWN_I = ((0, 0, 1), (0, 1, 0), (2, 2, 3), (2, 3, 2))
OWN_J = ((0, 2, 1), (1, 3, 0), (2, 1, 3), (3, 0, 2))


def chosen(g, values):
    total = 0
    for t, value in enumerate(values):
        total = total + jnp.where(g == t, value, 0)
    return total


def whole_kernel(nb, mine_hbm, w_hbm, v_hbm, wt_hbm, hx_hbm, k_hbm, vec_a, vec_b, m_out, *scratch):
    (w_ref, v_ref, wt_ref, hx_ref, k_ref, own, low, a_ref, u_ref, un, on, ow, sb, xr) = scratch[:14]
    (obuf, vbuf, line, bh, bl, mt8, red, tab, sib_s, sib_r, cross_s, cross_r, fwd_s, fwd_r) = scratch[14:28]
    relay, relay_r, onward_s, onward_r, mine, vec_out, edge = scratch[53:]
    (low_s, low_r, ow_s, ow_r, sb_s, sb_r, xr_s, xr_r, os, orr, vs, vr, zs, zr, rs, rr) = scratch[28:44]
    sets = [scratch[44 + 3 * p : 47 + 3 * p] for p in range(3)]
    shared = (w_ref, v_ref, wt_ref, hx_ref, k_ref)
    me, g = lax.axis_index("band"), lax.axis_index("grid")
    c, s = (g + 2) % 4, g + 1 - 2 * (g % 2)
    cs = (s + 2) % 4
    up, down = (me + 1) % nb, (me + nb - 1) % nb
    begin = pltpu.make_async_copy(mine_hbm, mine, edge.at[0])
    begin.start()
    loads = []
    for n, (a, b) in enumerate(((w_hbm, w_ref), (v_hbm, v_ref), (wt_hbm, wt_ref))):
        loads.append(pltpu.make_async_copy(a.at[0:384], b.at[0:384], tab.at[2 * n]))
        loads.append(pltpu.make_async_copy(a, b.at[384:1152], tab.at[2 * n + 1]))
    loads.append(pltpu.make_async_copy(hx_hbm, hx_ref, tab.at[6]))
    loads.append(pltpu.make_async_copy(k_hbm, k_ref, tab.at[7]))
    for copy in loads:
        copy.start()
    greet(nb, me, g)
    begin.wait()

    mine3 = mine.reshape(216, 4, 128)

    def cells(ref, b, q):
        return ref.at[span(b * 864 + q * 216, 216)]

    cross = []
    for n in range(4):
        b = nth(c, n)
        cross.append(rcopy(mine3.at[:, b, :], cells(own, b, g), cross_s.at[n], cross_r.at[n], me, c))
        cross[n].start()
    sib = []
    for b in range(4):
        sib.append(rcopy(mine3.at[:, b, :], cells(own, b, g), sib_s.at[b], sib_r.at[b], me, s))
        sib[b].start()
    rcopy(mine3.at[:, g, :], low.at[span(g * 216, 216)], low_s, low_r, up, c).start()

    def spread(t, carry):
        for b in range(4):
            own[span(b * 864 + g * 216 + t * 8, 8), :] = mine[pl.ds(t * 32 + b, 8, stride=4), :]
        return carry

    lax.fori_loop(0, 27, spread, 0)

    def low_part(q):
        rcopy(cells(own, g, q), low.at[span(q * 216, 216)], low_s, low_r, up, c).start()

    for b in range(4):
        landed(cells(own, b, s), sib_r.at[b])
    low_part(s)
    fwd = [
        rcopy(cells(own, nth(g, n), c), cells(own, nth(g, n), c), fwd_s.at[n], fwd_r.at[n], me, s) for n in range(4)
    ]

    def crossed(n):
        landed(cells(own, nth(g, n), c), cross_r.at[n])
        fwd[n].start()

    def forwarded(n):
        landed(cells(own, nth(g, n), cs), fwd_r.at[n])

    def spread_low(n):
        @pl.when(g % 2 == n)
        def _():
            low_part(c)

    def spread_low2(n):
        @pl.when(g % 2 == n)
        def _():
            low_part(cs)

    for n in range(2):
        crossed(n)
        spread_low(n)
    for n in range(2):
        forwarded(n)
        spread_low2(n)
    u_ref[...] = jnp.zeros_like(u_ref)
    for copy in loads:
        copy.wait()

    def lay(slot, src, base):
        for r in range(18):
            for xg in range(6):
                row, lane = (r // 3) * 48 + xg * 8, (r % 3) * 128
                a_ref[slot, row : row + 8, lane : lane + 128] = src[pl.ds(base + xg * 144 + r, 8, stride=18), :]

    def unlay(slot, dst, base):
        for r in range(18):
            for xg in range(6):
                row, lane = (r // 3) * 48 + xg * 8, (r % 3) * 128
                dst[pl.ds(base + xg * 144 + r, 8, stride=18), :] = u_ref[slot, row : row + 8, lane : lane + 128]

    def lay_band(n):
        b = nth(g, n)
        lay(b, own, b * 864)

    def unlay_band(n):
        b = nth(g, n)
        unlay(b, un, b * 864)

    lay_band(0)
    lay_band(1)

    back = [
        rcopy(on.at[span(q * 216, 216)], ow.at[span(q * 216, 216)], ow_s.at[n], ow_r.at[n], down, c)
        for n, q in enumerate((s, g, cs, c))
    ]
    pass_on = []
    for n in range(4):
        for h, q in enumerate((cs, s)):
            at = n * 2 + h
            pass_on.append(
                rcopy(cells(un, nth(g, n), q), sb.at[at * 216 : at * 216 + 216], sb_s.at[at], sb_r.at[at], me, s)
            )
    away = [
        rcopy(cells(un, nth(g, n), c), xr.at[(n ^ 2) * 216 : (n ^ 2) * 216 + 216], xr_s.at[n], xr_r.at[n ^ 2], me, c)
        for n in range(4)
    ]

    def send_away(n):
        at = n * 2
        landed(sb.at[at * 216 : at * 216 + 216], sb_r.at[at])
        part = span(nth(g, n) * 864 + c * 216, 216)
        un[part, :] = un[part, :] + sb[at * 216 : at * 216 + 216, :]
        away[n].start()

    plane = me // 8
    above, below = (me + 8) % nb, (me + nb - 8) % nb
    pd = (plane + 3) % 4
    along = []
    for n, (rows, to) in enumerate(
        (
            (pl.ds(plane * 216, 216), above),
            (pl.ds(plane * 216, 216), below),
            (pl.ds(pd * 216, 216), above),
        )
    ):
        along.append(rcopy(obuf.at[rows], obuf.at[rows], zs.at[n], zr.at[n], to, g))

    def own_slot(slot):
        return chosen(g, [row[slot] for row in OWN_I]), chosen(g, [row[slot] for row in OWN_J])

    def own_slot(slot):
        return chosen(g, [row[slot] for row in OWN_I]), chosen(g, [row[slot] for row in OWN_J])

    def pass_orbitals():
        landed(obuf.at[0:216], orr)
        along[0].start()

        @pl.when(me % 8 < 6)
        def _():
            along[1].start()

    def step(n, carry):
        @pl.when(n == 1)
        def _():
            scatter_slices(mine3, obuf, plane * 216, os, orr, me, g, ((0, 8),))
            crossed(2)
            crossed(3)
            landed(low, low_r)
            lay(4, low, 0)

        @pl.when(n == 2)
        def _():
            forwarded(2)
            forwarded(3)
            lay_band(2)
            lay_band(3)

        pairs = []
        for p, slot in ((0, 0), (1, 2)):
            i, j = own_slot(slot)
            weight = jnp.where((n == 0) & (p == 1) & (g % 2 == 1), 0.0, 1.0)
            i, j = jnp.where(n == 0, i, nth(g, 2 * n - 2 + p)), jnp.where(n == 0, j, 4)
            pairs.append((i, j, weight, jnp.where(i == j, 0.0, weight)))
        for p, (i, j, _, _) in enumerate(pairs):
            put(sets[p][0], 0, 288, 0, a_ref[i] * a_ref[j])

        potentials(sets[:2], shared)
        for p, (i, j, one, two) in enumerate(pairs):
            t = sets[p][1][...]
            u_ref[i] = u_ref[i] - one * a_ref[j] * t
            u_ref[j] = u_ref[j] - two * a_ref[i] * t
        return carry

    lax.fori_loop(0, 3, step, 0)

    unlay(4, on, 0)
    for copy in back:
        copy.start()
    pass_orbitals()
    i, j = own_slot(1)
    put(sets[0][0], 0, 288, 0, a_ref[i] * a_ref[j])
    potentials(sets[:1], shared)
    t = sets[0][1][...]
    u_ref[i] = u_ref[i] - a_ref[j] * t
    u_ref[j] = u_ref[j] - a_ref[i] * t
    for n in (2, 3):
        unlay_band(n)
        pass_on[2 * n].start()
        pass_on[2 * n + 1].start()
    for n in (0, 1):
        unlay_band(n)
    send_away(2)
    send_away(3)

    def add_owed(n, q):
        landed(ow.at[span(q * 216, 216)], ow_r.at[n])
        part = span(g * 864 + q * 216, 216)
        un[part, :] = un[part, :] + ow[span(q * 216, 216), :]

    def finish(n):
        b = nth(g, n)
        landed(sb.at[(n * 2 + 1) * 216 : (n * 2 + 2) * 216], sb_r.at[n * 2 + 1])
        landed(xr.at[n * 216 : n * 216 + 216], xr_r.at[n])

        def group(t, carry):
            value = (
                un[span(b * 864 + g * 216 + t * 8, 8), :]
                + sb[span((n * 2 + 1) * 216 + t * 8, 8), :]
                + xr[span(n * 216 + t * 8, 8), :]
            )
            vec_out[pl.ds(t * 32 + b, 8, stride=4), :] = value
            return carry

        lax.fori_loop(0, 27, group, 0)

    add_owed(0, cs)
    pass_on[0].start()
    pass_on[2].start()
    add_owed(1, c)
    send_away(0)
    send_away(1)
    add_owed(2, s)

    @pl.when(me % 8 >= 6)
    def _():
        along[1].start()

    pass_on[1].start()
    pass_on[3].start()
    landed(obuf.at[0:216], zr.at[0])
    along[2].start()
    finish(2)
    finish(3)
    add_owed(3, g)
    finish(0)
    finish(1)
    keep = [
        pltpu.make_async_copy(vec_out.at[0:432], vec_a, edge.at[1]),
        pltpu.make_async_copy(vec_out.at[432:864], vec_b, edge.at[2]),
    ]
    vec3, w = vec_out.reshape(216, 4, 128), me % 8
    slice_copy(vec3, (w + 4) % 8, relay, 0, vs, relay_r, me, c, (w + RELAY) % 8).start()
    scatter_slices(vec3, vbuf, 0, vs, vr, me, g, ((1, 4), (5, 8), (0, 1)))
    landed(relay, relay_r)
    onward = slice_copy(relay, 0, vbuf, (w + 8 - RELAY) % 8 * 27, onward_s, onward_r, me, g, (w + RELAY) % 8)
    onward.start()
    for copy in keep:
        copy.start()
    landed(obuf.at[0:216], zr.at[1])
    landed(obuf.at[0:216], zr.at[2])
    lay_orbitals(obuf, line, bh, bl)
    landed(vbuf.at[0:189], vr)
    landed(relay, onward_r)
    margin_tail(me, g, m_out, vbuf, bh, bl, mt8, red, rs, rr)
    landed(vbuf, os)
    landed(vbuf, vs)
    for copy in cross + fwd + sib + back + pass_on + away + along + [onward]:
        copy.wait_send()
    landed(on, low_s)
    for copy in keep:
        copy.wait()


def on_device(orbitals):
    nb = lax.axis_size("band")
    mine = orbitals.reshape(4, 216, 128).transpose(1, 0, 2).reshape(864, 128)
    vm = pl.BlockSpec(memory_space=pltpu.VMEM)
    hbm = pl.BlockSpec(memory_space=pl.ANY)
    dma = pltpu.SemaphoreType.DMA
    w, v, wt, hx, k = tables()

    def f32(*shape):
        return pltpu.VMEM(shape, F32)

    def b16(*shape):
        return pltpu.VMEM(shape, BF)

    first, second, margin = pl.pallas_call(
        functools.partial(whole_kernel, nb),
        out_shape=(
            jax.ShapeDtypeStruct((432, 128), F32),
            jax.ShapeDtypeStruct((432, 128), F32),
            jax.ShapeDtypeStruct((4, 32), F32),
        ),
        in_specs=[hbm] * 6,
        out_specs=(hbm, hbm, vm),
        scratch_shapes=[b16(1152, 384), b16(1152, 384), b16(1152, 384), b16(96, 96), f32(288, 384)]
        + [f32(3456, 128), f32(864, 128), f32(5, 288, 384), f32(5, 288, 384)]
        + [f32(3456, 128), f32(864, 128), f32(864, 128), f32(1728, 128), f32(864, 128)]
        + [f32(864, 4, 128), f32(216, 4, 128), f32(256, 128), b16(1792, 256), b16(1792, 256), f32(256, 128), f32(256, 128)]
        + [dma((8,)), dma((4,)), dma((4,)), dma((4,)), dma((4,)), dma((4,)), dma((4,)), dma, dma]
        + [dma((4,)), dma((4,)), dma((8,)), dma((8,)), dma((4,)), dma((4,))]
        + [dma] * 4
        + [dma((4,)), dma((4,)), dma, dma]
        + [b16(288, 768), f32(288, 384), b16(576, 768)] * 3
        + [f32(27, 4, 128), dma, dma, dma, f32(864, 128), f32(864, 128), dma((3,))],
        compiler_params=pltpu.CompilerParams(
            collective_id=3, has_side_effects=True, vmem_limit_bytes=60 * 1024 * 1024
        ),
    )(mine, w, v, wt, hx, k)
    vec = jnp.concatenate([first, second], axis=0)
    return vec.reshape(216, 4, 128).transpose(1, 0, 2).reshape(4, 27648), margin.T


def solution(mesh):
    return jax.shard_map(
        on_device,
        mesh=mesh,
        in_specs=(P("band", "grid"),),
        out_specs=(P("band", "grid"), P("grid", "band")),
        check_vma=False,
    )
```
